8 devices in a mesh: dp: 2 (over z, y), tp: 4 (over x, core).
Axes of the slice: x: 2, y: 2, z: 1, core: 2. Of those that a mesh axis runs over, the one named last changes fastest.
Arguments:
- hidden: bfloat16 [64, 512, 768], P('dp')
- positions: int32 [64, 80], P('dp')
- labels: int32 [64, 80], P('dp')
- weights: float32 [64, 80], P('dp')
- w_t: bfloat16 [768, 768], replicated
- b_t: float32 [768], replicated
- gamma: float32 [768], replicated
- beta: float32 [768], replicated
- embed: bfloat16 [30592, 768], P('tp')
- out_bias: float32 [30592], P('tp')
Outputs:
- output 1: float32 [], replicated
- output 2: bfloat16 [64, 512, 768], P('dp')
- output 3: float32 [768, 768], replicated
- output 4: float32 [768], replicated
- output 5: float32 [768], replicated
- output 6: float32 [768], replicated
- output 7: float32 [30592, 768], P('tp')
- output 8: float32 [30592], P('tp')
All inputs are finite; a program needn't handle non-finite values.
Results may differ from the reference program's by a relative error of at most 0.001.
Values sent between devices are 32-bit elements.
A program may use at most 1 GiB of HBM per device.

```python
import jax
import jax.numpy as jnp
from jax import lax

HIDDEN = 768
VOCAB_REAL = 30522
VOCAB_PAD = 30592
SEQ_LEN = 512
MAX_PRED = 80
BATCH_TOTAL = 64
BLOCK_SEQ = 8
NUM_BLOCKS = BATCH_TOTAL // BLOCK_SEQ
BLOCK_ROWS = BLOCK_SEQ * MAX_PRED
LN_EPS = 1e-12
LOSS_EPS = 1e-5


def setup_inputs(seed: int = 0) -> dict:
    key = jax.random.key(seed)
    keys = jax.random.split(key, 10)
    hidden = jax.random.normal(keys[0], (BATCH_TOTAL, SEQ_LEN, HIDDEN), jnp.float32).astype(jnp.bfloat16)
    row_keys = jax.random.split(keys[1], BATCH_TOTAL)
    positions = jax.vmap(lambda row_key: jax.random.permutation(row_key, SEQ_LEN)[:MAX_PRED])(row_keys).astype(jnp.int32)
    labels = jax.random.randint(keys[2], (BATCH_TOTAL, MAX_PRED), 0, VOCAB_REAL, dtype=jnp.int32)
    pred_counts = jax.random.randint(keys[3], (BATCH_TOTAL,), 1, MAX_PRED + 1, dtype=jnp.int32).at[0].set(MAX_PRED)
    weights = (jnp.arange(MAX_PRED, dtype=jnp.int32)[None, :] < pred_counts[:, None]).astype(jnp.float32)
    w_t = (jax.random.normal(keys[4], (HIDDEN, HIDDEN), jnp.float32) * HIDDEN ** -0.5).astype(jnp.bfloat16)
    b_t = 0.5 * jax.random.normal(keys[5], (HIDDEN,), jnp.float32)
    gamma = 1.0 + 0.3 * jax.random.normal(keys[6], (HIDDEN,), jnp.float32)
    beta = 0.3 * jax.random.normal(keys[7], (HIDDEN,), jnp.float32)
    embed = (jax.random.normal(keys[8], (VOCAB_PAD, HIDDEN), jnp.float32) * (1.5 * HIDDEN ** -0.5)).astype(jnp.bfloat16)
    raw_bias = 0.5 * jax.random.normal(keys[9], (VOCAB_PAD,), jnp.float32)
    out_bias = jnp.where(jnp.arange(VOCAB_PAD) < VOCAB_REAL, raw_bias, -1e9)
    return {"hidden": hidden, "positions": positions, "labels": labels, "weights": weights, "w_t": w_t, "b_t": b_t, "gamma": gamma, "beta": beta, "embed": embed, "out_bias": out_bias}


def gelu_norm(pre_act, gamma, beta):
    activated = jax.nn.gelu(pre_act, approximate=False)
    mean_val = jnp.mean(activated, axis=-1, keepdims=True)
    centered = activated - mean_val
    variance = jnp.mean(centered * centered, axis=-1, keepdims=True)
    return centered * lax.rsqrt(variance + LN_EPS) * gamma + beta


def reference(hidden, positions, labels, weights, w_t, b_t, gamma, beta, embed, out_bias):
    picked = jnp.take_along_axis(hidden, positions[:, :, None], axis=1)
    tok_rows = picked.reshape(BATCH_TOTAL * MAX_PRED, HIDDEN)
    pre_act = jnp.dot(tok_rows, w_t, preferred_element_type=jnp.float32) + b_t
    normed, norm_vjp = jax.vjp(gelu_norm, pre_act, gamma, beta)
    t_bf = normed.astype(jnp.bfloat16)
    flat_w = weights.reshape(-1)
    denom = jnp.sum(flat_w) + LOSS_EPS
    vocab_ids = jnp.arange(VOCAB_PAD, dtype=jnp.int32)

    def block_step(carry, block):
        d_embed, d_bias, loss_sum = carry
        t_blk, lab_blk, w_blk = block
        logits = jnp.dot(t_blk, embed.T, preferred_element_type=jnp.float32) + out_bias
        row_max = jnp.max(logits, axis=1)
        shifted = jnp.exp(logits - row_max[:, None])
        sum_exp = jnp.sum(shifted, axis=1)
        log_norm = jnp.log(sum_exp) + row_max
        lab_hot = lab_blk[:, None] == vocab_ids[None, :]
        target_logit = jnp.sum(jnp.where(lab_hot, logits, 0.0), axis=1)
        soft_probs = shifted * (1.0 / sum_exp)[:, None]
        d_logits = jnp.where(lab_hot, soft_probs - 1.0, soft_probs) * (w_blk / denom)[:, None]
        dz_bf = d_logits.astype(jnp.bfloat16)
        d_embed = d_embed + jnp.dot(dz_bf.T, t_blk, preferred_element_type=jnp.float32)
        d_bias = d_bias + jnp.sum(d_logits, axis=0)
        loss_sum = loss_sum + jnp.sum(w_blk * (log_norm - target_logit))
        d_normed = jnp.dot(dz_bf, embed, preferred_element_type=jnp.float32)
        return (d_embed, d_bias, loss_sum), d_normed

    init = (jnp.zeros((VOCAB_PAD, HIDDEN), jnp.float32), jnp.zeros((VOCAB_PAD,), jnp.float32), jnp.zeros((), jnp.float32))
    blocks = (t_bf.reshape(NUM_BLOCKS, BLOCK_ROWS, HIDDEN), labels.reshape(NUM_BLOCKS, BLOCK_ROWS), flat_w.reshape(NUM_BLOCKS, BLOCK_ROWS))
    (d_embed, d_out_bias, loss_sum), d_normed = lax.scan(block_step, init, blocks)
    loss = loss_sum / denom
    d_pre, d_gamma, d_beta = norm_vjp(d_normed.reshape(BATCH_TOTAL * MAX_PRED, HIDDEN))
    d_pre_bf = d_pre.astype(jnp.bfloat16)
    d_w_t = jnp.dot(tok_rows.T, d_pre_bf, preferred_element_type=jnp.float32)
    d_b_t = jnp.sum(d_pre, axis=0)
    d_rows = jnp.dot(d_pre_bf, w_t.T, preferred_element_type=jnp.float32).astype(jnp.bfloat16)
    row_ids = jnp.arange(BATCH_TOTAL)[:, None]
    d_hidden = jnp.zeros((BATCH_TOTAL, SEQ_LEN, HIDDEN), jnp.bfloat16).at[row_ids, positions].add(d_rows.reshape(BATCH_TOTAL, MAX_PRED, HIDDEN))
    return (loss, d_hidden, d_w_t, d_b_t, d_gamma, d_beta, d_embed, d_out_bias)
```

```python
import functools

import jax
import jax.numpy as jnp
from jax import lax
from jax.experimental import pallas as pl
from jax.experimental.pallas import tpu as pltpu
from jax.sharding import PartitionSpec as P

LN_EPS = 1e-12
LOSS_EPS = 1e-5
F32 = jnp.float32
BF16 = jnp.bfloat16
VT = 512
VMEM_LIMIT = 60 * 1024 * 1024
BUCKETS = (1024, 1536, 2048, 2560)

SWAP_DP = ((0, 1), (1, 0))
SWAP_CORE = ((0, 1), (1, 0), (2, 3), (3, 2))
SWAP_X = ((0, 2), (2, 0), (1, 3), (3, 1))


def gelu_norm(pre_act, gamma, beta):
    activated = jax.nn.gelu(pre_act, approximate=False)
    mean_val = jnp.mean(activated, axis=-1, keepdims=True)
    centered = activated - mean_val
    variance = jnp.mean(centered * centered, axis=-1, keepdims=True)
    return centered * lax.rsqrt(variance + LN_EPS) * gamma + beta


def swap_dp(x):
    return lax.ppermute(x, "dp", SWAP_DP)


def swap_core(x):
    return lax.ppermute(x, "tp", SWAP_CORE)


def swap_x(x):
    return lax.ppermute(x, "tp", SWAP_X)


def gather_tp(part, axis_tp):
    other_x = swap_x(part)
    core, x = axis_tp % 2, axis_tp // 2
    mine = jnp.where(x == 0, jnp.stack([part, other_x]), jnp.stack([other_x, part]))
    theirs = swap_core(mine)
    both = jnp.where(core == 0, jnp.stack([mine, theirs], 1), jnp.stack([theirs, mine], 1))
    return both.reshape(4 * part.shape[0], part.shape[1])


def call(body, out, grid, ins, outs, scratch, flops, nbytes, trans, args):
    return pl.pallas_call(
        body,
        out_shape=out,
        grid_spec=pltpu.PrefetchScalarGridSpec(
            num_scalar_prefetch=0, grid=grid, in_specs=ins, out_specs=outs, scratch_shapes=scratch
        ),
        compiler_params=pltpu.CompilerParams(
            dimension_semantics=("arbitrary",) * len(grid), vmem_limit_bytes=VMEM_LIMIT
        ),
        cost_estimate=pl.CostEstimate(flops=flops, bytes_accessed=nbytes, transcendentals=trans),
    )(*args)


def round_rows(x):
    rows, width = x.shape

    def body(x_ref, out_ref, out_t_ref):
        t = x_ref[...].astype(BF16)
        out_ref[...] = t
        out_t_ref[...] = t.T

    return call(
        body,
        (jax.ShapeDtypeStruct((rows, width), BF16), jax.ShapeDtypeStruct((width, rows), BF16)),
        (rows // 256,),
        [pl.BlockSpec((256, width), lambda i: (i, 0))],
        (pl.BlockSpec((256, width), lambda i: (i, 0)), pl.BlockSpec((width, 256), lambda i: (0, i))),
        [], rows * width, rows * width * 8, 0, (x,),
    )


def load_embed(e_ref, e_s, shard):
    steps = pl.cdiv(shard, VT)
    tail = shard - (steps - 1) * VT
    step = pl.program_id(0)

    @pl.when(step < steps - 1)
    def _():
        e_s[...] = e_ref[...]

    @pl.when(step == steps - 1)
    def _():
        e_s[:tail] = e_ref[:tail]
        e_s[tail:] = jnp.zeros((VT - tail, e_s.shape[1]), BF16)


def logits_body(shard, nb, e_ref, t_ref, bias_ref, lab_ref, z_ref, stat_ref, e_s):
    step = pl.program_id(0)

    @pl.when(step == 0)
    def _():
        stat_ref[0:1] = jnp.full((1, stat_ref.shape[1]), -jnp.inf, F32)
        stat_ref[1:3] = jnp.zeros((2, stat_ref.shape[1]), F32)

    load_embed(e_ref, e_s, shard)
    bias = jnp.broadcast_to(bias_ref[...], (128, VT)).T
    bias = jnp.concatenate([bias] * (nb // 128), axis=1)
    vocab = lax.broadcasted_iota(jnp.int32, (VT, nb), 0)
    for i in range(z_ref.shape[1] // nb):
        cols = slice(i * nb, (i + 1) * nb)
        z = jnp.dot(e_s[...], t_ref[:, cols], preferred_element_type=F32) + bias
        z_ref[:, cols] = z
        old = stat_ref[0:1, cols]
        new = jnp.maximum(old, jnp.max(z, axis=0, keepdims=True))
        hot = vocab == lab_ref[:, cols] - step * VT
        stat_ref[1:2, cols] = stat_ref[1:2, cols] * jnp.exp(old - new) + jnp.sum(jnp.exp(z - new), axis=0, keepdims=True)
        stat_ref[2:3, cols] += jnp.sum(jnp.where(hot, z, 0.0), axis=0, keepdims=True)
        stat_ref[0:1, cols] = new


def logits_pass(embed, t_t, bias, lab):
    shard, width = embed.shape
    rows = t_t.shape[1]
    steps = pl.cdiv(shard, VT)
    whole = lambda j: (0, 0)
    return call(
        functools.partial(logits_body, shard, 512 if rows % 512 == 0 else 256),
        (jax.ShapeDtypeStruct((steps * VT, rows), F32), jax.ShapeDtypeStruct((3, rows), F32)),
        (steps,),
        [
            pl.BlockSpec((VT, width), lambda j: (j, 0)),
            pl.BlockSpec((width, rows), whole),
            pl.BlockSpec((1, VT), lambda j: (0, j)),
            pl.BlockSpec((1, rows), whole),
        ],
        (pl.BlockSpec((VT, rows), lambda j: (j, 0)), pl.BlockSpec((3, rows), whole)),
        [pltpu.VMEM((VT, width), BF16)],
        2 * rows * shard * width, rows * shard * 4 + shard * width * 2, rows * shard,
        (embed, t_t, bias, lab),
    )


def grad_logits(z, vec_ref, lab_ref, cols, vocab, step):
    soft = jnp.exp(z - vec_ref[0:1, cols]) * vec_ref[1:2, cols]
    hot = vocab == lab_ref[:, cols] - step * VT
    return jnp.where(hot, soft - 1.0, soft) * vec_ref[2:3, cols]


def lane_groups(dz):
    acc = dz[:, :128]
    for k in range(1, dz.shape[1] // 128):
        acc = acc + dz[:, k * 128:(k + 1) * 128]
    return acc


def hidden_body(shard, nb, z_ref, vec_ref, lab_ref, e_ref, dz_ref, dt_ref, db_ref, e_s):
    step = pl.program_id(0)

    @pl.when(step == 0)
    def _():
        dt_ref[...] = jnp.zeros_like(dt_ref)

    load_embed(e_ref, e_s, shard)
    vocab = lax.broadcasted_iota(jnp.int32, (VT, nb), 0)
    acc = None
    for i in range(z_ref.shape[1] // nb):
        cols = slice(i * nb, (i + 1) * nb)
        dz = grad_logits(z_ref[:, cols], vec_ref, lab_ref, cols, vocab, step)
        part = lane_groups(dz)
        acc = part if acc is None else acc + part
        dz = dz.astype(BF16)
        dz_ref[:, cols] = dz
        dt_ref[:, cols] += lax.dot_general(e_s[...], dz, (((0,), (0,)), ((), ())), preferred_element_type=F32)
    db_ref[...] = jnp.sum(acc.T, axis=0, keepdims=True)


def hidden_pass(z, vec, lab, embed):
    shard, width = embed.shape
    padded, rows = z.shape
    whole = lambda j: (0, 0)
    return call(
        functools.partial(hidden_body, shard, 512 if rows % 512 == 0 else 256),
        (jax.ShapeDtypeStruct((padded, rows), BF16), jax.ShapeDtypeStruct((width, rows), F32), jax.ShapeDtypeStruct((1, padded), F32)),
        (padded // VT,),
        [
            pl.BlockSpec((VT, rows), lambda j: (j, 0)),
            pl.BlockSpec((3, rows), whole),
            pl.BlockSpec((1, rows), whole),
            pl.BlockSpec((VT, width), lambda j: (j, 0)),
        ],
        (pl.BlockSpec((VT, rows), lambda j: (j, 0)), pl.BlockSpec((width, rows), whole), pl.BlockSpec((1, VT), lambda j: (0, j))),
        [pltpu.VMEM((VT, width), BF16)],
        2 * rows * shard * width, rows * shard * 6, rows * shard,
        (z, vec, lab, embed),
    )


def embed_body(nb, dz_ref, z_ref, vec_ref, lab_ref, t_own_ref, t_oth_ref, db_own_ref, de_ref, db_ref, dz_s):
    step = pl.program_id(0)
    vocab = lax.broadcasted_iota(jnp.int32, (VT, nb), 0)
    acc = None
    for i in range(z_ref.shape[1] // nb):
        cols = slice(i * nb, (i + 1) * nb)
        dz = grad_logits(z_ref[:, cols], vec_ref, lab_ref, cols, vocab, step)
        part = lane_groups(dz)
        acc = part if acc is None else acc + part
        dz_s[:, cols] = dz.astype(BF16)
    de_ref[...] = jnp.dot(dz_ref[...], t_own_ref[...], preferred_element_type=F32)
    de_ref[...] += jnp.dot(dz_s[...], t_oth_ref[...], preferred_element_type=F32)
    db_ref[...] = db_own_ref[...] + jnp.sum(acc.T, axis=0, keepdims=True)


def embed_pass(dz_own, z_oth, vec, lab, t_own, t_oth, db_own, shard):
    padded, rows = z_oth.shape
    width = t_own.shape[1]
    whole = lambda j: (0, 0)
    tile = pl.BlockSpec((VT, rows), lambda j: (j, 0))
    strip = pl.BlockSpec((1, VT), lambda j: (0, j))
    return call(
        functools.partial(embed_body, 512 if rows % 512 == 0 else 256),
        (jax.ShapeDtypeStruct((shard, width), F32), jax.ShapeDtypeStruct((1, padded), F32)),
        (padded // VT,),
        [tile, tile, pl.BlockSpec((3, rows), whole), pl.BlockSpec((1, rows), whole), pl.BlockSpec((rows, width), whole), pl.BlockSpec((rows, width), whole), strip],
        (pl.BlockSpec((VT, width), lambda j: (j, 0)), strip),
        [pltpu.VMEM((VT, rows), BF16)],
        4 * rows * shard * width, rows * shard * 6 + shard * width * 4, rows * shard,
        (dz_own, z_oth, vec, lab, t_own, t_oth, db_own),
    )


def sum_tp(partial, core):
    half = partial.shape[0] // 2
    keep = lax.dynamic_slice_in_dim(partial, core * half, half)
    give = lax.dynamic_slice_in_dim(partial, (1 - core) * half, half)
    chip = keep + swap_core(give)
    mine = chip + swap_x(chip)
    theirs = swap_core(mine)
    return jnp.where(core == 0, jnp.concatenate([mine, theirs]), jnp.concatenate([theirs, mine]))


def sum_dp(partial, tp):
    quarter = partial.shape[0] // 4
    mine = lax.dynamic_slice_in_dim(partial, tp * quarter, quarter)
    return gather_tp(mine + swap_dp(mine), tp)


def solution(mesh):
    def branch(rows, args):
        (hidden, positions, labels, w_t, b_t, gamma, beta, embed, out_bias, counts, offsets, n_own, n_oth) = args
        batch, seq_len, width = hidden.shape
        max_pred = positions.shape[1]
        shard_vocab = embed.shape[0]
        tp = lax.axis_index("tp")
        core = tp % 2
        row = jnp.arange(rows, dtype=jnp.int32)
        in_seq = (row[:, None] >= offsets[None, :]) & (row[:, None] < (offsets + counts)[None, :])
        in_seq_f = in_seq.astype(F32)
        slot_row = jnp.where(row < n_own, row - jnp.sum(jnp.where(in_seq, offsets[None, :], 0), 1), -1)
        seq_row = jnp.sum(jnp.where(in_seq, jnp.arange(batch, dtype=jnp.int32)[None, :], 0), 1)
        lab_seq = jnp.dot(in_seq_f, labels.astype(F32), precision=lax.Precision.HIGHEST)
        slot_hot = slot_row[:, None] == jnp.arange(max_pred, dtype=jnp.int32)[None, :]
        lab_own = jnp.sum(jnp.where(slot_hot, lab_seq, 0.0), 1).astype(jnp.int32)
        lab_oth = swap_dp(lab_own)

        pos_hot = (positions[:, :, None] == jnp.arange(seq_len, dtype=jnp.int32)[None, None, :]).astype(BF16)
        picked = jnp.einsum("bps,bsd->bpd", pos_hot, hidden, preferred_element_type=F32).astype(BF16)
        slot_id = jnp.where(slot_row >= 0, seq_row * max_pred + slot_row, -1)
        compact = (slot_id[:, None] == jnp.arange(batch * max_pred, dtype=jnp.int32)[None, :]).astype(BF16)
        tok_rows = jnp.dot(compact, picked.reshape(batch * max_pred, width), preferred_element_type=F32).astype(BF16)
        pre_act = jnp.dot(tok_rows, w_t, preferred_element_type=F32) + b_t
        normed, norm_vjp = jax.vjp(gelu_norm, pre_act, gamma, beta)
        quarter = rows // 4
        t_quarter = lax.dynamic_slice_in_dim(normed, tp * quarter, quarter)
        t_own, t_own_t = round_rows(normed)
        t_oth, t_oth_t = round_rows(gather_tp(swap_dp(t_quarter), tp))

        def local_labels(lab):
            lab = lab - tp * shard_vocab
            return jnp.where((lab >= 0) & (lab < shard_vocab), lab, -1)[None, :]

        lab_own, lab_oth = local_labels(lab_own), local_labels(lab_oth)
        pad = -shard_vocab % VT
        bias = jnp.pad(out_bias, (0, pad), constant_values=-jnp.inf)[None, :]
        z_own, stat_own = logits_pass(embed, t_own_t, bias, lab_own)
        z_oth, stat_oth = logits_pass(embed, t_oth_t, bias, lab_oth)
        stats = jnp.concatenate([stat_own, stat_oth], axis=1)
        for swap in (swap_core, swap_x):
            other = swap(stats)
            best = jnp.maximum(stats[0], other[0])
            stats = jnp.stack([
                best,
                stats[1] * jnp.exp(stats[0] - best) + other[1] * jnp.exp(other[0] - best),
                stats[2] + other[2],
            ])
        row_max, sum_exp, target_logit = stats[0], stats[1], stats[2]
        w_all = jnp.concatenate([row < n_own, row < n_oth]).astype(F32)
        denom = (n_own + n_oth).astype(F32) + LOSS_EPS
        log_norm = jnp.log(sum_exp) + row_max
        half_loss = jnp.sum((w_all * (log_norm - target_logit)).reshape(2, rows), axis=1)
        loss = (half_loss[0] + half_loss[1]) / denom
        vec = jnp.stack([row_max, 1.0 / sum_exp, w_all / denom])
        dz_own, dt_t, db_own = hidden_pass(z_own, vec[:, :rows], lab_own, embed)
        d_normed = sum_tp(dt_t, core).T
        d_embed, d_bias = embed_pass(dz_own, z_oth, vec[:, rows:], lab_oth, t_own, t_oth, db_own, shard_vocab)
        d_out_bias = d_bias[0, :shard_vocab]

        d_pre, d_gamma, d_beta = norm_vjp(d_normed)
        d_pre_bf = d_pre.astype(BF16)
        d_w_t = jnp.einsum("nd,ne->de", tok_rows, d_pre_bf, preferred_element_type=F32)
        vecs = jnp.stack([jnp.sum(d_pre, axis=0), d_gamma, d_beta])
        pack = jnp.concatenate([d_w_t, vecs, jnp.zeros((29, width), F32)])
        pack = sum_dp(pack, tp)
        d_rows = jnp.einsum("ne,de->nd", d_pre_bf, w_t, preferred_element_type=F32).astype(BF16)
        d_slots = jnp.einsum("nq,nd->qd", compact, d_rows, preferred_element_type=F32).astype(BF16)
        d_hidden = jnp.einsum("bps,bpd->bsd", pos_hot, d_slots.reshape(batch, max_pred, width), preferred_element_type=F32).astype(BF16)
        return loss, d_hidden, pack[:width], pack[width], pack[width + 1], pack[width + 2], d_embed, d_out_bias

    def local_step(hidden, positions, labels, weights, w_t, b_t, gamma, beta, embed, out_bias):
        batch = hidden.shape[0]
        counts = jnp.sum(weights, axis=1).astype(jnp.int32)
        seq = jnp.arange(batch, dtype=jnp.int32)
        offsets = jnp.sum(jnp.where(seq[None, :] < seq[:, None], counts[None, :], 0), 1)
        n_own = jnp.sum(counts)
        n_oth = swap_dp(jnp.full((8, 128), n_own, jnp.int32))[0, 0]
        n_max = jnp.maximum(n_own, n_oth)
        which = sum((n_max > b).astype(jnp.int32) for b in BUCKETS[:-1])
        args = (hidden, positions, labels, w_t, b_t, gamma, beta, embed, out_bias, counts, offsets, n_own, n_oth)
        return lax.switch(which, [lambda a, b=b: branch(b, a) for b in BUCKETS], args)

    in_specs = (P("dp", None, None), P("dp", None), P("dp", None), P("dp", None), P(None, None), P(None), P(None), P(None), P("tp", None), P("tp"))
    out_specs = (P(), P("dp", None, None), P(None, None), P(None), P(None), P(None), P("tp", None), P("tp"))
    return jax.shard_map(local_step, mesh=mesh, in_specs=in_specs, out_specs=out_specs, check_vma=False)
```

```python
import functools

import jax
import jax.numpy as jnp
from jax import lax
from jax.experimental import pallas as pl
from jax.experimental.pallas import tpu as pltpu
from jax.sharding import PartitionSpec as P

LN_EPS = 1e-12
LOSS_EPS = 1e-5
F32 = jnp.float32
BF16 = jnp.bfloat16
VT = 512
WIN = 128
VMEM_LIMIT = 60 * 1024 * 1024
BUCKETS = (1024, 1536, 2048, 2560)

SWAP_DP = ((0, 1), (1, 0))
SWAP_CORE = ((0, 1), (1, 0), (2, 3), (3, 2))
SWAP_X = ((0, 2), (2, 0), (1, 3), (3, 1))


def swap_dp(x):
    return lax.ppermute(x, "dp", SWAP_DP)


def swap_core(x):
    return lax.ppermute(x, "tp", SWAP_CORE)


def swap_x(x):
    return lax.ppermute(x, "tp", SWAP_X)


def gather_tp(part, axis_tp):
    other_x = swap_x(part)
    core, x = axis_tp % 2, axis_tp // 2
    mine = jnp.where(x == 0, jnp.stack([part, other_x]), jnp.stack([other_x, part]))
    theirs = swap_core(mine)
    both = jnp.where(core == 0, jnp.stack([mine, theirs], 1), jnp.stack([theirs, mine], 1))
    return both.reshape(4 * part.shape[0], part.shape[1])


def call(body, out, grid, ins, outs, scratch, flops, nbytes, trans, args):
    return pl.pallas_call(
        body,
        out_shape=out,
        grid_spec=pltpu.PrefetchScalarGridSpec(
            num_scalar_prefetch=0, grid=grid, in_specs=ins, out_specs=outs, scratch_shapes=scratch
        ),
        compiler_params=pltpu.CompilerParams(
            dimension_semantics=("arbitrary",) * len(grid), vmem_limit_bytes=VMEM_LIMIT
        ),
        cost_estimate=pl.CostEstimate(flops=flops, bytes_accessed=nbytes, transcendentals=trans),
    )(*args)


def gather_body(per, meta_ref, idx_ref, h_ref, out_ref, acc):
    step = pl.program_id(0)

    @pl.when(step == 0)
    def _():
        acc[...] = jnp.zeros_like(acc)

    seq_len = h_ref.shape[1]
    lane = lax.broadcasted_iota(jnp.int32, (WIN, seq_len), 1).astype(F32)
    for i in range(per):
        col = jnp.broadcast_to(idx_ref[i], (WIN, WIN)).T
        hot = jnp.concatenate([col] * (seq_len // WIN), axis=1) == lane
        rows = jnp.dot(hot.astype(F32).astype(BF16), h_ref[i], preferred_element_type=F32)
        base = pl.multiple_of(meta_ref[step * per + i], 8)
        acc[pl.ds(base, WIN), :] += rows

    @pl.when(step == pl.num_programs(0) - 1)
    def _():
        out_ref[...] = acc[: out_ref.shape[0], :].astype(BF16)


def gather_pass(hidden, idx_win, base, rows):
    batch, seq_len, width = hidden.shape
    per = 4
    return pl.pallas_call(
        functools.partial(gather_body, per),
        out_shape=jax.ShapeDtypeStruct((rows, width), BF16),
        grid_spec=pltpu.PrefetchScalarGridSpec(
            num_scalar_prefetch=1, grid=(batch // per,),
            in_specs=[
                pl.BlockSpec((per, 1, WIN), lambda b, m: (b, 0, 0)),
                pl.BlockSpec((per, seq_len, width), lambda b, m: (b, 0, 0)),
            ],
            out_specs=pl.BlockSpec((rows, width), lambda b, m: (0, 0)),
            scratch_shapes=[pltpu.VMEM((rows + WIN, width), F32)],
        ),
        compiler_params=pltpu.CompilerParams(dimension_semantics=("arbitrary",), vmem_limit_bytes=VMEM_LIMIT),
        cost_estimate=pl.CostEstimate(flops=2 * batch * WIN * seq_len * width, bytes_accessed=batch * seq_len * width * 2, transcendentals=0),
    )(base, idx_win, hidden)


def transform_body(sub, meta_ref, h_ref, w_ref, vec_ref, t_ref, tt_ref, norm_ref, slope_ref, send_a_ref, send_b_ref, pre, t_s):
    step = pl.program_id(0)
    rows, width = h_ref.shape
    pre[...] = jnp.dot(h_ref[...], w_ref[...], preferred_element_type=F32) + vec_ref[0:1]

    def some(i, _):
        at = pl.ds(pl.multiple_of(i * sub, sub), sub)
        u = pre[at, :]
        cdf = 0.5 * (1.0 + lax.erf(u * 0.7071067811865476))
        act = u * cdf
        mean = jnp.mean(act, axis=1, keepdims=True)
        cent = act - mean
        inv = lax.rsqrt(jnp.mean(cent * cent, axis=1, keepdims=True) + LN_EPS)
        norm = cent * inv
        norm_ref[at, :] = norm
        slope_ref[at, :] = (cdf + u * (0.3989422804014327 * jnp.exp(-0.5 * u * u))) * inv
        t_s[at, :] = norm * vec_ref[1:2] + vec_ref[2:3]
        return 0

    lax.fori_loop(0, rows // sub, some, 0)
    t = t_s[...].astype(BF16)
    t_ref[...] = t
    tt_ref[...] = t.T

    @pl.when(step == meta_ref[0])
    def _():
        send_a_ref[...] = t_s[: rows // 2]
        send_b_ref[...] = t_s[rows // 2:]


def transform_pass(h, w_t, vecs, tp):
    rows, width = h.shape
    part = rows // 4
    strip = pl.BlockSpec((part, width), lambda i, m: (i, 0))
    half = pl.BlockSpec((part // 2, width), lambda i, m: (0, 0))
    return pl.pallas_call(
        functools.partial(transform_body, 32),
        out_shape=(
            jax.ShapeDtypeStruct((rows, width), BF16), jax.ShapeDtypeStruct((width, rows), BF16),
            jax.ShapeDtypeStruct((rows, width), F32), jax.ShapeDtypeStruct((rows, width), F32),
            jax.ShapeDtypeStruct((part // 2, width), F32), jax.ShapeDtypeStruct((part // 2, width), F32),
        ),
        grid_spec=pltpu.PrefetchScalarGridSpec(
            num_scalar_prefetch=1, grid=(4,),
            in_specs=[strip, pl.BlockSpec((width, width), lambda i, m: (0, 0)), pl.BlockSpec((8, width), lambda i, m: (0, 0))],
            out_specs=(strip, pl.BlockSpec((width, part), lambda i, m: (0, i)), strip, strip, half, half),
            scratch_shapes=[pltpu.VMEM((part, width), F32), pltpu.VMEM((part, width), F32)],
        ),
        compiler_params=pltpu.CompilerParams(dimension_semantics=("arbitrary",), vmem_limit_bytes=VMEM_LIMIT),
        cost_estimate=pl.CostEstimate(flops=2 * rows * width * width, bytes_accessed=rows * width * 14, transcendentals=2 * rows * width),
    )(tp.reshape(1), h, w_t, vecs)


def collect_body(place_ref, a_ref, b_ref, xa_ref, xb_ref, c_ref, t_ref, tt_ref):
    step = pl.program_id(0)
    pieces = ((a_ref, b_ref), (xa_ref, xb_ref), (c_ref.at[0], c_ref.at[1]), (c_ref.at[2], c_ref.at[3]))
    for i, (first, second) in enumerate(pieces):
        @pl.when(step == i)
        def _():
            t = jnp.concatenate([first[...], second[...]]).astype(BF16)
            t_ref[...] = t
            tt_ref[...] = t.T


def collect_pass(a, b, xa, xb, c, tp):
    part, width = 2 * a.shape[0], a.shape[1]
    rows = 4 * part
    place = tp ^ jnp.array([0, 2, 1, 3], jnp.int32)
    half = pl.BlockSpec((part // 2, width), lambda i, m: (0, 0))
    return pl.pallas_call(
        collect_body,
        out_shape=(jax.ShapeDtypeStruct((rows, width), BF16), jax.ShapeDtypeStruct((width, rows), BF16)),
        grid_spec=pltpu.PrefetchScalarGridSpec(
            num_scalar_prefetch=1, grid=(4,),
            in_specs=[half] * 4 + [pl.BlockSpec((4, part // 2, width), lambda i, m: (0, 0, 0))],
            out_specs=(pl.BlockSpec((part, width), lambda i, m: (m[i], 0)), pl.BlockSpec((width, part), lambda i, m: (0, m[i]))),
        ),
        compiler_params=pltpu.CompilerParams(dimension_semantics=("arbitrary",), vmem_limit_bytes=VMEM_LIMIT),
        cost_estimate=pl.CostEstimate(flops=rows * width, bytes_accessed=rows * width * 8, transcendentals=0),
    )(place, a, b, xa, xb, c)


def back_body(meta_ref, mine_ref, theirs_ref, norm_ref, slope_ref, h_ref, w_ref, gamma_ref, dh_ref, pack_ref):
    step = pl.program_id(0)
    last = pl.num_programs(0) - 1
    width = w_ref.shape[0]

    @pl.when(step == 0)
    def _():
        pack_ref[...] = jnp.zeros_like(pack_ref)

    @pl.when(step < last)
    def _():
        low = meta_ref[0] == 0
        mine, theirs = mine_ref[...].T, theirs_ref[...].T
        d_t = jnp.concatenate([jnp.where(low, mine, theirs), jnp.where(low, theirs, mine)], axis=1)
        norm = norm_ref[...]
        pack_ref[width + 1:width + 2] += jnp.sum(d_t * norm, axis=0, keepdims=True)
        pack_ref[width + 2:width + 3] += jnp.sum(d_t, axis=0, keepdims=True)
        g = d_t * gamma_ref[...]
        g_mean = jnp.mean(g, axis=1, keepdims=True)
        gn_mean = jnp.mean(g * norm, axis=1, keepdims=True)
        d_u = (g - g_mean - norm * gn_mean) * slope_ref[...]
        pack_ref[width:width + 1] += jnp.sum(d_u, axis=0, keepdims=True)
        d_u = d_u.astype(BF16)
        pack_ref[:width] += lax.dot_general(h_ref[...], d_u, (((0,), (0,)), ((), ())), preferred_element_type=F32)
        d_h = lax.dot_general(d_u, w_ref[...], (((1,), (1,)), ((), ())), preferred_element_type=F32)
        dh_ref[...] = d_h.astype(BF16).astype(F32)

    @pl.when(step == last)
    def _():
        dh_ref[...] = jnp.zeros_like(dh_ref)


def back_pass(mine, theirs, norm, slope, h, w_t, gamma, core):
    rows, width = norm.shape
    part = 128
    steps = rows // part
    strip = pl.BlockSpec((part, width), lambda i, m: (jnp.minimum(i, steps - 1), 0))
    flat = pl.BlockSpec((width // 2, part), lambda i, m: (0, jnp.minimum(i, steps - 1)))
    return pl.pallas_call(
        back_body,
        out_shape=(jax.ShapeDtypeStruct((rows + part, width), F32), jax.ShapeDtypeStruct((width + 32, width), F32)),
        grid_spec=pltpu.PrefetchScalarGridSpec(
            num_scalar_prefetch=1, grid=(steps + 1,),
            in_specs=[flat, flat, strip, strip, strip, pl.BlockSpec((width, width), lambda i, m: (0, 0)), pl.BlockSpec((1, width), lambda i, m: (0, 0))],
            out_specs=(pl.BlockSpec((part, width), lambda i, m: (i, 0)), pl.BlockSpec((width + 32, width), lambda i, m: (0, 0))),
        ),
        compiler_params=pltpu.CompilerParams(dimension_semantics=("arbitrary",), vmem_limit_bytes=VMEM_LIMIT),
        cost_estimate=pl.CostEstimate(flops=4 * rows * width * width, bytes_accessed=rows * width * 18, transcendentals=0),
    )(core.reshape(1), mine, theirs, norm, slope, h, w_t, gamma)


def scatter_body(per, meta_ref, idx_ref, dh_ref, out_ref):
    step = pl.program_id(0)
    seq_len = out_ref.shape[1]
    spot = lax.broadcasted_iota(jnp.int32, (seq_len, WIN), 0).astype(F32)
    for i in range(per):
        hot = (spot == idx_ref[i]).astype(F32).astype(BF16)
        base = pl.multiple_of(meta_ref[step * per + i], 8)
        rows = dh_ref[pl.ds(base, WIN), :].astype(BF16)
        out_ref[i] = jnp.dot(hot, rows, preferred_element_type=F32).astype(BF16)


def scatter_pass(dh, idx_win, base, batch, seq_len):
    width = dh.shape[1]
    per = 4
    return pl.pallas_call(
        functools.partial(scatter_body, per),
        out_shape=jax.ShapeDtypeStruct((batch, seq_len, width), BF16),
        grid_spec=pltpu.PrefetchScalarGridSpec(
            num_scalar_prefetch=1, grid=(batch // per,),
            in_specs=[
                pl.BlockSpec((per, 1, WIN), lambda b, m: (b, 0, 0)),
                pl.BlockSpec(dh.shape, lambda b, m: (0, 0)),
            ],
            out_specs=pl.BlockSpec((per, seq_len, width), lambda b, m: (b, 0, 0)),
        ),
        compiler_params=pltpu.CompilerParams(dimension_semantics=("arbitrary",), vmem_limit_bytes=VMEM_LIMIT),
        cost_estimate=pl.CostEstimate(flops=2 * batch * WIN * seq_len * width, bytes_accessed=batch * seq_len * width * 2, transcendentals=0),
    )(base, idx_win, dh)


def load_embed(e_ref, e_s, shard):
    steps = pl.cdiv(shard, VT)
    tail = shard - (steps - 1) * VT
    step = pl.program_id(0)

    @pl.when(step < steps - 1)
    def _():
        e_s[...] = e_ref[...]

    @pl.when(step == steps - 1)
    def _():
        e_s[:tail] = e_ref[:tail]
        e_s[tail:] = jnp.zeros((VT - tail, e_s.shape[1]), BF16)


def logits_body(shard, nb, e_ref, t_ref, bias_ref, lab_ref, z_ref, stat_ref, e_s):
    step = pl.program_id(0)

    @pl.when(step == 0)
    def _():
        stat_ref[0:1] = jnp.full((1, stat_ref.shape[1]), -jnp.inf, F32)
        stat_ref[1:3] = jnp.zeros((2, stat_ref.shape[1]), F32)

    load_embed(e_ref, e_s, shard)
    bias = jnp.broadcast_to(bias_ref[...], (128, VT)).T
    bias = jnp.concatenate([bias] * (nb // 128), axis=1)
    vocab = lax.broadcasted_iota(jnp.int32, (VT, nb), 0)
    for i in range(z_ref.shape[1] // nb):
        cols = slice(i * nb, (i + 1) * nb)
        z = jnp.dot(e_s[...], t_ref[:, cols], preferred_element_type=F32) + bias
        z_ref[:, cols] = z
        old = stat_ref[0:1, cols]
        new = jnp.maximum(old, jnp.max(z, axis=0, keepdims=True))
        hot = vocab == lab_ref[:, cols] - step * VT
        stat_ref[1:2, cols] = stat_ref[1:2, cols] * jnp.exp(old - new) + jnp.sum(jnp.exp(z - new), axis=0, keepdims=True)
        stat_ref[2:3, cols] += jnp.sum(jnp.where(hot, z, 0.0), axis=0, keepdims=True)
        stat_ref[0:1, cols] = new


def logits_pass(embed, t_t, bias, lab):
    shard, width = embed.shape
    rows = t_t.shape[1]
    steps = pl.cdiv(shard, VT)
    whole = lambda j: (0, 0)
    return call(
        functools.partial(logits_body, shard, 512 if rows % 512 == 0 else 256),
        (jax.ShapeDtypeStruct((steps * VT, rows), F32), jax.ShapeDtypeStruct((3, rows), F32)),
        (steps,),
        [
            pl.BlockSpec((VT, width), lambda j: (j, 0)),
            pl.BlockSpec((width, rows), whole),
            pl.BlockSpec((1, VT), lambda j: (0, j)),
            pl.BlockSpec((1, rows), whole),
        ],
        (pl.BlockSpec((VT, rows), lambda j: (j, 0)), pl.BlockSpec((3, rows), whole)),
        [pltpu.VMEM((VT, width), BF16)],
        2 * rows * shard * width, rows * shard * 4 + shard * width * 2, rows * shard,
        (embed, t_t, bias, lab),
    )


def grad_logits(z, vec_ref, lab_ref, cols, vocab, step):
    soft = jnp.exp(z - vec_ref[0:1, cols]) * vec_ref[1:2, cols]
    hot = vocab == lab_ref[:, cols] - step * VT
    return jnp.where(hot, soft - 1.0, soft) * vec_ref[2:3, cols]


def lane_groups(dz):
    acc = dz[:, :128]
    for k in range(1, dz.shape[1] // 128):
        acc = acc + dz[:, k * 128:(k + 1) * 128]
    return acc


def hidden_body(shard, nb, pieces, core_ref, *refs):
    z_refs, (vec_ref, lab_ref, e_ref, dz_ref, keep_ref, give_ref, db_ref, e_s, k_s) = refs[:pieces], refs[pieces:]
    step = pl.program_id(0)
    half = k_s.shape[1]

    @pl.when(step == 0)
    def _():
        keep_ref[...] = jnp.zeros_like(keep_ref)
        give_ref[...] = jnp.zeros_like(give_ref)

    load_embed(e_ref, e_s, shard)
    core = core_ref[0]
    k_s[...] = e_s[:, pl.ds(pl.multiple_of(core * half, 128), half)]
    g_s = e_s.at[:, pl.ds(pl.multiple_of((1 - core) * half, 128), half)]
    vocab = lax.broadcasted_iota(jnp.int32, (VT, nb), 0)
    acc = None
    for i in range(dz_ref.shape[1] // nb):
        cols = slice(i * nb, (i + 1) * nb)
        each = z_refs[0].shape[1]
        z_ref, at = z_refs[i * nb // each], i * nb % each
        dz = grad_logits(z_ref[:, at:at + nb], vec_ref, lab_ref, cols, vocab, step)
        part = lane_groups(dz)
        acc = part if acc is None else acc + part
        dz = dz.astype(BF16)
        dz_ref[:, cols] = dz
        keep_ref[:, cols] += lax.dot_general(k_s[...], dz, (((0,), (0,)), ((), ())), preferred_element_type=F32)
        give_ref[:, cols] += lax.dot_general(g_s[...], dz, (((0,), (0,)), ((), ())), preferred_element_type=F32)
    db_ref[...] = jnp.sum(acc.T, axis=0, keepdims=True)


def hidden_pass(zs, vec, lab, embed, core):
    shard, width = embed.shape
    padded = zs[0].shape[0]
    rows = sum(z.shape[1] for z in zs)
    whole = lambda j, m: (0, 0)
    tile = lambda n: pl.BlockSpec((VT, n), lambda j, m: (j, 0))
    return pl.pallas_call(
        functools.partial(hidden_body, shard, 512, len(zs)),
        out_shape=(
            jax.ShapeDtypeStruct((padded, rows), BF16),
            jax.ShapeDtypeStruct((width // 2, rows), F32), jax.ShapeDtypeStruct((width // 2, rows), F32),
            jax.ShapeDtypeStruct((1, padded), F32),
        ),
        grid_spec=pltpu.PrefetchScalarGridSpec(
            num_scalar_prefetch=1, grid=(padded // VT,),
            in_specs=[tile(z.shape[1]) for z in zs] + [pl.BlockSpec((3, rows), whole), pl.BlockSpec((1, rows), whole), tile(width)],
            out_specs=(tile(rows), pl.BlockSpec((width // 2, rows), whole), pl.BlockSpec((width // 2, rows), whole), pl.BlockSpec((1, VT), lambda j, m: (0, j))),
            scratch_shapes=[pltpu.VMEM((VT, width), BF16), pltpu.VMEM((VT, width // 2), BF16)],
        ),
        compiler_params=pltpu.CompilerParams(dimension_semantics=("arbitrary",), vmem_limit_bytes=VMEM_LIMIT),
        cost_estimate=pl.CostEstimate(flops=2 * rows * shard * width, bytes_accessed=rows * shard * 6, transcendentals=rows * shard),
    )(core.reshape(1), *zs, vec, lab, embed)


def embed_body(nb, dz_ref, z_ref, vec_ref, lab_ref, t_own_ref, t_oth_ref, db_own_ref, de_ref, db_ref, dz_s):
    step = pl.program_id(0)
    vocab = lax.broadcasted_iota(jnp.int32, (VT, nb), 0)
    acc = None
    for i in range(z_ref.shape[1] // nb):
        cols = slice(i * nb, (i + 1) * nb)
        dz = grad_logits(z_ref[:, cols], vec_ref, lab_ref, cols, vocab, step)
        part = lane_groups(dz)
        acc = part if acc is None else acc + part
        dz_s[:, cols] = dz.astype(BF16)
    de_ref[...] = jnp.dot(dz_ref[...], t_own_ref[...], preferred_element_type=F32)
    de_ref[...] += jnp.dot(dz_s[...], t_oth_ref[...], preferred_element_type=F32)
    db_ref[...] = db_own_ref[...] + jnp.sum(acc.T, axis=0, keepdims=True)


def embed_pass(dz_own, z_oth, vec, lab, t_own, t_oth, db_own, shard):
    padded, rows = z_oth.shape
    width = t_own.shape[1]
    whole = lambda j: (0, 0)
    tile = pl.BlockSpec((VT, rows), lambda j: (j, 0))
    strip = pl.BlockSpec((1, VT), lambda j: (0, j))
    return call(
        functools.partial(embed_body, 512 if rows % 512 == 0 else 256),
        (jax.ShapeDtypeStruct((shard, width), F32), jax.ShapeDtypeStruct((1, padded), F32)),
        (padded // VT,),
        [tile, tile, pl.BlockSpec((3, rows), whole), pl.BlockSpec((1, rows), whole), pl.BlockSpec((rows, width), whole), pl.BlockSpec((rows, width), whole), strip],
        (pl.BlockSpec((VT, width), lambda j: (j, 0)), strip),
        [pltpu.VMEM((VT, rows), BF16)],
        4 * rows * shard * width, rows * shard * 6 + shard * width * 4, rows * shard,
        (dz_own, z_oth, vec, lab, t_own, t_oth, db_own),
    )


def solution(mesh):
    def branch(rows, args):
        (hidden, positions, labels, w_t, b_t, gamma, beta, embed, out_bias, counts, offsets, n_own, n_oth) = args
        batch, seq_len, width = hidden.shape
        max_pred = positions.shape[1]
        shard_vocab = embed.shape[0]
        tp = lax.axis_index("tp")
        core = tp % 2
        row = jnp.arange(rows, dtype=jnp.int32)
        in_seq = (row[:, None] >= offsets[None, :]) & (row[:, None] < (offsets + counts)[None, :])
        slot_row = jnp.where(row < n_own, row - jnp.sum(jnp.where(in_seq, offsets[None, :], 0), 1), -1)
        lab_seq = jnp.dot(in_seq.astype(F32), labels.astype(F32), precision=lax.Precision.HIGHEST)
        slot_hot = slot_row[:, None] == jnp.arange(max_pred, dtype=jnp.int32)[None, :]
        lab_own = jnp.sum(jnp.where(slot_hot, lab_seq, 0.0), 1).astype(jnp.int32)
        lab_oth = swap_dp(lab_own)

        shift = offsets % 8
        base = offsets - shift
        live = jnp.where(jnp.arange(max_pred)[None, :] < counts[:, None], positions, -1).astype(F32)
        idx_win = jnp.full((batch, WIN), -1.0, F32)
        for k in range(8):
            moved = jnp.pad(live, ((0, 0), (k, WIN - max_pred - k)), constant_values=-1.0)
            idx_win = jnp.where((shift == k)[:, None], moved, idx_win)
        idx_win = idx_win[:, None, :]
        tok_rows = gather_pass(hidden, idx_win, base, rows)
        vecs = jnp.stack([b_t, gamma, beta] + [jnp.zeros_like(b_t)] * 5)
        t_own, t_own_t, norm, slope, send_a, send_b = transform_pass(tok_rows, w_t, vecs, tp)

        def local_labels(lab):
            lab = lab - tp * shard_vocab
            return jnp.where((lab >= 0) & (lab < shard_vocab), lab, -1)[None, :]

        lab_own, lab_oth = local_labels(lab_own), local_labels(lab_oth)
        pad = -shard_vocab % VT
        bias = jnp.pad(out_bias, (0, pad), constant_values=-jnp.inf)[None, :]

        def own_logits(i, tied):
            cols = slice(i * 512, (i + 1) * 512)
            t_cols, tied = lax.optimization_barrier((t_own_t[:, cols], tied))
            return logits_pass(embed, t_cols, bias, lab_own[:, cols]), tied

        a, b = swap_dp(send_a), swap_dp(send_b)
        parts = [logits_pass(embed, t_own_t[:, :512], bias, lab_own[:, :512])]
        (a, parts[0]) = lax.optimization_barrier((a, parts[0]))
        xa = swap_x(a)
        got, a = own_logits(1, a)
        parts.append(got)
        (b, parts[1]) = lax.optimization_barrier((b, parts[1]))
        xb = swap_x(b)
        for i in range(2, rows // 512):
            got, b = own_logits(i, b)
            parts.append(got)
        (xa, xb, parts[-1]) = lax.optimization_barrier((xa, xb, parts[-1]))
        c = swap_core(jnp.stack([a, b, xa, xb]))
        t_oth, t_oth_t = collect_pass(a, b, xa, xb, c, tp)
        z_own = [p[0] for p in parts]
        stat_own = jnp.concatenate([p[1] for p in parts], axis=1)
        z_oth, stat_oth = logits_pass(embed, t_oth_t, bias, lab_oth)
        stats = jnp.concatenate([stat_own, stat_oth], axis=1)
        for swap in (swap_core, swap_x):
            other = swap(stats)
            best = jnp.maximum(stats[0], other[0])
            stats = jnp.stack([
                best,
                stats[1] * jnp.exp(stats[0] - best) + other[1] * jnp.exp(other[0] - best),
                stats[2] + other[2],
            ])
        row_max, sum_exp, target_logit = stats[0], stats[1], stats[2]
        w_all = jnp.concatenate([row < n_own, row < n_oth]).astype(F32)
        denom = (n_own + n_oth).astype(F32) + LOSS_EPS
        log_norm = jnp.log(sum_exp) + row_max
        half_loss = jnp.sum((w_all * (log_norm - target_logit)).reshape(2, rows), axis=1)
        loss = (half_loss[0] + half_loss[1]) / denom
        vec = jnp.stack([row_max, 1.0 / sum_exp, w_all / denom])
        dz_own, keep, give, db_own = hidden_pass(z_own, vec[:, :rows], lab_own, embed, core)
        chip = keep + swap_core(give)
        other = swap_x(chip)
        d_embed, d_bias = embed_pass(dz_own, z_oth, vec[:, rows:], lab_oth, t_own, t_oth, db_own, shard_vocab)
        d_out_bias = d_bias[0, :shard_vocab]
        (other, d_out_bias) = lax.optimization_barrier((other, d_out_bias))
        mine = chip + other
        theirs = swap_core(mine)
        d_rows, pack = back_pass(mine, theirs, norm, slope, tok_rows, w_t, gamma[None, :], core)
        quarter = pack.shape[0] // 4
        pack = lax.dynamic_slice_in_dim(pack, tp * quarter, quarter)
        other = swap_dp(pack)
        d_hidden = scatter_pass(d_rows, idx_win, base, batch, seq_len)
        (other, d_hidden) = lax.optimization_barrier((other, d_hidden))
        pack = gather_tp(pack + other, tp)
        return loss, d_hidden, pack[:width], pack[width], pack[width + 1], pack[width + 2], d_embed, d_out_bias

    def local_step(hidden, positions, labels, weights, w_t, b_t, gamma, beta, embed, out_bias):
        batch = hidden.shape[0]
        counts = jnp.sum(weights, axis=1).astype(jnp.int32)
        seq = jnp.arange(batch, dtype=jnp.int32)
        offsets = jnp.sum(jnp.where(seq[None, :] < seq[:, None], counts[None, :], 0), 1)
        n_own = jnp.sum(counts)
        n_oth = swap_dp(jnp.full((8, 128), n_own, jnp.int32))[0, 0]
        n_max = jnp.maximum(n_own, n_oth)
        which = sum((n_max > b).astype(jnp.int32) for b in BUCKETS[:-1])
        args = (hidden, positions, labels, w_t, b_t, gamma, beta, embed, out_bias, counts, offsets, n_own, n_oth)
        return lax.switch(which, [lambda a, b=b: branch(b, a) for b in BUCKETS], args)

    in_specs = (P("dp", None, None), P("dp", None), P("dp", None), P("dp", None), P(None, None), P(None), P(None), P(None), P("tp", None), P("tp"))
    out_specs = (P(), P("dp", None, None), P(None, None), P(None), P(None), P(None), P("tp", None), P("tp"))
    return jax.shard_map(local_step, mesh=mesh, in_specs=in_specs, out_specs=out_specs, check_vma=False)
```

```python
import functools

import jax
import jax.numpy as jnp
from jax import lax
from jax.experimental import pallas as pl
from jax.experimental.pallas import tpu as pltpu
from jax.sharding import PartitionSpec as P

LN_EPS = 1e-12
LOSS_EPS = 1e-5
F32 = jnp.float32
BF16 = jnp.bfloat16
VT = 512
WIN = 128
VMEM_LIMIT = 60 * 1024 * 1024
BUCKETS = (2560, 2048, 1024, 1536)

SWAP_DP = ((0, 1), (1, 0))
SWAP_CORE = ((0, 1), (1, 0), (2, 3), (3, 2))
SWAP_X = ((0, 2), (2, 0), (1, 3), (3, 1))


def swap_dp(x):
    return lax.ppermute(x, "dp", SWAP_DP)


def swap_core(x):
    return lax.ppermute(x, "tp", SWAP_CORE)


def swap_x(x):
    return lax.ppermute(x, "tp", SWAP_X)


def call(body, out, grid, ins, outs, scratch, flops, nbytes, trans, args):
    return pl.pallas_call(
        body,
        out_shape=out,
        grid_spec=pltpu.PrefetchScalarGridSpec(
            num_scalar_prefetch=0, grid=grid, in_specs=ins, out_specs=outs, scratch_shapes=scratch
        ),
        compiler_params=pltpu.CompilerParams(
            dimension_semantics=("arbitrary",) * len(grid), vmem_limit_bytes=VMEM_LIMIT
        ),
        cost_estimate=pl.CostEstimate(flops=flops, bytes_accessed=nbytes, transcendentals=trans),
    )(*args)


def gather_body(per, meta_ref, idx_ref, h_ref, out_ref, acc):
    step = pl.program_id(0)

    @pl.when(step == 0)
    def _():
        acc[...] = jnp.zeros_like(acc)

    seq_len = h_ref.shape[1]
    lane = lax.broadcasted_iota(jnp.int32, (WIN, seq_len), 1).astype(F32)
    for i in range(per):
        col = jnp.broadcast_to(idx_ref[i], (WIN, WIN)).T
        hot = jnp.concatenate([col] * (seq_len // WIN), axis=1) == lane
        rows = jnp.dot(hot.astype(F32).astype(BF16), h_ref[i], preferred_element_type=F32)
        base = pl.multiple_of(meta_ref[step * per + i], 8)
        acc[pl.ds(base, WIN), :] += rows

    @pl.when(step == pl.num_programs(0) - 1)
    def _():
        out_ref[...] = acc[: out_ref.shape[0], :].astype(BF16)


def gather_pass(hidden, idx_win, base, rows):
    batch, seq_len, width = hidden.shape
    per = 4
    return pl.pallas_call(
        functools.partial(gather_body, per),
        out_shape=jax.ShapeDtypeStruct((rows, width), BF16),
        grid_spec=pltpu.PrefetchScalarGridSpec(
            num_scalar_prefetch=1, grid=(batch // per,),
            in_specs=[
                pl.BlockSpec((per, 1, WIN), lambda b, m: (b, 0, 0)),
                pl.BlockSpec((per, seq_len, width), lambda b, m: (b, 0, 0)),
            ],
            out_specs=pl.BlockSpec((rows, width), lambda b, m: (0, 0)),
            scratch_shapes=[pltpu.VMEM((rows + WIN, width), F32)],
        ),
        compiler_params=pltpu.CompilerParams(dimension_semantics=("arbitrary",), vmem_limit_bytes=VMEM_LIMIT),
        cost_estimate=pl.CostEstimate(flops=2 * batch * WIN * seq_len * width, bytes_accessed=batch * seq_len * width * 2, transcendentals=0),
    )(base, idx_win, hidden)


def transform_body(sub, meta_ref, h_ref, w_ref, vec_ref, t_ref, tt_ref, norm_ref, slope_ref, send_ref, pre, t_s):
    step = pl.program_id(0)
    rows, width = h_ref.shape
    pre[...] = jnp.dot(h_ref[...], w_ref[...], preferred_element_type=F32) + vec_ref[0:1]

    def some(i, _):
        at = pl.ds(pl.multiple_of(i * sub, sub), sub)
        u = pre[at, :]
        cdf = 0.5 * (1.0 + lax.erf(u * 0.7071067811865476))
        act = u * cdf
        mean = jnp.mean(act, axis=1, keepdims=True)
        cent = act - mean
        inv = lax.rsqrt(jnp.mean(cent * cent, axis=1, keepdims=True) + LN_EPS)
        norm = cent * inv
        norm_ref[at, :] = norm
        slope_ref[at, :] = (cdf + u * (0.3989422804014327 * jnp.exp(-0.5 * u * u))) * inv
        t_s[at, :] = norm * vec_ref[1:2] + vec_ref[2:3]
        return 0

    lax.fori_loop(0, rows // sub, some, 0)
    t = t_s[...].astype(BF16)
    t_ref[...] = t
    tt_ref[...] = t.T

    @pl.when(step == meta_ref[0])
    def _():
        send_ref[...] = t_s[...]


def transform_pass(h, w_t, vecs, tp, rows):
    width = h.shape[1]
    part = rows // 4
    strip = pl.BlockSpec((part, width), lambda i, m: (i, 0))
    return pl.pallas_call(
        functools.partial(transform_body, 32),
        out_shape=(
            jax.ShapeDtypeStruct((rows, width), BF16), jax.ShapeDtypeStruct((width, rows), BF16),
            jax.ShapeDtypeStruct((rows, width), F32), jax.ShapeDtypeStruct((rows, width), F32),
            jax.ShapeDtypeStruct((part, width), F32),
        ),
        grid_spec=pltpu.PrefetchScalarGridSpec(
            num_scalar_prefetch=1, grid=(4,),
            in_specs=[strip, pl.BlockSpec((width, width), lambda i, m: (0, 0)), pl.BlockSpec((8, width), lambda i, m: (0, 0))],
            out_specs=(strip, pl.BlockSpec((width, part), lambda i, m: (0, i)), strip, strip, pl.BlockSpec((part, width), lambda i, m: (0, 0))),
            scratch_shapes=[pltpu.VMEM((part, width), F32), pltpu.VMEM((part, width), F32)],
        ),
        compiler_params=pltpu.CompilerParams(dimension_semantics=("arbitrary",), vmem_limit_bytes=VMEM_LIMIT),
        cost_estimate=pl.CostEstimate(flops=2 * rows * width * width, bytes_accessed=rows * width * 14, transcendentals=2 * rows * width),
    )(tp.reshape(1), h, w_t, vecs)


def collect_body(place_ref, *refs):
    t_ref, tt_ref = refs[4:]
    for i, piece in enumerate(refs[:4]):
        @pl.when(pl.program_id(0) == i)
        def _():
            t = piece[...].astype(BF16)
            t_ref[...] = t
            tt_ref[...] = t.T


def collect_pass(pieces, tp):
    part, width = pieces[0].shape
    rows = 4 * part
    place = tp ^ jnp.array([0, 2, 1, 3], jnp.int32)
    return pl.pallas_call(
        collect_body,
        out_shape=(jax.ShapeDtypeStruct((rows, width), BF16), jax.ShapeDtypeStruct((width, rows), BF16)),
        grid_spec=pltpu.PrefetchScalarGridSpec(
            num_scalar_prefetch=1, grid=(4,),
            in_specs=[pl.BlockSpec((part, width), lambda i, m: (0, 0))] * 4,
            out_specs=(pl.BlockSpec((part, width), lambda i, m: (m[i], 0)), pl.BlockSpec((width, part), lambda i, m: (0, m[i]))),
        ),
        compiler_params=pltpu.CompilerParams(dimension_semantics=("arbitrary",), vmem_limit_bytes=VMEM_LIMIT),
        cost_estimate=pl.CostEstimate(flops=rows * width, bytes_accessed=rows * width * 8, transcendentals=0),
    )(place, *pieces)


def back_body(meta_ref, mine_ref, theirs_ref, norm_ref, slope_ref, h_ref, w_ref, gamma_ref, dh_ref, pack_ref):
    step = pl.program_id(0)
    last = pl.num_programs(0) - 1
    width = w_ref.shape[0]

    @pl.when(step == 0)
    def _():
        pack_ref[...] = jnp.zeros_like(pack_ref)

    @pl.when(step < last)
    def _():
        low = meta_ref[0] == 0
        mine, theirs = mine_ref[...].T, theirs_ref[...].T
        d_t = jnp.concatenate([jnp.where(low, mine, theirs), jnp.where(low, theirs, mine)], axis=1)
        norm = norm_ref[...]
        pack_ref[width + 1:width + 2] += jnp.sum(d_t * norm, axis=0, keepdims=True)
        pack_ref[width + 2:width + 3] += jnp.sum(d_t, axis=0, keepdims=True)
        g = d_t * gamma_ref[...]
        g_mean = jnp.mean(g, axis=1, keepdims=True)
        gn_mean = jnp.mean(g * norm, axis=1, keepdims=True)
        d_u = (g - g_mean - norm * gn_mean) * slope_ref[...]
        pack_ref[width:width + 1] += jnp.sum(d_u, axis=0, keepdims=True)
        d_u = d_u.astype(BF16)
        pack_ref[:width] += lax.dot_general(h_ref[...], d_u, (((0,), (0,)), ((), ())), preferred_element_type=F32)
        d_h = lax.dot_general(d_u, w_ref[...], (((1,), (1,)), ((), ())), preferred_element_type=F32)
        dh_ref[...] = d_h.astype(BF16).astype(F32)

    @pl.when(step == last)
    def _():
        dh_ref[...] = jnp.zeros_like(dh_ref)


def back_pass(mine, theirs, norm, slope, h, w_t, gamma, core, rows):
    width = norm.shape[1]
    part = 128
    steps = rows // part
    strip = pl.BlockSpec((part, width), lambda i, m: (jnp.minimum(i, steps - 1), 0))
    flat = pl.BlockSpec((width // 2, part), lambda i, m: (0, jnp.minimum(i, steps - 1)))
    return pl.pallas_call(
        back_body,
        out_shape=(jax.ShapeDtypeStruct((rows + part, width), F32), jax.ShapeDtypeStruct((width + 32, width), F32)),
        grid_spec=pltpu.PrefetchScalarGridSpec(
            num_scalar_prefetch=1, grid=(steps + 1,),
            in_specs=[flat, flat, strip, strip, strip, pl.BlockSpec((width, width), lambda i, m: (0, 0)), pl.BlockSpec((1, width), lambda i, m: (0, 0))],
            out_specs=(pl.BlockSpec((part, width), lambda i, m: (i, 0)), pl.BlockSpec((width + 32, width), lambda i, m: (0, 0))),
        ),
        compiler_params=pltpu.CompilerParams(dimension_semantics=("arbitrary",), vmem_limit_bytes=VMEM_LIMIT),
        cost_estimate=pl.CostEstimate(flops=4 * rows * width * width, bytes_accessed=rows * width * 18, transcendentals=0),
    )(core.reshape(1), mine, theirs, norm, slope, h, w_t, gamma)


def scatter_body(per, meta_ref, idx_ref, dh_ref, out_ref):
    step = pl.program_id(0)
    seq_len = out_ref.shape[1]
    spot = lax.broadcasted_iota(jnp.int32, (seq_len, WIN), 0).astype(F32)
    for i in range(per):
        hot = (spot == idx_ref[i]).astype(F32).astype(BF16)
        base = pl.multiple_of(meta_ref[step * per + i], 8)
        rows = dh_ref[pl.ds(base, WIN), :].astype(BF16)
        out_ref[i] = jnp.dot(hot, rows, preferred_element_type=F32).astype(BF16)


def scatter_pass(dh, idx_win, base, batch, seq_len):
    width = dh.shape[1]
    per = 4
    return pl.pallas_call(
        functools.partial(scatter_body, per),
        out_shape=jax.ShapeDtypeStruct((batch, seq_len, width), BF16),
        grid_spec=pltpu.PrefetchScalarGridSpec(
            num_scalar_prefetch=1, grid=(batch // per,),
            in_specs=[
                pl.BlockSpec((per, 1, WIN), lambda b, m: (b, 0, 0)),
                pl.BlockSpec(dh.shape, lambda b, m: (0, 0)),
            ],
            out_specs=pl.BlockSpec((per, seq_len, width), lambda b, m: (b, 0, 0)),
        ),
        compiler_params=pltpu.CompilerParams(dimension_semantics=("arbitrary",), vmem_limit_bytes=VMEM_LIMIT),
        cost_estimate=pl.CostEstimate(flops=2 * batch * WIN * seq_len * width, bytes_accessed=batch * seq_len * width * 2, transcendentals=0),
    )(base, idx_win, dh)


def clear_tail(e_ref, shard):
    steps = pl.cdiv(shard, VT)
    tail = shard - (steps - 1) * VT

    @pl.when(pl.program_id(0) == steps - 1)
    def _():
        e_ref[tail:] = jnp.zeros((VT - tail, e_ref.shape[1]), BF16)


def logits_body(shard, nb, target, e_ref, t_ref, bias_ref, lab_ref, z_ref, stat_ref):
    step = pl.program_id(0)

    @pl.when(step == 0)
    def _():
        stat_ref[0:1] = jnp.full((1, stat_ref.shape[1]), -jnp.inf, F32)
        stat_ref[1:3] = jnp.zeros((2, stat_ref.shape[1]), F32)

    clear_tail(e_ref, shard)
    bias = jnp.broadcast_to(bias_ref[...], (128, VT)).T
    bias = jnp.concatenate([bias] * (nb // 128), axis=1)
    vocab = lax.broadcasted_iota(jnp.int32, (VT, nb), 0)
    for i in range(z_ref.shape[1] // nb):
        cols = slice(i * nb, (i + 1) * nb)
        z = jnp.dot(e_ref[...], t_ref[:, cols], preferred_element_type=F32) + bias
        z_ref[:, cols] = z
        old = stat_ref[0:1, cols]
        new = jnp.maximum(old, jnp.max(z, axis=0, keepdims=True))
        stat_ref[1:2, cols] = stat_ref[1:2, cols] * jnp.exp(old - new) + jnp.sum(jnp.exp(z - new), axis=0, keepdims=True)
        if target:
            hot = vocab == lab_ref[:, cols] - step * VT
            stat_ref[2:3, cols] += jnp.sum(jnp.where(hot, z, 0.0), axis=0, keepdims=True)
        stat_ref[0:1, cols] = new


def logits_pass(embed, t_t, bias, lab, target):
    shard, width = embed.shape
    rows = t_t.shape[1]
    steps = pl.cdiv(shard, VT)
    whole = lambda j: (0, 0)
    return call(
        functools.partial(logits_body, shard, 512, target),
        (jax.ShapeDtypeStruct((steps * VT, rows), F32), jax.ShapeDtypeStruct((3, rows), F32)),
        (steps,),
        [
            pl.BlockSpec((VT, width), lambda j: (j, 0)),
            pl.BlockSpec((width, rows), whole),
            pl.BlockSpec((1, VT), lambda j: (0, j)),
            pl.BlockSpec((1, rows), whole),
        ],
        (pl.BlockSpec((VT, rows), lambda j: (j, 0)), pl.BlockSpec((3, rows), whole)),
        [],
        2 * rows * shard * width, rows * shard * 4 + shard * width * 2, rows * shard,
        (embed, t_t, bias, lab),
    )


def grad_logits(z, vec_ref, lab_ref, cols, vocab, step):
    soft = jnp.exp(z - vec_ref[0:1, cols]) * vec_ref[1:2, cols]
    hot = vocab == lab_ref[:, cols] - step * VT
    return jnp.where(hot, soft - vec_ref[2:3, cols], soft)


def lane_groups(dz):
    acc = dz[:, :128]
    for k in range(1, dz.shape[1] // 128):
        acc = acc + dz[:, k * 128:(k + 1) * 128]
    return acc


def hidden_body(shard, nb, core_ref, z_ref, vec_ref, lab_ref, e_ref, dz_ref, keep_ref, give_ref, db_ref, dt_s):
    step = pl.program_id(0)
    half = keep_ref.shape[0]

    @pl.when(step == 0)
    def _():
        dt_s[...] = jnp.zeros_like(dt_s)

    clear_tail(e_ref, shard)
    vocab = lax.broadcasted_iota(jnp.int32, (VT, nb), 0)
    acc = None
    for i in range(dz_ref.shape[1] // nb):
        cols = slice(i * nb, (i + 1) * nb)
        dz = grad_logits(z_ref[:, cols], vec_ref, lab_ref, cols, vocab, step)
        part = lane_groups(dz)
        acc = part if acc is None else acc + part
        dz = dz.astype(BF16)
        dz_ref[:, cols] = dz
        dt_s[:, cols] += lax.dot_general(e_ref[...], dz, (((0,), (0,)), ((), ())), preferred_element_type=F32)
    db_ref[...] = jnp.sum(acc.T, axis=0, keepdims=True)

    @pl.when(step == pl.num_programs(0) - 1)
    def _():
        core = core_ref[0]
        keep_ref[...] = dt_s[pl.ds(pl.multiple_of(core * half, 8), half), :]
        give_ref[...] = dt_s[pl.ds(pl.multiple_of((1 - core) * half, 8), half), :]


def hidden_pass(z, vec, lab, embed, core):
    shard, width = embed.shape
    padded, rows = z.shape
    whole = lambda j, m: (0, 0)
    tile = lambda n: pl.BlockSpec((VT, n), lambda j, m: (j, 0))
    flat = pl.BlockSpec((width // 2, rows), whole)
    return pl.pallas_call(
        functools.partial(hidden_body, shard, 512),
        out_shape=(
            jax.ShapeDtypeStruct((padded, rows), BF16),
            jax.ShapeDtypeStruct((width // 2, rows), F32), jax.ShapeDtypeStruct((width // 2, rows), F32),
            jax.ShapeDtypeStruct((1, padded), F32),
        ),
        grid_spec=pltpu.PrefetchScalarGridSpec(
            num_scalar_prefetch=1, grid=(padded // VT,),
            in_specs=[tile(rows), pl.BlockSpec((3, rows), whole), pl.BlockSpec((1, rows), whole), tile(width)],
            out_specs=(tile(rows), flat, flat, pl.BlockSpec((1, VT), lambda j, m: (0, j))),
            scratch_shapes=[pltpu.VMEM((width, rows), F32)],
        ),
        compiler_params=pltpu.CompilerParams(dimension_semantics=("arbitrary",), vmem_limit_bytes=VMEM_LIMIT),
        cost_estimate=pl.CostEstimate(flops=2 * rows * shard * width, bytes_accessed=rows * shard * 6, transcendentals=rows * shard),
    )(core.reshape(1), z, vec, lab, embed)


def embed_body(start, nb, dz_ref, z_ref, vec_ref, lab_ref, t_own_ref, t_oth_ref, db_own_ref, *refs):
    de_ref, db_ref, dz_s = refs[-3:]
    step = pl.program_id(0) + start
    vocab = lax.broadcasted_iota(jnp.int32, (VT, nb), 0)
    acc = None
    for i in range(z_ref.shape[1] // nb):
        cols = slice(i * nb, (i + 1) * nb)
        dz = grad_logits(z_ref[:, cols], vec_ref, lab_ref, cols, vocab, step)
        part = lane_groups(dz)
        acc = part if acc is None else acc + part
        dz_s[:, cols] = dz.astype(BF16)
    de_ref[...] = jnp.dot(dz_ref[...], t_own_ref[...], preferred_element_type=F32)
    de_ref[...] += jnp.dot(dz_s[...], t_oth_ref[...], preferred_element_type=F32)
    db_ref[...] = db_own_ref[...] + jnp.sum(acc.T, axis=0, keepdims=True)


def embed_pass(start, count, dz_own, z_oth, vec, lab, t_own, t_oth, db_own, shard, before):
    rows = z_oth.shape[1]
    width = t_own.shape[1]
    whole = lambda j: (0, 0)
    tile = pl.BlockSpec((VT, rows), lambda j: (j + start, 0))
    strip = pl.BlockSpec((1, VT), lambda j: (0, j + start))
    args = (dz_own, z_oth, vec, lab, t_own, t_oth, db_own) + (() if before is None else (before,))
    return pl.pallas_call(
        functools.partial(embed_body, start, 512),
        out_shape=(jax.ShapeDtypeStruct((shard, width), F32), jax.ShapeDtypeStruct((1, count * VT), F32)),
        grid_spec=pltpu.PrefetchScalarGridSpec(
            num_scalar_prefetch=0, grid=(count,),
            in_specs=[tile, tile, pl.BlockSpec((3, rows), whole), pl.BlockSpec((1, rows), whole), pl.BlockSpec((rows, width), whole), pl.BlockSpec((rows, width), whole), strip]
            + ([] if before is None else [pl.BlockSpec(memory_space=pl.ANY)]),
            out_specs=(pl.BlockSpec((VT, width), lambda j: (j + start, 0)), pl.BlockSpec((1, VT), lambda j: (0, j))),
            scratch_shapes=[pltpu.VMEM((VT, rows), BF16)],
        ),
        input_output_aliases={} if before is None else {7: 0},
        compiler_params=pltpu.CompilerParams(dimension_semantics=("arbitrary",), vmem_limit_bytes=VMEM_LIMIT),
        cost_estimate=pl.CostEstimate(flops=4 * rows * count * VT * width, bytes_accessed=rows * count * VT * 6 + count * VT * width * 4, transcendentals=rows * count * VT),
    )(*args)


def combine(stats):
    for swap in (swap_core, swap_x):
        other = swap(stats)
        best = jnp.maximum(stats[0], other[0])
        stats = jnp.stack([
            best,
            stats[1] * jnp.exp(stats[0] - best) + other[1] * jnp.exp(other[0] - best),
            stats[2] + other[2],
        ])
    return stats


def tie(*values):
    return lax.optimization_barrier(values)


def solution(mesh):
    def branch(rows, args):
        (tok_rows, hidden_shape, labels, w_t, b_t, gamma, beta, embed, out_bias, counts, offsets, base, idx_win, n_own, n_oth) = args
        batch, seq_len, width = hidden_shape
        max_pred = labels.shape[1]
        shard_vocab = embed.shape[0]
        tp = lax.axis_index("tp")
        core = tp % 2
        row = jnp.arange(rows, dtype=jnp.int32)
        in_seq = (row[:, None] >= offsets[None, :]) & (row[:, None] < (offsets + counts)[None, :])
        slot_row = jnp.where(row < n_own, row - jnp.sum(jnp.where(in_seq, offsets[None, :], 0), 1), -1)
        lab_seq = jnp.dot(in_seq.astype(F32), labels.astype(F32), precision=lax.Precision.HIGHEST)
        slot_hot = slot_row[:, None] == jnp.arange(max_pred, dtype=jnp.int32)[None, :]
        lab_own = jnp.sum(jnp.where(slot_hot, lab_seq, 0.0), 1).astype(jnp.int32)
        lab_oth = swap_dp(lab_own)

        def local_labels(lab):
            lab = lab - tp * shard_vocab
            return jnp.where((lab >= 0) & (lab < shard_vocab), lab, -1)[None, :]

        lab_own, lab_oth = local_labels(lab_own), local_labels(lab_oth)
        pad = -shard_vocab % VT
        bias = jnp.pad(out_bias, (0, pad), constant_values=-jnp.inf)[None, :]
        denom = (n_own + n_oth).astype(F32) + LOSS_EPS

        def vectors(stats, n):
            scale = (row < n).astype(F32) / denom
            return jnp.stack([stats[0], scale / stats[1], scale])

        vecs = jnp.stack([b_t, gamma, beta] + [jnp.zeros_like(b_t)] * 5)
        t_own, t_own_t, norm, slope, send = transform_pass(tok_rows, w_t, vecs, tp, rows)
        got = swap_dp(send)
        z_own, stat_own = logits_pass(embed, t_own_t, bias, lab_own, True)
        got, stat_own = tie(got, stat_own)
        got_x, got_core = swap_x(got), swap_core(got)
        stat_own = combine(stat_own)
        own_loss = jnp.sum(jnp.where(row < n_own, jnp.log(stat_own[1]) + stat_own[0] - stat_own[2], 0.0))
        oth_loss = swap_dp(jnp.full((8, 128), own_loss))
        loss = (own_loss + oth_loss[0, 0]) / denom
        dz_own, keep, give, db_own = hidden_pass(z_own, vectors(stat_own, n_own), lab_own, embed, core)
        got_x, keep = tie(got_x, keep)
        got_far = swap_core(got_x)
        given = swap_core(give)
        t_oth, t_oth_t = collect_pass((got, got_x, got_core, got_far), tp)
        given, t_oth_t = tie(given, t_oth_t)
        chip = keep + given
        chip, t_oth_t = tie(chip, t_oth_t)
        other = swap_x(chip)
        z_oth, stat_oth = logits_pass(embed, t_oth_t, bias, lab_oth, False)
        vec_oth = vectors(combine(stat_oth), n_oth)

        def embed_tiles(start, count, before):
            return embed_pass(start, count, dz_own, z_oth, vec_oth, lab_oth, t_own, t_oth, db_own, shard_vocab, before)

        cuts = (0, 3, 5, 10, (shard_vocab + pad) // VT)
        d_embed, db_0 = embed_tiles(cuts[0], cuts[1] - cuts[0], None)
        other, d_embed = tie(other, d_embed)
        mine = chip + other
        mine, d_embed = tie(mine, d_embed)
        theirs = swap_core(mine)
        d_embed, db_1 = embed_tiles(cuts[1], cuts[2] - cuts[1], d_embed)
        theirs, d_embed = tie(theirs, d_embed)
        d_rows, pack = back_pass(mine, theirs, norm, slope, tok_rows, w_t, gamma[None, :], core, rows)
        quarter = pack.shape[0] // 4
        pack = lax.dynamic_slice_in_dim(pack, tp * quarter, quarter)
        pack, d_embed = tie(pack, d_embed)
        far = swap_dp(pack)
        d_embed, db_2 = embed_tiles(cuts[2], cuts[3] - cuts[2], d_embed)
        far, d_embed = tie(far, d_embed)
        pack = pack + far
        pack, d_embed = tie(pack, d_embed)
        far = swap_x(pack)
        d_embed, db_3 = embed_tiles(cuts[3], cuts[4] - cuts[3], d_embed)
        far, d_rows, d_embed = tie(far, d_rows, d_embed)
        x = tp // 2
        pair = jnp.where(x == 0, jnp.stack([pack, far]), jnp.stack([far, pack]))
        pair, d_rows = tie(pair, d_rows)
        theirs = swap_core(pair)
        d_hidden = scatter_pass(d_rows, idx_win, base, batch, seq_len)
        theirs, d_hidden = tie(theirs, d_hidden)
        pack = jnp.where(core == 0, jnp.stack([pair, theirs], 1), jnp.stack([theirs, pair], 1)).reshape(4 * quarter, width)
        d_out_bias = jnp.concatenate([db_0, db_1, db_2, db_3], axis=1)[0, :shard_vocab]
        return loss, d_hidden, pack[:width], pack[width], pack[width + 1], pack[width + 2], d_embed, d_out_bias

    def local_step(hidden, positions, labels, weights, w_t, b_t, gamma, beta, embed, out_bias):
        batch, max_pred = positions.shape
        counts = jnp.sum(weights, axis=1).astype(jnp.int32)
        seq = jnp.arange(batch, dtype=jnp.int32)
        offsets = jnp.sum(jnp.where(seq[None, :] < seq[:, None], counts[None, :], 0), 1)
        n_own = jnp.sum(counts)
        n_oth = swap_dp(jnp.full((8, 128), n_own, jnp.int32))
        shift = offsets % 8
        base = offsets - shift
        live = jnp.where(jnp.arange(max_pred)[None, :] < counts[:, None], positions, -1).astype(F32)
        idx_win = jnp.full((batch, WIN), -1.0, F32)
        for k in range(8):
            moved = jnp.pad(live, ((0, 0), (k, WIN - max_pred - k)), constant_values=-1.0)
            idx_win = jnp.where((shift == k)[:, None], moved, idx_win)
        idx_win = idx_win[:, None, :]
        tok_rows = gather_pass(hidden, idx_win, base, batch * max_pred)
        n_oth, tok_rows = tie(n_oth, tok_rows)
        n_oth = n_oth[0, 0]
        n_max = jnp.maximum(n_own, n_oth)
        which = jnp.where(n_max > 2048, 0, jnp.where(n_max > 1536, 1, jnp.where(n_max > 1024, 3, 2)))
        args = (tok_rows, labels, w_t, b_t, gamma, beta, embed, out_bias, counts, offsets, base, idx_win, n_own, n_oth)
        return lax.switch(which, [lambda a, b=b: branch(b, a[:1] + (hidden.shape,) + a[1:]) for b in BUCKETS], args)

    in_specs = (P("dp", None, None), P("dp", None), P("dp", None), P("dp", None), P(None, None), P(None), P(None), P(None), P("tp", None), P("tp"))
    out_specs = (P(), P("dp", None, None), P(None, None), P(None), P(None), P(None), P("tp", None), P("tp"))
    return jax.shard_map(local_step, mesh=mesh, in_specs=in_specs, out_specs=out_specs, check_vma=False)
```

```python
import functools

import jax
import jax.numpy as jnp
from jax import lax
from jax.experimental import pallas as pl
from jax.experimental.pallas import tpu as pltpu
from jax.sharding import PartitionSpec as P

LN_EPS = 1e-12
LOSS_EPS = 1e-5
F32 = jnp.float32
BF16 = jnp.bfloat16
VT = 512
VB = 1536
VE = 512
COLS = 5
HEAD = 3
CB = 512
MAIN = 1536
ROWS = 128
SUB = 64
BACK = 256
PER = MAIN // 4 // ROWS
PER_X = 2
CUT = 1024
WIN = 128
VMEM_LIMIT = 60 * 1024 * 1024

SWAP_DP = tuple((i, i ^ 1) for i in range(2))
SWAP_CORE = tuple((i, i ^ 1) for i in range(4))
SWAP_X = tuple((i, i ^ 2) for i in range(4))
FIRST, SECOND, THIRD = (slice(i, i + 1) for i in range(3))


def whole(*shape):
    return pl.BlockSpec(shape, lambda *_: (0,) * len(shape))


def swap_dp(x):
    return lax.ppermute(x, "dp", SWAP_DP)


def swap_core(x):
    return lax.ppermute(x, "tp", SWAP_CORE)


def swap_x(x):
    return lax.ppermute(x, "tp", SWAP_X)


def gather_body(per, meta_ref, idx_ref, h_ref, out_ref, acc):
    step = pl.program_id(0)

    @pl.when(step == 0)
    def _():
        acc[...] = jnp.zeros_like(acc)

    seq_len = h_ref.shape[1]
    lane = lax.broadcasted_iota(jnp.int32, (WIN, seq_len), 1).astype(F32)
    for i in range(per):
        col = jnp.broadcast_to(idx_ref[i], (WIN, WIN)).T
        hot = jnp.concatenate([col] * (seq_len // WIN), axis=1) == lane
        rows = jnp.dot(hot.astype(F32).astype(BF16), h_ref[i], preferred_element_type=F32)
        base = pl.multiple_of(meta_ref[step * per + i], 8)
        acc[pl.ds(base, WIN), :] += rows

    @pl.when(step == pl.num_programs(0) - 1)
    def _():
        out_ref[...] = acc[: out_ref.shape[0], :].astype(BF16)


def gather_pass(hidden, idx_win, base, rows):
    batch, seq_len, width = hidden.shape
    per = 4
    return pl.pallas_call(
        functools.partial(gather_body, per),
        out_shape=jax.ShapeDtypeStruct((rows, width), BF16),
        grid_spec=pltpu.PrefetchScalarGridSpec(
            num_scalar_prefetch=1, grid=(batch // per,),
            in_specs=[
                pl.BlockSpec((per, 1, WIN), lambda b, m: (b, 0, 0)),
                pl.BlockSpec((per, seq_len, width), lambda b, m: (b, 0, 0)),
            ],
            out_specs=whole(rows, width),
            scratch_shapes=[pltpu.VMEM((rows + WIN, width), F32)],
        ),
        compiler_params=pltpu.CompilerParams(dimension_semantics=("arbitrary",), vmem_limit_bytes=VMEM_LIMIT),
        cost_estimate=pl.CostEstimate(flops=2 * batch * WIN * seq_len * width, bytes_accessed=batch * seq_len * width * 2, transcendentals=0),
    )(base, idx_win, hidden)


def transform_body(sub, meta_ref, h_ref, w_ref, vec_ref, t_ref, tt_ref, norm_ref, slope_ref, send_ref, send_x_ref, pre, t_s):
    step = pl.program_id(0)
    tp = meta_ref[0]

    @pl.when(step < meta_ref[1])
    def _():
        transform_block(sub, h_ref, w_ref, vec_ref, t_ref, tt_ref, norm_ref, slope_ref, pre, t_s)

    @pl.when((step >= PER * tp) & (step < PER * (tp + 1)))
    def _():
        send_ref[...] = t_s[...]

    @pl.when((step >= 4 * PER + PER_X * tp) & (step < 4 * PER + PER_X * (tp + 1)))
    def _():
        send_x_ref[...] = t_s[...]


def transform_block(sub, h_ref, w_ref, vec_ref, t_ref, tt_ref, norm_ref, slope_ref, pre, t_s):
    pre[...] = jnp.dot(h_ref[...], w_ref[...], preferred_element_type=F32) + vec_ref[FIRST]

    def some(i, _):
        at = pl.ds(pl.multiple_of(i * sub, sub), sub)
        u = pre[at, :]
        cdf = 0.5 * (1.0 + lax.erf(u * 0.7071067811865476))
        act = u * cdf
        mean = jnp.mean(act, axis=1, keepdims=True)
        cent = act - mean
        inv = lax.rsqrt(jnp.mean(cent * cent, axis=1, keepdims=True) + LN_EPS)
        norm = cent * inv
        norm_ref[at, :] = norm
        slope_ref[at, :] = (cdf + u * (0.3989422804014327 * jnp.exp(-0.5 * u * u))) * inv
        t_s[at, :] = norm * vec_ref[SECOND] + vec_ref[THIRD]
        return 0

    lax.fori_loop(0, ROWS // sub, some, 0)
    t = t_s[...].astype(BF16)
    t_ref[...] = t
    tt_ref[...] = t.T


def transform_pass(h, w_t, vecs, tp, blocks):
    total, width = h.shape
    strip = pl.BlockSpec((ROWS, width), lambda i, m: (jnp.minimum(i, m[1] - 1), 0))
    return pl.pallas_call(
        functools.partial(transform_body, SUB),
        out_shape=(
            jax.ShapeDtypeStruct((total, width), BF16), jax.ShapeDtypeStruct((width, total), BF16),
            jax.ShapeDtypeStruct((total, width), F32), jax.ShapeDtypeStruct((total, width), F32),
            jax.ShapeDtypeStruct((PER * ROWS, width), F32), jax.ShapeDtypeStruct((PER_X * ROWS, width), F32),
        ),
        grid_spec=pltpu.PrefetchScalarGridSpec(
            num_scalar_prefetch=1, grid=(total // ROWS,),
            in_specs=[strip, whole(width, width), whole(8, width)],
            out_specs=(
                strip, pl.BlockSpec((width, ROWS), lambda i, m: (0, jnp.minimum(i, m[1] - 1))), strip, strip,
                pl.BlockSpec((ROWS, width), lambda i, m: (jnp.clip(i - PER * m[0], 0, PER - 1), 0)),
                pl.BlockSpec((ROWS, width), lambda i, m: (jnp.clip(i - 4 * PER - PER_X * m[0], 0, PER_X - 1), 0)),
            ),
            scratch_shapes=[pltpu.VMEM((ROWS, width), F32), pltpu.VMEM((ROWS, width), F32)],
        ),
        compiler_params=pltpu.CompilerParams(dimension_semantics=("arbitrary",), vmem_limit_bytes=VMEM_LIMIT),
        cost_estimate=pl.CostEstimate(flops=2 * MAIN * width * width, bytes_accessed=MAIN * width * 14, transcendentals=2 * MAIN * width),
    )(jnp.stack([tp, blocks]), h, w_t, vecs)


def collect_body(source_ref, *refs):
    step = pl.program_id(0)
    active, source = step < source_ref[4 * PER + 4 * PER_X], source_ref[step]
    x_ref, t_ref, tt_ref = refs[4:]

    def put(rows):
        t = rows.astype(BF16)
        t_ref[...] = t
        tt_ref[...] = t.T

    for i, piece in enumerate(refs[:4]):
        @pl.when(active & (source >= i * PER) & (source < (i + 1) * PER))
        def _():
            put(piece[pl.ds(pl.multiple_of((source - i * PER) * ROWS, ROWS), ROWS), :])

    @pl.when(active & (source >= 4 * PER))
    def _():
        at = source - 4 * PER
        put(x_ref[lax.div(at, PER_X), pl.ds(pl.multiple_of(lax.rem(at, PER_X) * ROWS, ROWS), ROWS), :])


def collect_pass(pieces, extra, tp, total, blocks):
    part, width = pieces[0].shape
    piece = tp ^ jnp.arange(4, dtype=jnp.int32)
    piece = jnp.where((piece == 1) | (piece == 2), piece ^ 3, piece)[:, None]
    source = jnp.concatenate([
        (piece * PER + jnp.arange(PER, dtype=jnp.int32)).reshape(-1),
        (4 * PER + piece * PER_X + jnp.arange(PER_X, dtype=jnp.int32)).reshape(-1),
        blocks.reshape(1),
    ])
    at = lambda i, m: jnp.minimum(i, m[4 * PER + 4 * PER_X] - 1)
    return pl.pallas_call(
        collect_body,
        out_shape=(jax.ShapeDtypeStruct((total, width), BF16), jax.ShapeDtypeStruct((width, total), BF16)),
        grid_spec=pltpu.PrefetchScalarGridSpec(
            num_scalar_prefetch=1, grid=(total // ROWS,),
            in_specs=[whole(part, width)] * 4 + [whole(*extra.shape)],
            out_specs=(pl.BlockSpec((ROWS, width), lambda i, m: (at(i, m), 0)), pl.BlockSpec((width, ROWS), lambda i, m: (0, at(i, m)))),
        ),
        compiler_params=pltpu.CompilerParams(dimension_semantics=("arbitrary",), vmem_limit_bytes=VMEM_LIMIT),
        cost_estimate=pl.CostEstimate(flops=MAIN * width, bytes_accessed=MAIN * width * 8, transcendentals=0),
    )(source, *pieces, extra)


def back_body(meta_ref, mine_a_ref, theirs_a_ref, mine_b_ref, theirs_b_ref, extra_ref, norm_ref, slope_ref, h_ref, w_ref, gamma_ref, dh_ref, pack_ref):
    step = pl.program_id(0)
    last = meta_ref[1]
    width = w_ref.shape[0]

    @pl.when(step == 0)
    def _():
        pack_ref[...] = jnp.zeros_like(pack_ref)

    @pl.when(step < last)
    def _():
        low = meta_ref[0] == 0
        in_a, in_b = step < CUT // BACK, step < MAIN // BACK
        mine = jnp.where(in_a, mine_a_ref[...], jnp.where(in_b, mine_b_ref[...], extra_ref[0])).T
        theirs = jnp.where(in_a, theirs_a_ref[...], jnp.where(in_b, theirs_b_ref[...], extra_ref[1])).T
        d_t = jnp.concatenate([jnp.where(low, mine, theirs), jnp.where(low, theirs, mine)], axis=1)
        norm = norm_ref[...]
        pack_ref[width + 1:width + 2] += jnp.sum(d_t * norm, axis=0, keepdims=True)
        pack_ref[width + 2:width + 3] += jnp.sum(d_t, axis=0, keepdims=True)
        g = d_t * gamma_ref[...]
        g_mean = jnp.mean(g, axis=1, keepdims=True)
        gn_mean = jnp.mean(g * norm, axis=1, keepdims=True)
        d_u = (g - g_mean - norm * gn_mean) * slope_ref[...]
        pack_ref[width:width + 1] += jnp.sum(d_u, axis=0, keepdims=True)
        d_u = d_u.astype(BF16)
        pack_ref[:width] += lax.dot_general(h_ref[...], d_u, (((0,), (0,)), ((), ())), preferred_element_type=F32)
        d_h = lax.dot_general(d_u, w_ref[...], (((1,), (1,)), ((), ())), preferred_element_type=F32)
        dh_ref[...] = d_h.astype(BF16).astype(F32)

    @pl.when(step == last)
    def _():
        dh_ref[...] = jnp.zeros_like(dh_ref)


def back_pass(a, b, extra, norm, slope, h, w_t, gamma, core, blocks):
    total, width = norm.shape
    strip = pl.BlockSpec((BACK, width), lambda i, m: (jnp.minimum(i, m[1] - 1), 0))
    flat = lambda start, count: pl.BlockSpec((width // 2, BACK), lambda i, m: (0, jnp.clip(i - start, 0, count - 1)))
    at_a, at_b = flat(0, CUT // BACK), flat(CUT // BACK, (MAIN - CUT) // BACK)
    extra_blocks = extra.shape[2] // BACK
    return pl.pallas_call(
        back_body,
        out_shape=(jax.ShapeDtypeStruct((total + BACK, width), F32), jax.ShapeDtypeStruct((width + 32, width), F32)),
        grid_spec=pltpu.PrefetchScalarGridSpec(
            num_scalar_prefetch=1, grid=(total // BACK + 1,),
            in_specs=[
                at_a, at_a, at_b, at_b,
                pl.BlockSpec((2, width // 2, BACK), lambda i, m: (0, 0, jnp.clip(i - MAIN // BACK, 0, extra_blocks - 1))),
                strip, strip, strip, whole(width, width), whole(1, width),
            ],
            out_specs=(pl.BlockSpec((BACK, width), lambda i, m: (jnp.minimum(i, m[1]), 0)), whole(width + 32, width)),
        ),
        compiler_params=pltpu.CompilerParams(dimension_semantics=("arbitrary",), vmem_limit_bytes=VMEM_LIMIT),
        cost_estimate=pl.CostEstimate(flops=4 * MAIN * width * width, bytes_accessed=MAIN * width * 18, transcendentals=0),
    )(jnp.stack([core, blocks]), *a, *b, extra, norm, slope, h, w_t, gamma)


def scatter_body(per, meta_ref, idx_ref, dh_ref, out_ref):
    step = pl.program_id(0)
    seq_len = out_ref.shape[1]
    spot = lax.broadcasted_iota(jnp.int32, (seq_len, WIN), 0).astype(F32)
    for i in range(per):
        hot = (spot == idx_ref[i]).astype(F32).astype(BF16)
        base = pl.multiple_of(meta_ref[step * per + i], 8)
        rows = dh_ref[pl.ds(base, WIN), :].astype(BF16)
        out_ref[i] = jnp.dot(hot, rows, preferred_element_type=F32).astype(BF16)


def scatter_pass(dh, idx_win, base, batch, seq_len):
    width = dh.shape[1]
    per = 4
    return pl.pallas_call(
        functools.partial(scatter_body, per),
        out_shape=jax.ShapeDtypeStruct((batch, seq_len, width), BF16),
        grid_spec=pltpu.PrefetchScalarGridSpec(
            num_scalar_prefetch=1, grid=(batch // per,),
            in_specs=[
                pl.BlockSpec((per, 1, WIN), lambda b, m: (b, 0, 0)),
                whole(*dh.shape),
            ],
            out_specs=pl.BlockSpec((per, seq_len, width), lambda b, m: (b, 0, 0)),
        ),
        compiler_params=pltpu.CompilerParams(dimension_semantics=("arbitrary",), vmem_limit_bytes=VMEM_LIMIT),
        cost_estimate=pl.CostEstimate(flops=2 * batch * WIN * seq_len * width, bytes_accessed=batch * seq_len * width * 2, transcendentals=0),
    )(base, idx_win, dh)


def plan(steps, ncol, core):
    at = jnp.minimum(jnp.arange(steps * COLS, dtype=jnp.int32), steps * ncol - 1)
    return jnp.concatenate([jnp.stack([steps * ncol, ncol, core]), lax.div(at, ncol), lax.rem(at, ncol)])


def place(meta_ref, steps):
    at = pl.program_id(0)
    return at < meta_ref[0], meta_ref[HEAD + at], meta_ref[HEAD + steps * COLS + at], meta_ref[1]


def blocks_of(steps, start=0):
    row = lambda i, m: m[HEAD + i] + start
    col = lambda i, m: m[HEAD + steps * COLS + i]
    return (
        lambda *shape: pl.BlockSpec(shape, lambda i, m: (row(i, m), col(i, m))),
        lambda *shape: pl.BlockSpec(shape, lambda i, m: (row(i, m), 0)),
        lambda *shape: pl.BlockSpec(shape, lambda i, m: (0, col(i, m))),
    )


def clear_tail(e_ref, shard, step, at):
    tail = shard - shard // VB * VB

    @pl.when((step == shard // VB) & (at == 0))
    def _():
        e_ref[tail:] = jnp.zeros((VB - tail, e_ref.shape[1]), BF16)


def logits_body(shard, target, meta_ref, e_ref, t_ref, bias_ref, lab_ref, soft_ref, stat_ref, bias_s):
    active, step, at, _ = place(meta_ref, pl.cdiv(shard, VB))

    @pl.when(active & (at == 0))
    def _():
        bias_s[...] = jnp.broadcast_to(bias_ref[...], (128, VB)).T

    clear_tail(e_ref, shard, step, at)

    @pl.when(active)
    def _():
        vocab = lax.broadcasted_iota(jnp.int32, (VT, CB), 0)
        tops, tots, hits = [], [], []
        for k in range(VB // VT):
            rows = slice(k * VT, (k + 1) * VT)
            z = jnp.dot(e_ref[rows], t_ref[...], preferred_element_type=F32) + jnp.concatenate([bias_s[rows]] * (CB // 128), axis=1)
            top = jnp.max(z, axis=0, keepdims=True)
            soft = jnp.exp(z - top)
            soft_ref[rows] = soft
            tops.append(top)
            tots.append(jnp.sum(soft, axis=0, keepdims=True))
            if target:
                hot = vocab == lab_ref[...] - (step * VB + k * VT)
                hits.append(jnp.sum(jnp.where(hot, z, 0.0), axis=0, keepdims=True))
        hit = sum(hits[1:], hits[0]) if target else jnp.zeros_like(tops[0])
        stat_ref[...] = jnp.concatenate(tops + tots + [hit, hit], axis=0)


def params():
    return pltpu.CompilerParams(dimension_semantics=("arbitrary",), vmem_limit_bytes=VMEM_LIMIT)


def logits_pass(embed, t_t, bias, lab, target, meta):
    shard, width = embed.shape
    total = t_t.shape[1]
    steps = pl.cdiv(shard, VB)
    both, by_row, by_col = blocks_of(steps)
    return pl.pallas_call(
        functools.partial(logits_body, shard, target),
        out_shape=(jax.ShapeDtypeStruct((steps * VB, total), F32), jax.ShapeDtypeStruct((steps * 8, total), F32)),
        grid_spec=pltpu.PrefetchScalarGridSpec(
            num_scalar_prefetch=1, grid=(steps * COLS,),
            in_specs=[by_row(VB, width), by_col(width, CB), pl.BlockSpec((1, VB), lambda i, m: (0, m[HEAD + i])), by_col(1, CB)],
            out_specs=(both(VB, CB), both(8, CB)),
            scratch_shapes=[pltpu.VMEM((VB, 128), F32)],
        ),
        compiler_params=params(),
        cost_estimate=pl.CostEstimate(flops=2 * MAIN * shard * width, bytes_accessed=MAIN * shard * 4, transcendentals=MAIN * shard),
    )(meta, embed, t_t, bias, lab)


def grad_logits(soft, factor, scale, lab, vocab):
    soft = soft * factor
    return jnp.where(vocab == lab, soft - scale, soft)


def lane_groups(dz):
    acc = dz[:, :128]
    for k in range(1, dz.shape[1] // 128):
        acc = acc + dz[:, k * 128:(k + 1) * 128]
    return acc


def hidden_body(shard, meta_ref, soft_ref, vec_ref, lab_ref, e_ref, dz_ref, keep_ref, give_ref, extra_ref, db_ref, dt_s, acc_s):
    steps = pl.cdiv(shard, VB)
    active, step, at, ncol = place(meta_ref, steps)
    cols = pl.ds(pl.multiple_of(at * CB, CB), CB)
    half = keep_ref.shape[0]

    @pl.when(active & (step == 0))
    def _():
        dt_s[:, cols] = jnp.zeros((dt_s.shape[0], CB), F32)

    @pl.when(active & (at == 0))
    def _():
        acc_s[...] = jnp.zeros_like(acc_s)

    clear_tail(e_ref, shard, step, at)

    @pl.when(active)
    def _():
        vocab = lax.broadcasted_iota(jnp.int32, (VT, CB), 0)
        for k in range(VB // VT):
            rows = slice(k * VT, (k + 1) * VT)
            dz = grad_logits(soft_ref[rows], vec_ref[k:k + 1], vec_ref[-1:], lab_ref[...] - (step * VB + k * VT), vocab)
            acc_s[rows] += lane_groups(dz)
            dz_ref[rows] = dz.astype(BF16)
        dt_s[:, cols] += lax.dot_general(e_ref[...], dz_ref[...], (((0,), (0,)), ((), ())), preferred_element_type=F32)

    @pl.when(active & (at == ncol - 1))
    def _():
        db_ref[...] = jnp.sum(acc_s[...].T, axis=0, keepdims=True)

    @pl.when(pl.program_id(0) == steps * ncol - 1)
    def _():
        core = meta_ref[2]
        mine = pl.ds(pl.multiple_of(core * half, 8), half)
        yours = pl.ds(pl.multiple_of((1 - core) * half, 8), half)
        keep_ref[...] = dt_s[mine, :MAIN]
        give_ref[...] = dt_s[yours, :MAIN]

        @pl.when(ncol * CB > MAIN)
        def _():
            extra_ref[0] = dt_s[mine, MAIN:]
            extra_ref[1] = dt_s[yours, MAIN:]


def hidden_pass(soft, vec, lab, embed, meta):
    shard, width = embed.shape
    padded, total = soft.shape
    steps = padded // VB
    both, by_row, by_col = blocks_of(steps)
    flat = whole(width // 2, MAIN)
    return pl.pallas_call(
        functools.partial(hidden_body, shard),
        out_shape=(
            jax.ShapeDtypeStruct((padded, total), BF16),
            jax.ShapeDtypeStruct((width // 2, MAIN), F32), jax.ShapeDtypeStruct((width // 2, MAIN), F32),
            jax.ShapeDtypeStruct((2, width // 2, total - MAIN), F32),
            jax.ShapeDtypeStruct((1, padded), F32),
        ),
        grid_spec=pltpu.PrefetchScalarGridSpec(
            num_scalar_prefetch=1, grid=(steps * COLS,),
            in_specs=[both(VB, CB), both(8, CB), by_col(1, CB), by_row(VB, width)],
            out_specs=(both(VB, CB), flat, flat, whole(2, width // 2, total - MAIN), pl.BlockSpec((1, VB), lambda i, m: (0, m[HEAD + i]))),
            scratch_shapes=[pltpu.VMEM((width, total), F32), pltpu.VMEM((VB, 128), F32)],
        ),
        compiler_params=params(),
        cost_estimate=pl.CostEstimate(flops=2 * MAIN * shard * width, bytes_accessed=MAIN * shard * 6, transcendentals=0),
    )(meta, soft, vec, lab, embed)


def embed_body(start, count, meta_ref, dz_ref, soft_ref, vec_ref, lab_ref, t_own_ref, t_oth_ref, db_own_ref, *refs):
    de_ref, db_ref, dz_s, acc_s = refs[-4:]
    active, step, at, ncol = place(meta_ref, count)
    step = step + start

    @pl.when(active & (at == 0))
    def _():
        acc_s[...] = jnp.zeros_like(acc_s)

    @pl.when(active)
    def _():
        vocab = lax.broadcasted_iota(jnp.int32, (VE, CB), 0)
        dz = grad_logits(soft_ref[...], vec_ref[pl.ds(lax.rem(step, VB // VT), 1), :], vec_ref[-1:], lab_ref[...] - step * VE, vocab)
        acc_s[...] += lane_groups(dz)
        dz_s[...] = dz.astype(BF16)
        old = jnp.where(at == 0, 0.0, de_ref[...])
        de_ref[...] = old + jnp.dot(dz_ref[...], t_own_ref[...], preferred_element_type=F32)
        de_ref[...] += jnp.dot(dz_s[...], t_oth_ref[...], preferred_element_type=F32)

    @pl.when(active & (at == ncol - 1))
    def _():
        db_ref[...] = db_own_ref[...] + jnp.sum(acc_s[...].T, axis=0, keepdims=True)


def embed_pass(start, count, dz_own, soft_oth, vec, lab, t_own, t_oth, db_own, shard, before, meta):
    width = t_own.shape[1]
    both, by_row, by_col = blocks_of(count, start)
    feed = pl.BlockSpec((CB, width), lambda i, m: (m[HEAD + count * COLS + i], 0))
    stats = pl.BlockSpec((8, CB), lambda i, m: (lax.div(m[HEAD + i] + start, VB // VT), m[HEAD + count * COLS + i]))
    args = (meta, dz_own, soft_oth, vec, lab, t_own, t_oth, db_own) + (() if before is None else (before,))
    return pl.pallas_call(
        functools.partial(embed_body, start, count),
        out_shape=(jax.ShapeDtypeStruct((shard, width), F32), jax.ShapeDtypeStruct((1, count * VE), F32)),
        grid_spec=pltpu.PrefetchScalarGridSpec(
            num_scalar_prefetch=1, grid=(count * COLS,),
            in_specs=[both(VE, CB), both(VE, CB), stats, by_col(1, CB), feed, feed, pl.BlockSpec((1, VE), lambda i, m: (0, m[HEAD + i] + start))]
            + ([] if before is None else [pl.BlockSpec(memory_space=pl.ANY)]),
            out_specs=(by_row(VE, width), pl.BlockSpec((1, VE), lambda i, m: (0, m[HEAD + i]))),
            scratch_shapes=[pltpu.VMEM((VE, CB), BF16), pltpu.VMEM((VE, 128), F32)],
        ),
        input_output_aliases={} if before is None else {8: 0},
        compiler_params=params(),
        cost_estimate=pl.CostEstimate(flops=4 * MAIN * count * VE * width, bytes_accessed=MAIN * count * VE * 6 + count * VE * width * 4, transcendentals=0),
    )(*args)


def combine(stat):
    stat = stat.reshape(-1, 8, stat.shape[1])
    parts = VB // VT
    tops = stat[:, :parts]
    top = jnp.max(tops, axis=(0, 1))
    stats = jnp.stack([top, jnp.sum(stat[:, parts:2 * parts] * jnp.exp(tops - top), axis=(0, 1)), jnp.sum(stat[:, -1], axis=0)])
    for swap in (swap_core, swap_x):
        other = swap(stats)
        best = jnp.maximum(stats[0], other[0])
        stats = jnp.stack([
            best,
            stats[1] * jnp.exp(stats[0] - best) + other[1] * jnp.exp(other[0] - best),
            stats[2] + other[2],
        ])
    return stats, stat


def tie(*values):
    return lax.optimization_barrier(values)


def solution(mesh):
    def step(tok_rows, hidden_shape, labels, w_t, b_t, gamma, beta, embed, out_bias, counts, offsets, base, idx_win, n_own, n_oth):
        batch, seq_len, width = hidden_shape
        max_pred = labels.shape[1]
        shard_vocab = embed.shape[0]
        tp = lax.axis_index("tp")
        core = tp % 2
        rows = batch * max_pred
        n_max = jnp.maximum(n_own, n_oth)
        ncol = (n_max + CB - 1) // CB
        blocks = ncol * (CB // ROWS)
        many = n_max > MAIN
        row = jnp.arange(rows, dtype=jnp.int32)
        in_seq = (row[:, None] >= offsets[None, :]) & (row[:, None] < (offsets + counts)[None, :])
        slot_row = jnp.where(row < n_own, row - jnp.sum(jnp.where(in_seq, offsets[None, :], 0), 1), -1)
        lab_seq = jnp.dot(in_seq.astype(F32), labels.astype(F32), precision=lax.Precision.HIGHEST)
        slot_hot = slot_row[:, None] == jnp.arange(max_pred, dtype=jnp.int32)[None, :]
        lab_own = jnp.sum(jnp.where(slot_hot, lab_seq, 0.0), 1).astype(jnp.int32)
        lab_oth = swap_dp(lab_own)

        def local_labels(lab):
            lab = lab - tp * shard_vocab
            return jnp.where((lab >= 0) & (lab < shard_vocab), lab, -1)[None, :]

        lab_own, lab_oth = local_labels(lab_own), local_labels(lab_oth)
        pad = -shard_vocab % VB
        bias = jnp.pad(out_bias, (0, pad), constant_values=-jnp.inf)[None, :]
        denom = (n_own + n_oth).astype(F32) + LOSS_EPS

        def vectors(stats, stat, n):
            scale = (row < n).astype(F32) / denom
            part = jnp.arange(8, dtype=jnp.int32)[:, None] < VB // VT
            factor = jnp.exp(jnp.where(part, stat, 0.0) - stats[0]) * (scale / stats[1])
            return jnp.where(part, factor, scale).reshape(-1, rows)

        meta = plan(pl.cdiv(shard_vocab, VB), ncol, core)
        vecs = jnp.stack([b_t, gamma, beta] + [jnp.zeros_like(b_t)] * 5)
        t_own, t_own_t, norm, slope, send, send_x = transform_pass(tok_rows, w_t, vecs, tp, blocks)

        def fetch_rest(part):
            got = swap_dp(part)
            pair = jnp.stack([got, swap_x(got)])
            return jnp.concatenate([pair, swap_core(pair)])

        rest_t = lax.cond(many, fetch_rest, lambda part: jnp.zeros((4,) + part.shape, F32), send_x)
        send, rest_t = tie(send, rest_t)
        got = swap_dp(send)
        z_own, stat_own = logits_pass(embed, t_own_t, bias, lab_own, True, meta)
        got, stat_own = tie(got, stat_own)
        stat_own, tops_own = combine(stat_own)
        got_x, got_core = swap_x(got), swap_core(got)
        own_loss = jnp.sum(jnp.where(row < n_own, jnp.log(stat_own[1]) + stat_own[0] - stat_own[2], 0.0))
        oth_loss = swap_dp(jnp.full((8, 128), own_loss))
        dz_own, keep, give, rest_dt, db_own = hidden_pass(z_own, vectors(stat_own, tops_own, n_own), lab_own, embed, meta)
        got_x, got_core, oth_loss, keep = tie(got_x, got_core, oth_loss, keep)
        loss = (own_loss + oth_loss[0, 0]) / denom
        got_far = swap_core(got_x)
        given = swap_core(give)
        t_oth, t_oth_t = collect_pass((got, got_x, got_core, got_far), rest_t, tp, rows, blocks)

        def sum_rest(pair):
            chip = pair[0] + swap_core(pair[1])
            mine = chip + swap_x(chip)
            return jnp.stack([mine, swap_core(mine)])

        given, t_oth_t, rest_dt = tie(given, t_oth_t, rest_dt)
        rest_dt = lax.cond(many, sum_rest, lambda pair: pair, rest_dt)
        chip_a, chip_b = keep[:, :CUT] + given[:, :CUT], keep[:, CUT:] + given[:, CUT:]
        chip_a, chip_b, t_oth_t, rest_dt = tie(chip_a, chip_b, t_oth_t, rest_dt)
        other_a = swap_x(chip_a)
        z_oth, stat_oth = logits_pass(embed, t_oth_t, bias, lab_oth, False, meta)
        other_a, stat_oth = tie(other_a, stat_oth)
        stat_oth, tops_oth = combine(stat_oth)
        chip_b, stat_oth = tie(chip_b, stat_oth)
        other_b = swap_x(chip_b)
        mine_a = chip_a + other_a
        theirs_a = swap_core(mine_a)
        vec_oth = vectors(stat_oth, tops_oth, n_oth)

        def embed_tiles(start, count, before):
            return embed_pass(start, count, dz_own, z_oth, vec_oth, lab_oth, t_own, t_oth, db_own, shard_vocab, before, plan(count, ncol, core))

        d_embed, db_0 = embed_tiles(0, 5, None)
        other_b, theirs_a, d_embed = tie(other_b, theirs_a, d_embed)
        mine_b = chip_b + other_b
        theirs_b = swap_core(mine_b)
        d_rows, pack = back_pass((mine_a, theirs_a), (mine_b, theirs_b), rest_dt, norm, slope, tok_rows, w_t, gamma[None, :], core, ncol * (CB // BACK))
        quarter = pack.shape[0] // 4
        pack = lax.dynamic_slice_in_dim(pack, tp * quarter, quarter)
        pack, d_embed = tie(pack, d_embed)
        far = swap_dp(pack)
        d_embed, db_1 = embed_tiles(5, 5, d_embed)
        far, d_embed = tie(far, d_embed)
        pack = pack + far
        pack, d_embed = tie(pack, d_embed)
        far = swap_x(pack)
        d_embed, db_2 = embed_tiles(10, 5, d_embed)
        far, d_rows, d_embed = tie(far, d_rows, d_embed)
        x = tp // 2
        pair = jnp.where(x == 0, jnp.stack([pack, far]), jnp.stack([far, pack]))
        pair, d_rows = tie(pair, d_rows)
        theirs = swap_core(pair)
        d_hidden = scatter_pass(d_rows, idx_win, base, batch, seq_len)
        theirs, d_hidden = tie(theirs, d_hidden)
        pack = jnp.where(core == 0, jnp.stack([pair, theirs], 1), jnp.stack([theirs, pair], 1)).reshape(4 * quarter, width)
        d_out_bias = jnp.concatenate([db_0, db_1, db_2], axis=1)[0, :shard_vocab]
        return loss, d_hidden, pack[:width], pack[width], pack[width + 1], pack[width + 2], d_embed, d_out_bias

    def local_step(hidden, positions, labels, weights, w_t, b_t, gamma, beta, embed, out_bias):
        batch, max_pred = positions.shape
        counts = jnp.sum(weights, axis=1).astype(jnp.int32)
        seq = jnp.arange(batch, dtype=jnp.int32)
        offsets = jnp.sum(jnp.where(seq[None, :] < seq[:, None], counts[None, :], 0), 1)
        n_own = jnp.sum(counts)
        n_oth = swap_dp(jnp.full((8, 128), n_own, jnp.int32))
        shift = offsets % 8
        base = offsets - shift
        live = jnp.where(jnp.arange(max_pred)[None, :] < counts[:, None], positions, -1).astype(F32)
        idx_win = jnp.full((batch, WIN), -1.0, F32)
        for k in range(8):
            moved = jnp.pad(live, ((0, 0), (k, WIN - max_pred - k)), constant_values=-1.0)
            idx_win = jnp.where((shift == k)[:, None], moved, idx_win)
        idx_win = idx_win[:, None, :]
        tok_rows = gather_pass(hidden, idx_win, base, batch * max_pred)
        n_oth, tok_rows = tie(n_oth, tok_rows)
        n_oth = n_oth[0, 0]
        return step(tok_rows, hidden.shape, labels, w_t, b_t, gamma, beta, embed, out_bias, counts, offsets, base, idx_win, n_own, n_oth)

    in_specs = (P("dp", None, None), P("dp", None), P("dp", None), P("dp", None), P(None, None), P(None), P(None), P(None), P("tp", None), P("tp"))
    out_specs = (P(), P("dp", None, None), P(None, None), P(None), P(None), P(None), P("tp", None), P("tp"))
    return jax.shard_map(local_step, mesh=mesh, in_specs=in_specs, out_specs=out_specs, check_vma=False)
```

```python
import functools

import jax
import jax.numpy as jnp
from jax import lax
from jax.experimental import pallas as pl
from jax.experimental.pallas import tpu as pltpu
from jax.sharding import PartitionSpec as P

LN_EPS = 1e-12
LOSS_EPS = 1e-5
F32 = jnp.float32
BF16 = jnp.bfloat16
VT = 512
CB = 512
MAIN = 1536
CHUNKS = 2
CUT = 1024
SUB = 64
BACK = 256
WIN = 128
VMEM_LIMIT = 60 * 1024 * 1024

SWAP_DP = tuple((i, i ^ 1) for i in range(2))
SWAP_CORE = tuple((i, i ^ 1) for i in range(4))
SWAP_X = tuple((i, i ^ 2) for i in range(4))
FIRST, SECOND, THIRD = (slice(i, i + 1) for i in range(3))


def whole(*shape):
    return pl.BlockSpec(shape, lambda *_: (0,) * len(shape))


def swap_dp(x):
    return lax.ppermute(x, "dp", SWAP_DP)


def swap_core(x):
    return lax.ppermute(x, "tp", SWAP_CORE)


def swap_x(x):
    return lax.ppermute(x, "tp", SWAP_X)


def gather_body(per, meta_ref, idx_ref, h_ref, out_ref, acc):
    step = pl.program_id(0)

    @pl.when(step == 0)
    def _():
        acc[...] = jnp.zeros_like(acc)

    seq_len = h_ref.shape[1]
    lane = lax.broadcasted_iota(jnp.int32, (WIN, seq_len), 1).astype(F32)
    for i in range(per):
        col = jnp.broadcast_to(idx_ref[i], (WIN, WIN)).T
        hot = jnp.concatenate([col] * (seq_len // WIN), axis=1) == lane
        rows = jnp.dot(hot.astype(F32).astype(BF16), h_ref[i], preferred_element_type=F32)
        base = pl.multiple_of(meta_ref[step * per + i], 8)
        acc[pl.ds(base, WIN), :] += rows

    @pl.when(step == pl.num_programs(0) - 1)
    def _():
        out_ref[...] = acc[: out_ref.shape[0], :].astype(BF16)


def gather_pass(hidden, idx_win, base, rows):
    batch, seq_len, width = hidden.shape
    per = 4
    return pl.pallas_call(
        functools.partial(gather_body, per),
        out_shape=jax.ShapeDtypeStruct((rows, width), BF16),
        grid_spec=pltpu.PrefetchScalarGridSpec(
            num_scalar_prefetch=1, grid=(batch // per,),
            in_specs=[
                pl.BlockSpec((per, 1, WIN), lambda b, m: (b, 0, 0)),
                pl.BlockSpec((per, seq_len, width), lambda b, m: (b, 0, 0)),
            ],
            out_specs=whole(rows, width),
            scratch_shapes=[pltpu.VMEM((rows + WIN, width), F32)],
        ),
        compiler_params=pltpu.CompilerParams(dimension_semantics=("arbitrary",), vmem_limit_bytes=VMEM_LIMIT),
        cost_estimate=pl.CostEstimate(flops=2 * batch * WIN * seq_len * width, bytes_accessed=batch * seq_len * width * 2, transcendentals=0),
    )(base, idx_win, hidden)


def transform_body(meta_ref, h_ref, w_ref, vec_ref, t_ref, tt_ref, norm_ref, slope_ref, send_ref, pre, t_s):
    pre[...] = jnp.dot(h_ref[...], w_ref[...], preferred_element_type=F32) + vec_ref[FIRST]

    def some(i, _):
        at = pl.ds(pl.multiple_of(i * SUB, SUB), SUB)
        u = pre[at, :]
        cdf = 0.5 * (1.0 + lax.erf(u * 0.7071067811865476))
        act = u * cdf
        mean = jnp.mean(act, axis=1, keepdims=True)
        cent = act - mean
        inv = lax.rsqrt(jnp.mean(cent * cent, axis=1, keepdims=True) + LN_EPS)
        norm = cent * inv
        norm_ref[at, :] = norm
        slope_ref[at, :] = (cdf + u * (0.3989422804014327 * jnp.exp(-0.5 * u * u))) * inv
        t_s[at, :] = norm * vec_ref[SECOND] + vec_ref[THIRD]
        return 0

    lax.fori_loop(0, h_ref.shape[0] // SUB, some, 0)
    t = t_s[...].astype(BF16)
    t_ref[...] = t
    tt_ref[...] = t.T

    @pl.when(pl.program_id(0) == meta_ref[0])
    def _():
        send_ref[...] = t_s[...]


def transform_pass(h, w_t, vecs, tp, chunk):
    width = h.shape[1]
    part = MAIN // 4
    strip = pl.BlockSpec((part, width), lambda i, m: (i, 0))
    return pl.pallas_call(
        transform_body,
        out_shape=(
            jax.ShapeDtypeStruct((MAIN, width), BF16), jax.ShapeDtypeStruct((width, MAIN), BF16),
            jax.ShapeDtypeStruct((MAIN, width), F32), jax.ShapeDtypeStruct((MAIN, width), F32),
            jax.ShapeDtypeStruct((part, width), F32),
        ),
        grid_spec=pltpu.PrefetchScalarGridSpec(
            num_scalar_prefetch=1, grid=(4,),
            in_specs=[pl.BlockSpec((part, width), lambda i, m: (m[1] * 4 + i, 0)), whole(width, width), whole(8, width)],
            out_specs=(strip, pl.BlockSpec((width, part), lambda i, m: (0, i)), strip, strip, whole(part, width)),
            scratch_shapes=[pltpu.VMEM((part, width), F32), pltpu.VMEM((part, width), F32)],
        ),
        compiler_params=params(),
        cost_estimate=pl.CostEstimate(flops=2 * MAIN * width * width, bytes_accessed=MAIN * width * 14, transcendentals=2 * MAIN * width),
    )(jnp.stack([tp, chunk]), h, w_t, vecs)


def collect_body(place_ref, *refs):
    t_ref, tt_ref = refs[4:]
    for i, piece in enumerate(refs[:4]):
        @pl.when(pl.program_id(0) == i)
        def _():
            t = piece[...].astype(BF16)
            t_ref[...] = t
            tt_ref[...] = t.T


def collect_pass(pieces, tp):
    part, width = pieces[0].shape
    return pl.pallas_call(
        collect_body,
        out_shape=(jax.ShapeDtypeStruct((MAIN, width), BF16), jax.ShapeDtypeStruct((width, MAIN), BF16)),
        grid_spec=pltpu.PrefetchScalarGridSpec(
            num_scalar_prefetch=1, grid=(4,),
            in_specs=[whole(part, width)] * 4,
            out_specs=(pl.BlockSpec((part, width), lambda i, m: (m[i], 0)), pl.BlockSpec((width, part), lambda i, m: (0, m[i]))),
        ),
        compiler_params=params(),
        cost_estimate=pl.CostEstimate(flops=MAIN * width, bytes_accessed=MAIN * width * 8, transcendentals=0),
    )(tp ^ jnp.array([0, 2, 1, 3], jnp.int32), *pieces)


def back_body(meta_ref, mine_a_ref, theirs_a_ref, mine_b_ref, theirs_b_ref, norm_ref, slope_ref, h_ref, w_ref, gamma_ref, old_ref, dh_ref, pack_ref):
    step = pl.program_id(0)
    last = pl.num_programs(0) - 1
    width = w_ref.shape[0]

    @pl.when(step == 0)
    def _():
        pack_ref[...] = jnp.zeros_like(pack_ref)

    @pl.when(step < last)
    def _():
        low = meta_ref[0] == 0
        in_a = step < CUT // BACK
        mine = jnp.where(in_a, mine_a_ref[...], mine_b_ref[...]).T
        theirs = jnp.where(in_a, theirs_a_ref[...], theirs_b_ref[...]).T
        d_t = jnp.concatenate([jnp.where(low, mine, theirs), jnp.where(low, theirs, mine)], axis=1)
        norm = norm_ref[...]
        d_gamma = jnp.sum(d_t * norm, axis=0, keepdims=True)
        d_beta = jnp.sum(d_t, axis=0, keepdims=True)
        g = d_t * gamma_ref[...]
        g_mean = jnp.mean(g, axis=1, keepdims=True)
        gn_mean = jnp.mean(g * norm, axis=1, keepdims=True)
        d_u = (g - g_mean - norm * gn_mean) * slope_ref[...]
        d_b = jnp.sum(d_u, axis=0, keepdims=True)
        pack_ref[width:width + 8] += jnp.concatenate([d_b, d_gamma, d_beta] + [jnp.zeros_like(d_b)] * 5)
        d_u = d_u.astype(BF16)
        pack_ref[:width] += lax.dot_general(h_ref[...], d_u, (((0,), (0,)), ((), ())), preferred_element_type=F32)
        d_h = lax.dot_general(d_u, w_ref[...], (((1,), (1,)), ((), ())), preferred_element_type=F32)
        dh_ref[...] = d_h.astype(BF16).astype(F32)

    @pl.when(step == last)
    def _():
        dh_ref[...] = jnp.zeros_like(dh_ref)


def back_pass(a, b, norm, slope, h, w_t, gamma, core, chunk, old):
    width = norm.shape[1]
    steps = MAIN // BACK
    strip = pl.BlockSpec((BACK, width), lambda i, m: (jnp.minimum(i, steps - 1), 0))
    flat = lambda start, count: pl.BlockSpec((width // 2, BACK), lambda i, m: (0, jnp.clip(i - start, 0, count - 1)))
    at_a, at_b = flat(0, CUT // BACK), flat(CUT // BACK, (MAIN - CUT) // BACK)
    return pl.pallas_call(
        back_body,
        out_shape=(jax.ShapeDtypeStruct(old.shape, F32), jax.ShapeDtypeStruct((width + 32, width), F32)),
        grid_spec=pltpu.PrefetchScalarGridSpec(
            num_scalar_prefetch=1, grid=(steps + 1,),
            in_specs=[
                at_a, at_a, at_b, at_b, strip, strip,
                pl.BlockSpec((BACK, width), lambda i, m: (m[1] * steps + jnp.minimum(i, steps - 1), 0)),
                whole(width, width), whole(1, width), pl.BlockSpec(memory_space=pl.ANY),
            ],
            out_specs=(pl.BlockSpec((BACK, width), lambda i, m: (m[1] * steps + i, 0)), whole(width + 32, width)),
        ),
        input_output_aliases={10: 0},
        compiler_params=params(),
        cost_estimate=pl.CostEstimate(flops=4 * MAIN * width * width, bytes_accessed=MAIN * width * 18, transcendentals=0),
    )(jnp.stack([core, chunk]), *a, *b, norm, slope, h, w_t, gamma, old)


def scatter_body(per, meta_ref, idx_ref, dh_ref, out_ref):
    step = pl.program_id(0)
    seq_len = out_ref.shape[1]
    spot = lax.broadcasted_iota(jnp.int32, (seq_len, WIN), 0).astype(F32)
    for i in range(per):
        hot = (spot == idx_ref[i]).astype(F32).astype(BF16)
        base = pl.multiple_of(meta_ref[step * per + i], 8)
        rows = dh_ref[pl.ds(base, WIN), :].astype(BF16)
        out_ref[i] = jnp.dot(hot, rows, preferred_element_type=F32).astype(BF16)


def scatter_pass(dh, idx_win, base, batch, seq_len):
    width = dh.shape[1]
    per = 4
    return pl.pallas_call(
        functools.partial(scatter_body, per),
        out_shape=jax.ShapeDtypeStruct((batch, seq_len, width), BF16),
        grid_spec=pltpu.PrefetchScalarGridSpec(
            num_scalar_prefetch=1, grid=(batch // per,),
            in_specs=[
                pl.BlockSpec((per, 1, WIN), lambda b, m: (b, 0, 0)),
                whole(*dh.shape),
            ],
            out_specs=pl.BlockSpec((per, seq_len, width), lambda b, m: (b, 0, 0)),
        ),
        compiler_params=pltpu.CompilerParams(dimension_semantics=("arbitrary",), vmem_limit_bytes=VMEM_LIMIT),
        cost_estimate=pl.CostEstimate(flops=2 * batch * WIN * seq_len * width, bytes_accessed=batch * seq_len * width * 2, transcendentals=0),
    )(base, idx_win, dh)


def params():
    return pltpu.CompilerParams(dimension_semantics=("arbitrary",), vmem_limit_bytes=VMEM_LIMIT)


def scratch_array(*shape):
    return pl.pallas_call(
        lambda out_ref: None, out_shape=jax.ShapeDtypeStruct(shape, F32), out_specs=pl.BlockSpec(memory_space=pl.ANY)
    )()


def by_tile(rows, cols, start=0):
    return pl.BlockSpec((rows, cols), lambda j, *_: (j + start, 0))


def strip_of(start=0):
    return pl.BlockSpec((1, VT), lambda j, *_: (0, j + start))


def clear_tail(e_ref, shard):
    tail = shard % VT

    @pl.when(pl.program_id(0) == shard // VT)
    def _():
        e_ref[tail:] = jnp.zeros((VT - tail, e_ref.shape[1]), BF16)


def columns():
    return [slice(i, i + CB) for i in range(0, MAIN, CB)]


def logits_body(shard, target, e_ref, t_ref, bias_ref, lab_ref, soft_ref, stat_ref):
    clear_tail(e_ref, shard)
    bias = jnp.broadcast_to(bias_ref[...], (128, VT)).T
    bias = jnp.concatenate([bias] * (CB // 128), axis=1)
    vocab = lax.broadcasted_iota(jnp.int32, (VT, CB), 0)
    for cols in columns():
        z = jnp.dot(e_ref[...], t_ref[:, cols], preferred_element_type=F32) + bias
        top = jnp.max(z, axis=0, keepdims=True)
        soft = jnp.exp(z - top)
        soft_ref[:, cols] = soft
        stat_ref[FIRST, cols] = top
        stat_ref[SECOND, cols] = jnp.sum(soft, axis=0, keepdims=True)
        if target:
            hot = vocab == lab_ref[:, cols] - pl.program_id(0) * VT
            stat_ref[THIRD, cols] = jnp.sum(jnp.where(hot, z, 0.0), axis=0, keepdims=True)


def logits_pass(embed, t_t, bias, lab, target):
    shard, width = embed.shape
    steps = pl.cdiv(shard, VT)
    return pl.pallas_call(
        functools.partial(logits_body, shard, target),
        out_shape=(jax.ShapeDtypeStruct((steps * VT, MAIN), F32), jax.ShapeDtypeStruct((steps * 8, MAIN), F32)),
        grid_spec=pltpu.PrefetchScalarGridSpec(
            num_scalar_prefetch=0, grid=(steps,),
            in_specs=[by_tile(VT, width), whole(width, MAIN), strip_of(), whole(1, MAIN)],
            out_specs=(by_tile(VT, MAIN), by_tile(8, MAIN)),
        ),
        compiler_params=params(),
        cost_estimate=pl.CostEstimate(flops=2 * MAIN * shard * width, bytes_accessed=MAIN * shard * 4, transcendentals=MAIN * shard),
    )(embed, t_t, bias, lab)


def grad_logits(soft_ref, vec_ref, lab_ref, cols, vocab, step):
    soft = soft_ref[:, cols] * vec_ref[FIRST, cols]
    return jnp.where(vocab == lab_ref[:, cols] - step * VT, soft - vec_ref[SECOND, cols], soft)


def lane_groups(dz):
    acc = dz[:, :128]
    for k in range(128, CB, 128):
        acc = acc + dz[:, k:k + 128]
    return acc


def hidden_body(shard, core_ref, soft_ref, vec_ref, lab_ref, e_ref, dz_ref, keep_ref, give_ref, db_ref, dt_s):
    step = pl.program_id(0)
    half = keep_ref.shape[0]

    @pl.when(step == 0)
    def _():
        dt_s[...] = jnp.zeros_like(dt_s)

    clear_tail(e_ref, shard)
    vocab = lax.broadcasted_iota(jnp.int32, (VT, CB), 0)
    acc = []
    for cols in columns():
        dz = grad_logits(soft_ref, vec_ref, lab_ref, cols, vocab, step)
        acc.append(lane_groups(dz))
        dz = dz.astype(BF16)
        dz_ref[:, cols] = dz
        dt_s[:, cols] += lax.dot_general(e_ref[...], dz, (((0,), (0,)), ((), ())), preferred_element_type=F32)
    db_ref[...] = jnp.sum(sum(acc[1:], acc[0]).T, axis=0, keepdims=True)

    @pl.when(step == pl.num_programs(0) - 1)
    def _():
        core = core_ref[0]
        keep_ref[...] = dt_s[pl.ds(pl.multiple_of(core * half, 8), half), :]
        give_ref[...] = dt_s[pl.ds(pl.multiple_of((1 - core) * half, 8), half), :]


def hidden_pass(soft, vec, lab, embed, core):
    shard, width = embed.shape
    padded = soft.shape[0]
    flat = whole(width // 2, MAIN)
    return pl.pallas_call(
        functools.partial(hidden_body, shard),
        out_shape=(
            jax.ShapeDtypeStruct((padded, MAIN), BF16),
            jax.ShapeDtypeStruct((width // 2, MAIN), F32), jax.ShapeDtypeStruct((width // 2, MAIN), F32),
            jax.ShapeDtypeStruct((1, padded), F32),
        ),
        grid_spec=pltpu.PrefetchScalarGridSpec(
            num_scalar_prefetch=1, grid=(padded // VT,),
            in_specs=[by_tile(VT, MAIN), by_tile(8, MAIN), whole(1, MAIN), by_tile(VT, width)],
            out_specs=(by_tile(VT, MAIN), flat, flat, strip_of()),
            scratch_shapes=[pltpu.VMEM((width, MAIN), F32)],
        ),
        compiler_params=params(),
        cost_estimate=pl.CostEstimate(flops=2 * MAIN * shard * width, bytes_accessed=MAIN * shard * 6, transcendentals=0),
    )(core.reshape(1), soft, vec, lab, embed)


def embed_body(start, meta_ref, dz_ref, soft_ref, vec_ref, lab_ref, t_own_ref, t_oth_ref, db_own_ref, old_ref, de_ref, db_ref, dz_s):
    step = pl.program_id(0) + start
    vocab = lax.broadcasted_iota(jnp.int32, (VT, CB), 0)
    acc = []
    for cols in columns():
        dz = grad_logits(soft_ref, vec_ref, lab_ref, cols, vocab, step)
        acc.append(lane_groups(dz))
        dz_s[:, cols] = dz.astype(BF16)
    old = jnp.where(meta_ref[0] == 0, 0.0, old_ref[...])
    de_ref[...] = old + jnp.dot(dz_ref[...], t_own_ref[...], preferred_element_type=F32)
    de_ref[...] += jnp.dot(dz_s[...], t_oth_ref[...], preferred_element_type=F32)
    db_ref[...] = db_own_ref[...] + jnp.sum(sum(acc[1:], acc[0]).T, axis=0, keepdims=True)


def embed_pass(start, count, dz_own, soft_oth, vec, lab, t_own, t_oth, db_own, old, chunk):
    shard, width = old.shape
    return pl.pallas_call(
        functools.partial(embed_body, start),
        out_shape=(jax.ShapeDtypeStruct((shard, width), F32), jax.ShapeDtypeStruct((1, count * VT), F32)),
        grid_spec=pltpu.PrefetchScalarGridSpec(
            num_scalar_prefetch=1, grid=(count,),
            in_specs=[
                by_tile(VT, MAIN, start), by_tile(VT, MAIN, start), by_tile(8, MAIN, start), whole(1, MAIN),
                whole(MAIN, width), whole(MAIN, width), strip_of(start), by_tile(VT, width, start),
            ],
            out_specs=(by_tile(VT, width, start), strip_of()),
            scratch_shapes=[pltpu.VMEM((VT, MAIN), BF16)],
        ),
        input_output_aliases={8: 0},
        compiler_params=params(),
        cost_estimate=pl.CostEstimate(flops=4 * MAIN * count * VT * width, bytes_accessed=MAIN * count * VT * 6 + count * VT * width * 4, transcendentals=0),
    )(chunk.reshape(1), dz_own, soft_oth, vec, lab, t_own, t_oth, db_own, old)


def combine(stat):
    top, tot, hit = (stat.reshape(-1, 8, MAIN)[:, i] for i in range(3))
    best = jnp.max(top, axis=0)
    stats = jnp.stack([best, jnp.sum(tot * jnp.exp(top - best), axis=0), jnp.sum(hit, axis=0)])
    for swap in (swap_core, swap_x):
        other = swap(stats)
        best = jnp.maximum(stats[0], other[0])
        stats = jnp.stack([
            best,
            stats[1] * jnp.exp(stats[0] - best) + other[1] * jnp.exp(other[0] - best),
            stats[2] + other[2],
        ])
    return stats, top


def tie(*values):
    return lax.optimization_barrier(values)


def solution(mesh):
    def local_step(hidden, positions, labels, weights, w_t, b_t, gamma, beta, embed, out_bias):
        batch, seq_len, width = hidden.shape
        max_pred = positions.shape[1]
        shard_vocab = embed.shape[0]
        tiles = pl.cdiv(shard_vocab, VT)
        tp = lax.axis_index("tp")
        core = tp % 2
        counts = jnp.sum(weights, axis=1).astype(jnp.int32)
        seq = jnp.arange(batch, dtype=jnp.int32)
        offsets = jnp.sum(jnp.where(seq[None, :] < seq[:, None], counts[None, :], 0), 1)
        n_own = jnp.sum(counts)
        n_oth = swap_dp(jnp.full((8, 128), n_own, jnp.int32))
        shift = offsets % 8
        base = offsets - shift
        live = jnp.where(jnp.arange(max_pred)[None, :] < counts[:, None], positions, -1).astype(F32)
        idx_win = jnp.full((batch, WIN), -1.0, F32)
        for k in range(8):
            moved = jnp.pad(live, ((0, 0), (k, WIN - max_pred - k)), constant_values=-1.0)
            idx_win = jnp.where((shift == k)[:, None], moved, idx_win)
        idx_win = idx_win[:, None, :]
        tok_rows = gather_pass(hidden, idx_win, base, CHUNKS * MAIN)
        n_oth, tok_rows = tie(n_oth, tok_rows)
        n_oth = n_oth[0, 0]
        trips = jnp.where(jnp.maximum(n_own, n_oth) > MAIN, CHUNKS, 1)
        denom = (n_own + n_oth).astype(F32) + LOSS_EPS
        bias = jnp.pad(out_bias, (0, tiles * VT - shard_vocab), constant_values=-jnp.inf)[None, :]
        vecs = jnp.stack([b_t, gamma, beta] + [jnp.zeros_like(b_t)] * 5)

        def local_labels(lab):
            lab = lab - tp * shard_vocab
            return jnp.where((lab >= 0) & (lab < shard_vocab), lab, -1)[None, :]

        def trip(carry):
            chunk, d_embed, d_rows, pack_sum, bias_sum, loss_sum = carry
            row = chunk * MAIN + jnp.arange(MAIN, dtype=jnp.int32)
            in_seq = (row[:, None] >= offsets[None, :]) & (row[:, None] < (offsets + counts)[None, :])
            slot_row = jnp.where(row < n_own, row - jnp.sum(jnp.where(in_seq, offsets[None, :], 0), 1), -1)
            lab_seq = jnp.dot(in_seq.astype(F32), labels.astype(F32), precision=lax.Precision.HIGHEST)
            slot_hot = slot_row[:, None] == jnp.arange(max_pred, dtype=jnp.int32)[None, :]
            lab_own = jnp.sum(jnp.where(slot_hot, lab_seq, 0.0), 1).astype(jnp.int32)
            lab_oth = swap_dp(lab_own)

            def vectors(stats, tops, n):
                scale = (row < n).astype(F32) / denom
                factor = jnp.exp(tops - stats[0]) * (scale / stats[1])
                first = jnp.arange(8, dtype=jnp.int32)[:, None] == 0
                return jnp.where(first, factor[:, None], scale).reshape(-1, MAIN)

            t_own, t_own_t, norm, slope, send = transform_pass(tok_rows, w_t, vecs, tp, chunk)
            got = swap_dp(send)
            soft_own, stat_own = logits_pass(embed, t_own_t, bias, local_labels(lab_own), True)
            got, stat_own, lab_oth = tie(got, stat_own, lab_oth)
            stat_own, tops_own = combine(stat_own)
            got_x, got_core = swap_x(got), swap_core(got)
            loss_sum = loss_sum + jnp.sum(jnp.where(row < n_own, jnp.log(stat_own[1]) + stat_own[0] - stat_own[2], 0.0))
            dz_own, keep, give, db_own = hidden_pass(soft_own, vectors(stat_own, tops_own, n_own), local_labels(lab_own), embed, core)
            got_x, got_core, keep = tie(got_x, got_core, keep)
            got_far = swap_core(got_x)
            given = swap_core(give)
            t_oth, t_oth_t = collect_pass((got, got_x, got_core, got_far), tp)
            given, t_oth_t = tie(given, t_oth_t)
            chip_a, chip_b = keep[:, :CUT] + given[:, :CUT], keep[:, CUT:] + given[:, CUT:]
            chip_a, chip_b, t_oth_t = tie(chip_a, chip_b, t_oth_t)
            other_a = swap_x(chip_a)
            soft_oth, stat_oth = logits_pass(embed, t_oth_t, bias, local_labels(lab_oth), False)
            other_a, stat_oth = tie(other_a, stat_oth)
            stat_oth, tops_oth = combine(stat_oth)
            chip_b, stat_oth = tie(chip_b, stat_oth)
            other_b = swap_x(chip_b)
            mine_a = chip_a + other_a
            theirs_a = swap_core(mine_a)
            vec_oth = vectors(stat_oth, tops_oth, n_oth)

            def embed_tiles(start, count, old):
                return embed_pass(start, count, dz_own, soft_oth, vec_oth, local_labels(lab_oth), t_own, t_oth, db_own, old, chunk)

            d_embed, db_0 = embed_tiles(0, 7, d_embed)
            other_b, theirs_a, d_embed = tie(other_b, theirs_a, d_embed)
            mine_b = chip_b + other_b
            theirs_b = swap_core(mine_b)
            d_rows, pack = back_pass((mine_a, theirs_a), (mine_b, theirs_b), norm, slope, tok_rows, w_t, gamma[None, :], core, chunk, d_rows)
            quarter = pack.shape[0] // 4
            pack = lax.dynamic_slice_in_dim(pack, tp * quarter, quarter)
            pack, d_embed = tie(pack, d_embed)
            far = swap_dp(pack)
            d_embed, db_1 = embed_tiles(7, tiles - 7, d_embed)
            far, d_embed = tie(far, d_embed)
            bias_sum = bias_sum + jnp.concatenate([db_0, db_1], axis=1)
            return chunk + 1, d_embed, d_rows, pack_sum + (pack + far), bias_sum, loss_sum

        start = (
            jnp.int32(0), scratch_array(shard_vocab, width), scratch_array(CHUNKS * MAIN + BACK, width),
            jnp.zeros(((width + 32) // 4, width), F32), jnp.zeros((1, tiles * VT), F32), jnp.zeros((), F32),
        )
        _, d_embed, d_rows, pack, d_out_bias, loss = lax.while_loop(lambda carry: carry[0] < trips, trip, start)
        far = swap_x(pack)
        loss_oth = swap_dp(jnp.full((8, 128), loss))
        d_hidden = scatter_pass(d_rows, idx_win, base, batch, seq_len)
        far, loss_oth, d_hidden = tie(far, loss_oth, d_hidden)
        pair = jnp.where(tp // 2 == 0, jnp.stack([pack, far]), jnp.stack([far, pack]))
        theirs = swap_core(pair)
        pack = jnp.where(core == 0, jnp.stack([pair, theirs], 1), jnp.stack([theirs, pair], 1)).reshape(-1, width)
        loss = (loss + loss_oth[0, 0]) / denom
        return loss, d_hidden, pack[:width], pack[width], pack[width + 1], pack[width + 2], d_embed, d_out_bias[0, :shard_vocab]

    in_specs = (P("dp", None, None), P("dp", None), P("dp", None), P("dp", None), P(None, None), P(None), P(None), P(None), P("tp", None), P("tp"))
    out_specs = (P(), P("dp", None, None), P(None, None), P(None), P(None), P(None), P("tp", None), P("tp"))
    return jax.shard_map(local_step, mesh=mesh, in_specs=in_specs, out_specs=out_specs, check_vma=False)
```

```python
import functools

import jax
import jax.numpy as jnp
from jax import lax
from jax.experimental import pallas as pl
from jax.experimental.pallas import tpu as pltpu
from jax.sharding import PartitionSpec as P


LN_EPS = 1e-12
LOSS_EPS = 1e-5
F32 = jnp.float32
BF16 = jnp.bfloat16
VT = 512
CB = 512
MAIN = 1536
CHUNKS = 2
CUT = 1024
SUB = 64
BACK = 256
WIN = 128
VMEM_LIMIT = 60 * 1024 * 1024

SWAP_DP = tuple((i, i ^ 1) for i in range(2))
SWAP_CORE = tuple((i, i ^ 1) for i in range(4))
SWAP_X = tuple((i, i ^ 2) for i in range(4))
FIRST, SECOND, THIRD = (slice(i, i + 1) for i in range(3))


def whole(*shape):
    return pl.BlockSpec(shape, lambda *_: (0,) * len(shape))


def swap_dp(x):
    return lax.ppermute(x, "dp", SWAP_DP)


def swap_core(x):
    return lax.ppermute(x, "tp", SWAP_CORE)


def swap_x(x):
    return lax.ppermute(x, "tp", SWAP_X)


def gather_body(per, meta_ref, idx_ref, h_ref, out_ref, acc):
    step = pl.program_id(0)

    @pl.when(step == 0)
    def _():
        acc[...] = jnp.zeros_like(acc)

    seq_len = h_ref.shape[1]
    lane = lax.broadcasted_iota(jnp.int32, (WIN, seq_len), 1).astype(F32)
    for i in range(per):
        col = jnp.broadcast_to(idx_ref[i], (WIN, WIN)).T
        hot = jnp.concatenate([col] * (seq_len // WIN), axis=1) == lane
        rows = jnp.dot(hot.astype(F32).astype(BF16), h_ref[i], preferred_element_type=F32)
        base = pl.multiple_of(meta_ref[step * per + i], 8)
        acc[pl.ds(base, WIN), :] += rows

    @pl.when(step == pl.num_programs(0) - 1)
    def _():
        out_ref[...] = acc[: out_ref.shape[0], :].astype(BF16)


def gather_pass(hidden, idx_win, base, rows):
    batch, seq_len, width = hidden.shape
    per = 4
    return pl.pallas_call(
        functools.partial(gather_body, per),
        out_shape=jax.ShapeDtypeStruct((rows, width), BF16),
        grid_spec=pltpu.PrefetchScalarGridSpec(
            num_scalar_prefetch=1, grid=(batch // per,),
            in_specs=[
                pl.BlockSpec((per, 1, WIN), lambda b, m: (b, 0, 0)),
                pl.BlockSpec((per, seq_len, width), lambda b, m: (b, 0, 0)),
            ],
            out_specs=whole(rows, width),
            scratch_shapes=[pltpu.VMEM((rows + WIN, width), F32)],
        ),
        compiler_params=pltpu.CompilerParams(dimension_semantics=("arbitrary",), vmem_limit_bytes=VMEM_LIMIT),
        cost_estimate=pl.CostEstimate(flops=2 * batch * WIN * seq_len * width, bytes_accessed=batch * seq_len * width * 2, transcendentals=0),
    )(base, idx_win, hidden)


def transform_body(meta_ref, h_ref, w_ref, vec_ref, t_ref, tt_ref, norm_ref, slope_ref, send_ref, pre, t_s):
    pre[...] = jnp.dot(h_ref[...], w_ref[...], preferred_element_type=F32) + vec_ref[FIRST]

    def some(i, _):
        at = pl.ds(pl.multiple_of(i * SUB, SUB), SUB)
        u = pre[at, :]
        cdf = 0.5 * (1.0 + lax.erf(u * 0.7071067811865476))
        act = u * cdf
        mean = jnp.mean(act, axis=1, keepdims=True)
        cent = act - mean
        inv = lax.rsqrt(jnp.mean(cent * cent, axis=1, keepdims=True) + LN_EPS)
        norm = cent * inv
        norm_ref[at, :] = norm
        slope_ref[at, :] = (cdf + u * (0.3989422804014327 * jnp.exp(-0.5 * u * u))) * inv
        t_s[at, :] = norm * vec_ref[SECOND] + vec_ref[THIRD]
        return 0

    lax.fori_loop(0, h_ref.shape[0] // SUB, some, 0)
    t = t_s[...].astype(BF16)
    t_ref[...] = t
    tt_ref[...] = t.T

    @pl.when(pl.program_id(0) == meta_ref[0])
    def _():
        send_ref[...] = t_s[...]


def transform_pass(h, w_t, vecs, tp, chunk):
    width = h.shape[1]
    part = MAIN // 4
    strip = pl.BlockSpec((part, width), lambda i, m: (i, 0))
    return pl.pallas_call(
        transform_body,
        out_shape=(
            jax.ShapeDtypeStruct((MAIN, width), BF16), jax.ShapeDtypeStruct((width, MAIN), BF16),
            jax.ShapeDtypeStruct((MAIN, width), F32), jax.ShapeDtypeStruct((MAIN, width), F32),
            jax.ShapeDtypeStruct((part, width), F32),
        ),
        grid_spec=pltpu.PrefetchScalarGridSpec(
            num_scalar_prefetch=1, grid=(4,),
            in_specs=[pl.BlockSpec((part, width), lambda i, m: (m[1] * 4 + i, 0)), whole(width, width), whole(8, width)],
            out_specs=(strip, pl.BlockSpec((width, part), lambda i, m: (0, i)), strip, strip, whole(part, width)),
            scratch_shapes=[pltpu.VMEM((part, width), F32), pltpu.VMEM((part, width), F32)],
        ),
        compiler_params=params(),
        cost_estimate=pl.CostEstimate(flops=2 * MAIN * width * width, bytes_accessed=MAIN * width * 14, transcendentals=2 * MAIN * width),
    )(jnp.stack([tp, chunk]), h, w_t, vecs)


def collect_body(place_ref, *refs):
    t_ref, tt_ref = refs[4:]
    for i, piece in enumerate(refs[:4]):
        @pl.when(pl.program_id(0) == i)
        def _():
            t = piece[...].astype(BF16)
            t_ref[...] = t
            tt_ref[...] = t.T


def collect_pass(pieces, tp):
    part, width = pieces[0].shape
    return pl.pallas_call(
        collect_body,
        out_shape=(jax.ShapeDtypeStruct((MAIN, width), BF16), jax.ShapeDtypeStruct((width, MAIN), BF16)),
        grid_spec=pltpu.PrefetchScalarGridSpec(
            num_scalar_prefetch=1, grid=(4,),
            in_specs=[whole(part, width)] * 4,
            out_specs=(pl.BlockSpec((part, width), lambda i, m: (m[i], 0)), pl.BlockSpec((width, part), lambda i, m: (0, m[i]))),
        ),
        compiler_params=params(),
        cost_estimate=pl.CostEstimate(flops=MAIN * width, bytes_accessed=MAIN * width * 8, transcendentals=0),
    )(tp ^ jnp.array([0, 2, 1, 3], jnp.int32), *pieces)


def back_body(meta_ref, mine_a_ref, theirs_a_ref, mine_b_ref, theirs_b_ref, norm_ref, slope_ref, h_ref, w_ref, gamma_ref, old_ref, dh_ref, pack_ref):
    step = pl.program_id(0)
    last = pl.num_programs(0) - 1
    width = w_ref.shape[0]

    @pl.when(step == 0)
    def _():
        pack_ref[...] = jnp.zeros_like(pack_ref)

    @pl.when(step < last)
    def _():
        low = meta_ref[0] == 0
        in_a = step < CUT // BACK
        mine = jnp.where(in_a, mine_a_ref[...], mine_b_ref[...]).T
        theirs = jnp.where(in_a, theirs_a_ref[...], theirs_b_ref[...]).T
        d_t = jnp.concatenate([jnp.where(low, mine, theirs), jnp.where(low, theirs, mine)], axis=1)
        norm = norm_ref[...]
        d_gamma = jnp.sum(d_t * norm, axis=0, keepdims=True)
        d_beta = jnp.sum(d_t, axis=0, keepdims=True)
        g = d_t * gamma_ref[...]
        g_mean = jnp.mean(g, axis=1, keepdims=True)
        gn_mean = jnp.mean(g * norm, axis=1, keepdims=True)
        d_u = (g - g_mean - norm * gn_mean) * slope_ref[...]
        d_b = jnp.sum(d_u, axis=0, keepdims=True)
        pack_ref[width:width + 8] += jnp.concatenate([d_b, d_gamma, d_beta] + [jnp.zeros_like(d_b)] * 5)
        d_u = d_u.astype(BF16)
        pack_ref[:width] += lax.dot_general(h_ref[...], d_u, (((0,), (0,)), ((), ())), preferred_element_type=F32)
        d_h = lax.dot_general(d_u, w_ref[...], (((1,), (1,)), ((), ())), preferred_element_type=F32)
        dh_ref[...] = d_h.astype(BF16).astype(F32)

    @pl.when(step == last)
    def _():
        dh_ref[...] = jnp.zeros_like(dh_ref)


def back_pass(a, b, norm, slope, h, w_t, gamma, core, chunk, old):
    width = norm.shape[1]
    steps = MAIN // BACK
    strip = pl.BlockSpec((BACK, width), lambda i, m: (jnp.minimum(i, steps - 1), 0))
    flat = lambda start, count: pl.BlockSpec((width // 2, BACK), lambda i, m: (0, jnp.clip(i - start, 0, count - 1)))
    at_a, at_b = flat(0, CUT // BACK), flat(CUT // BACK, (MAIN - CUT) // BACK)
    return pl.pallas_call(
        back_body,
        out_shape=(jax.ShapeDtypeStruct(old.shape, F32), jax.ShapeDtypeStruct((width + 32, width), F32)),
        grid_spec=pltpu.PrefetchScalarGridSpec(
            num_scalar_prefetch=1, grid=(steps + 1,),
            in_specs=[
                at_a, at_a, at_b, at_b, strip, strip,
                pl.BlockSpec((BACK, width), lambda i, m: (m[1] * steps + jnp.minimum(i, steps - 1), 0)),
                whole(width, width), whole(1, width), pl.BlockSpec(memory_space=pl.ANY),
            ],
            out_specs=(pl.BlockSpec((BACK, width), lambda i, m: (m[1] * steps + i, 0)), whole(width + 32, width)),
        ),
        input_output_aliases={10: 0},
        compiler_params=params(),
        cost_estimate=pl.CostEstimate(flops=4 * MAIN * width * width, bytes_accessed=MAIN * width * 18, transcendentals=0),
    )(jnp.stack([core, chunk]), *a, *b, norm, slope, h, w_t, gamma, old)


def scatter_body(per, meta_ref, idx_ref, dh_ref, out_ref):
    step = pl.program_id(0)
    seq_len = out_ref.shape[1]
    spot = lax.broadcasted_iota(jnp.int32, (seq_len, WIN), 0).astype(F32)
    for i in range(per):
        hot = (spot == idx_ref[i]).astype(F32).astype(BF16)
        at = pl.multiple_of((meta_ref[step * per + i] - meta_ref[step * per]) * 8, 8)
        rows = dh_ref[pl.ds(at, WIN), :].astype(BF16)
        out_ref[i] = jnp.dot(hot, rows, preferred_element_type=F32).astype(BF16)


def scatter_pass(dh, idx_win, base, batch, seq_len, max_pred):
    width = dh.shape[1]
    per = 4
    span = (per - 1) * max_pred + WIN
    return pl.pallas_call(
        functools.partial(scatter_body, per),
        out_shape=jax.ShapeDtypeStruct((batch, seq_len, width), BF16),
        grid_spec=pltpu.PrefetchScalarGridSpec(
            num_scalar_prefetch=1, grid=(batch // per,),
            in_specs=[
                pl.BlockSpec((per, 1, WIN), lambda b, m: (b, 0, 0)),
                pl.BlockSpec((pl.Element(span), pl.Element(width)), lambda b, m: (m[b * per] * 8, 0)),
            ],
            out_specs=pl.BlockSpec((per, seq_len, width), lambda b, m: (b, 0, 0)),
        ),
        compiler_params=pltpu.CompilerParams(dimension_semantics=("arbitrary",), vmem_limit_bytes=VMEM_LIMIT),
        cost_estimate=pl.CostEstimate(flops=2 * batch * WIN * seq_len * width, bytes_accessed=batch * seq_len * width * 2, transcendentals=0),
    )(lax.div(base, 8), idx_win, dh)


def params():
    return pltpu.CompilerParams(dimension_semantics=("arbitrary",), vmem_limit_bytes=VMEM_LIMIT)


def scratch_array(*shape):
    return pl.pallas_call(
        lambda out_ref: None, out_shape=jax.ShapeDtypeStruct(shape, F32), out_specs=pl.BlockSpec(memory_space=pl.ANY)
    )()


def by_tile(rows, cols, start=0):
    return pl.BlockSpec((rows, cols), lambda j, *_: (j + start, 0))


def strip_of(start=0):
    return pl.BlockSpec((1, VT), lambda j, *_: (0, j + start))


def clear_tail(e_ref, shard):
    tail = shard % VT

    @pl.when(pl.program_id(0) == shard // VT)
    def _():
        e_ref[tail:] = jnp.zeros((VT - tail, e_ref.shape[1]), BF16)


def columns():
    return [slice(i, i + CB) for i in range(0, MAIN, CB)]


def logits_body(shard, target, e_ref, t_ref, bias_ref, lab_ref, soft_ref, stat_ref):
    clear_tail(e_ref, shard)
    bias = jnp.broadcast_to(bias_ref[...], (128, VT)).T
    bias = jnp.concatenate([bias] * (CB // 128), axis=1)
    vocab = lax.broadcasted_iota(jnp.int32, (VT, CB), 0)
    for cols in columns():
        z = jnp.dot(e_ref[...], t_ref[:, cols], preferred_element_type=F32) + bias
        top = jnp.max(z, axis=0, keepdims=True)
        soft = jnp.exp(z - top)
        soft_ref[:, cols] = soft
        stat_ref[FIRST, cols] = top
        stat_ref[SECOND, cols] = jnp.sum(soft, axis=0, keepdims=True)
        if target:
            hot = vocab == lab_ref[:, cols] - pl.program_id(0) * VT
            stat_ref[THIRD, cols] = jnp.sum(jnp.where(hot, z, 0.0), axis=0, keepdims=True)


def logits_pass(embed, t_t, bias, lab, target):
    shard, width = embed.shape
    steps = pl.cdiv(shard, VT)
    return pl.pallas_call(
        functools.partial(logits_body, shard, target),
        out_shape=(jax.ShapeDtypeStruct((steps * VT, MAIN), F32), jax.ShapeDtypeStruct((steps * 8, MAIN), F32)),
        grid_spec=pltpu.PrefetchScalarGridSpec(
            num_scalar_prefetch=0, grid=(steps,),
            in_specs=[by_tile(VT, width), whole(width, MAIN), strip_of(), whole(1, MAIN)],
            out_specs=(by_tile(VT, MAIN), by_tile(8, MAIN)),
        ),
        compiler_params=params(),
        cost_estimate=pl.CostEstimate(flops=2 * MAIN * shard * width, bytes_accessed=MAIN * shard * 4, transcendentals=MAIN * shard),
    )(embed, t_t, bias, lab)


def grad_logits(soft_ref, vec_ref, lab_ref, cols, vocab, step):
    soft = soft_ref[:, cols] * vec_ref[FIRST, cols]
    return jnp.where(vocab == lab_ref[:, cols] - step * VT, soft - vec_ref[SECOND, cols], soft)


def lane_groups(dz):
    acc = dz[:, :128]
    for k in range(128, CB, 128):
        acc = acc + dz[:, k:k + 128]
    return acc


def hidden_body(shard, core_ref, soft_ref, vec_ref, lab_ref, e_ref, dz_ref, keep_ref, give_ref, db_ref, dt_s):
    step = pl.program_id(0)
    half = keep_ref.shape[0]

    @pl.when(step == 0)
    def _():
        dt_s[...] = jnp.zeros_like(dt_s)

    clear_tail(e_ref, shard)
    vocab = lax.broadcasted_iota(jnp.int32, (VT, CB), 0)
    acc = []
    for cols in columns():
        dz = grad_logits(soft_ref, vec_ref, lab_ref, cols, vocab, step)
        acc.append(lane_groups(dz))
        dz_ref[:, cols] = dz.astype(BF16)
    dt_s[...] += lax.dot_general(e_ref[...], dz_ref[...], (((0,), (0,)), ((), ())), preferred_element_type=F32)
    db_ref[...] = jnp.sum(sum(acc[1:], acc[0]).T, axis=0, keepdims=True)

    @pl.when(step == pl.num_programs(0) - 1)
    def _():
        core = core_ref[0]
        keep_ref[...] = dt_s[pl.ds(pl.multiple_of(core * half, 8), half), :]
        give_ref[...] = dt_s[pl.ds(pl.multiple_of((1 - core) * half, 8), half), :]


def hidden_pass(soft, vec, lab, embed, core):
    shard, width = embed.shape
    padded = soft.shape[0]
    flat = whole(width // 2, MAIN)
    return pl.pallas_call(
        functools.partial(hidden_body, shard),
        out_shape=(
            jax.ShapeDtypeStruct((padded, MAIN), BF16),
            jax.ShapeDtypeStruct((width // 2, MAIN), F32), jax.ShapeDtypeStruct((width // 2, MAIN), F32),
            jax.ShapeDtypeStruct((1, padded), F32),
        ),
        grid_spec=pltpu.PrefetchScalarGridSpec(
            num_scalar_prefetch=1, grid=(padded // VT,),
            in_specs=[by_tile(VT, MAIN), by_tile(8, MAIN), whole(1, MAIN), by_tile(VT, width)],
            out_specs=(by_tile(VT, MAIN), flat, flat, strip_of()),
            scratch_shapes=[pltpu.VMEM((width, MAIN), F32)],
        ),
        compiler_params=params(),
        cost_estimate=pl.CostEstimate(flops=2 * MAIN * shard * width, bytes_accessed=MAIN * shard * 6, transcendentals=0),
    )(core.reshape(1), soft, vec, lab, embed)


def embed_body(start, meta_ref, dz_ref, soft_ref, vec_ref, lab_ref, t_own_ref, t_oth_ref, db_own_ref, old_ref, de_ref, db_ref, dz_s):
    step = pl.program_id(0) + start
    vocab = lax.broadcasted_iota(jnp.int32, (VT, CB), 0)
    acc = []
    for cols in columns():
        dz = grad_logits(soft_ref, vec_ref, lab_ref, cols, vocab, step)
        acc.append(lane_groups(dz))
        dz_s[:, cols] = dz.astype(BF16)
    old = jnp.where(meta_ref[0] == 0, 0.0, old_ref[...])
    de_ref[...] = old + jnp.dot(dz_ref[...], t_own_ref[...], preferred_element_type=F32)
    de_ref[...] += jnp.dot(dz_s[...], t_oth_ref[...], preferred_element_type=F32)
    db_ref[...] = db_own_ref[...] + jnp.sum(sum(acc[1:], acc[0]).T, axis=0, keepdims=True)


def embed_pass(start, count, dz_own, soft_oth, vec, lab, t_own, t_oth, db_own, old, chunk):
    shard, width = old.shape
    return pl.pallas_call(
        functools.partial(embed_body, start),
        out_shape=(jax.ShapeDtypeStruct((shard, width), F32), jax.ShapeDtypeStruct((1, count * VT), F32)),
        grid_spec=pltpu.PrefetchScalarGridSpec(
            num_scalar_prefetch=1, grid=(count,),
            in_specs=[
                by_tile(VT, MAIN, start), by_tile(VT, MAIN, start), by_tile(8, MAIN, start), whole(1, MAIN),
                whole(MAIN, width), whole(MAIN, width), strip_of(start), by_tile(VT, width, start),
            ],
            out_specs=(by_tile(VT, width, start), strip_of()),
            scratch_shapes=[pltpu.VMEM((VT, MAIN), BF16)],
        ),
        input_output_aliases={8: 0},
        compiler_params=params(),
        cost_estimate=pl.CostEstimate(flops=4 * MAIN * count * VT * width, bytes_accessed=MAIN * count * VT * 6 + count * VT * width * 4, transcendentals=0),
    )(chunk.reshape(1), dz_own, soft_oth, vec, lab, t_own, t_oth, db_own, old)


def combine(stat):
    top, tot, hit = (stat.reshape(-1, 8, MAIN)[:, i] for i in range(3))
    best = jnp.max(top, axis=0)
    stats = jnp.stack([best, jnp.sum(tot * jnp.exp(top - best), axis=0), jnp.sum(hit, axis=0)])
    for swap in (swap_core, swap_x):
        other = swap(stats)
        best = jnp.maximum(stats[0], other[0])
        stats = jnp.stack([
            best,
            stats[1] * jnp.exp(stats[0] - best) + other[1] * jnp.exp(other[0] - best),
            stats[2] + other[2],
        ])
    return stats, top


def tie(*values):
    return lax.optimization_barrier(values)


def solution(mesh):
    def local_step(hidden, positions, labels, weights, w_t, b_t, gamma, beta, embed, out_bias):
        batch, seq_len, width = hidden.shape
        max_pred = positions.shape[1]
        shard_vocab = embed.shape[0]
        tiles = pl.cdiv(shard_vocab, VT)
        tp = lax.axis_index("tp")
        core = tp % 2
        counts = jnp.sum(weights, axis=1).astype(jnp.int32)
        seq = jnp.arange(batch, dtype=jnp.int32)
        offsets = jnp.sum(jnp.where(seq[None, :] < seq[:, None], counts[None, :], 0), 1)
        n_own = jnp.sum(counts)
        n_oth = swap_dp(jnp.full((8, 128), n_own, jnp.int32))
        shift = offsets % 8
        base = offsets - shift
        live = jnp.where(jnp.arange(max_pred)[None, :] < counts[:, None], positions, -1).astype(F32)
        idx_win = jnp.full((batch, WIN), -1.0, F32)
        for k in range(8):
            moved = jnp.pad(live, ((0, 0), (k, WIN - max_pred - k)), constant_values=-1.0)
            idx_win = jnp.where((shift == k)[:, None], moved, idx_win)
        idx_win = idx_win[:, None, :]
        tok_rows = gather_pass(hidden, idx_win, base, CHUNKS * MAIN)
        n_oth, tok_rows = tie(n_oth, tok_rows)
        n_oth = n_oth[0, 0]
        trips = jnp.where(jnp.maximum(n_own, n_oth) > MAIN, CHUNKS, 1)
        denom = (n_own + n_oth).astype(F32) + LOSS_EPS
        bias = jnp.pad(out_bias, (0, tiles * VT - shard_vocab), constant_values=-jnp.inf)[None, :]
        vecs = jnp.stack([b_t, gamma, beta] + [jnp.zeros_like(b_t)] * 5)

        def local_labels(lab):
            lab = lab - tp * shard_vocab
            return jnp.where((lab >= 0) & (lab < shard_vocab), lab, -1)[None, :]

        def trip(carry):
            chunk, d_embed, d_rows, pack_sum, bias_sum, loss_sum = carry
            row = chunk * MAIN + jnp.arange(MAIN, dtype=jnp.int32)
            in_seq = (row[:, None] >= offsets[None, :]) & (row[:, None] < (offsets + counts)[None, :])
            slot_row = jnp.where(row < n_own, row - jnp.sum(jnp.where(in_seq, offsets[None, :], 0), 1), -1)
            lab_seq = jnp.dot(in_seq.astype(F32), labels.astype(F32), precision=lax.Precision.HIGHEST)
            slot_hot = slot_row[:, None] == jnp.arange(max_pred, dtype=jnp.int32)[None, :]
            lab_own = jnp.sum(jnp.where(slot_hot, lab_seq, 0.0), 1).astype(jnp.int32)
            lab_oth = swap_dp(lab_own)

            def vectors(stats, tops, n):
                scale = (row < n).astype(F32) / denom
                factor = jnp.exp(tops - stats[0]) * (scale / stats[1])
                first = jnp.arange(8, dtype=jnp.int32)[:, None] == 0
                return jnp.where(first, factor[:, None], scale).reshape(-1, MAIN)

            t_own, t_own_t, norm, slope, send = transform_pass(tok_rows, w_t, vecs, tp, chunk)
            got = swap_dp(send)
            soft_own, stat_own = logits_pass(embed, t_own_t, bias, local_labels(lab_own), True)
            got, stat_own, lab_oth = tie(got, stat_own, lab_oth)
            stat_own, tops_own = combine(stat_own)
            got_x, got_core = swap_x(got), swap_core(got)
            loss_sum = loss_sum + jnp.sum(jnp.where(row < n_own, jnp.log(stat_own[1]) + stat_own[0] - stat_own[2], 0.0))
            dz_own, keep, give, db_own = hidden_pass(soft_own, vectors(stat_own, tops_own, n_own), local_labels(lab_own), embed, core)
            got_x, got_core, keep = tie(got_x, got_core, keep)
            got_far, give = tie(swap_core(got_x), give)
            given = swap_core(give)
            t_oth, t_oth_t = collect_pass((got, got_x, got_core, got_far), tp)
            given, t_oth_t = tie(given, t_oth_t)
            chip_a, chip_b = keep[:, :CUT] + given[:, :CUT], keep[:, CUT:] + given[:, CUT:]
            chip_a, chip_b, t_oth_t = tie(chip_a, chip_b, t_oth_t)
            other_a = swap_x(chip_a)
            soft_oth, stat_oth = logits_pass(embed, t_oth_t, bias, local_labels(lab_oth), False)
            other_a, stat_oth = tie(other_a, stat_oth)
            stat_oth, tops_oth = combine(stat_oth)
            chip_b, stat_oth = tie(chip_b, stat_oth)
            other_b = swap_x(chip_b)
            mine_a = chip_a + other_a
            theirs_a = swap_core(mine_a)
            vec_oth = vectors(stat_oth, tops_oth, n_oth)

            def embed_tiles(start, count, old):
                return embed_pass(start, count, dz_own, soft_oth, vec_oth, local_labels(lab_oth), t_own, t_oth, db_own, old, chunk)

            d_embed, db_0 = embed_tiles(0, 7, d_embed)
            other_b, theirs_a, d_embed = tie(other_b, theirs_a, d_embed)
            mine_b = chip_b + other_b
            theirs_b = swap_core(mine_b)
            d_rows, pack = back_pass((mine_a, theirs_a), (mine_b, theirs_b), norm, slope, tok_rows, w_t, gamma[None, :], core, chunk, d_rows)
            quarter = pack.shape[0] // 4
            pack = lax.dynamic_slice_in_dim(pack, tp * quarter, quarter)
            pack, d_embed = tie(pack, d_embed)
            far = swap_dp(pack)
            d_embed, db_1 = embed_tiles(7, tiles - 7, d_embed)
            far, d_embed = tie(far, d_embed)
            bias_sum = bias_sum + jnp.concatenate([db_0, db_1], axis=1)
            return chunk + 1, d_embed, d_rows, pack_sum + (pack + far), bias_sum, loss_sum

        start = (
            jnp.int32(0), scratch_array(shard_vocab, width), scratch_array(CHUNKS * MAIN + BACK, width),
            jnp.zeros(((width + 32) // 4, width), F32), jnp.zeros((1, tiles * VT), F32), jnp.zeros((), F32),
        )
        _, d_embed, d_rows, pack, d_out_bias, loss = lax.while_loop(lambda carry: carry[0] < trips, trip, start)
        far = swap_x(pack)
        loss_oth = swap_dp(jnp.full((8, 128), loss))
        d_hidden = scatter_pass(d_rows, idx_win, base, batch, seq_len, max_pred)
        far, loss_oth, d_hidden = tie(far, loss_oth, d_hidden)
        pair = jnp.where(tp // 2 == 0, jnp.stack([pack, far]), jnp.stack([far, pack]))
        theirs = swap_core(pair)
        pack = jnp.where(core == 0, jnp.stack([pair, theirs], 1), jnp.stack([theirs, pair], 1)).reshape(-1, width)
        loss = (loss + loss_oth[0, 0]) / denom
        return loss, d_hidden, pack[:width], pack[width], pack[width + 1], pack[width + 2], d_embed, d_out_bias[0, :shard_vocab]

    in_specs = (P("dp", None, None), P("dp", None), P("dp", None), P("dp", None), P(None, None), P(None), P(None), P(None), P("tp", None), P("tp"))
    out_specs = (P(), P("dp", None, None), P(None, None), P(None), P(None), P(None), P("tp", None), P("tp"))
    return jax.shard_map(local_step, mesh=mesh, in_specs=in_specs, out_specs=out_specs, check_vma=False)
```

```python
import functools

import jax
import jax.numpy as jnp
from jax import lax
from jax.experimental import pallas as pl
from jax.experimental.pallas import tpu as pltpu
from jax.sharding import PartitionSpec as P


LN_EPS = 1e-12
LOSS_EPS = 1e-5
F32 = jnp.float32
BF16 = jnp.bfloat16
VT = 512
CB = 512
MAIN = 1536
CHUNKS = 2
CUT = 1024
SUB = 64
BACK = 256
WIN = 128
VMEM_LIMIT = 44 * 1024 * 1024

SWAP_DP = tuple((i, i ^ 1) for i in range(2))
SWAP_CORE = tuple((i, i ^ 1) for i in range(4))
SWAP_X = tuple((i, i ^ 2) for i in range(4))
FIRST, SECOND, THIRD = (slice(i, i + 1) for i in range(3))


def whole(*shape):
    return pl.BlockSpec(shape, lambda *_: (0,) * len(shape))


def swap_dp(x):
    return lax.ppermute(x, "dp", SWAP_DP)


def swap_core(x):
    return lax.ppermute(x, "tp", SWAP_CORE)


def swap_x(x):
    return lax.ppermute(x, "tp", SWAP_X)


def gather_body(per, meta_ref, idx_ref, h_ref, out_ref, acc):
    step = pl.program_id(0)

    @pl.when(step == 0)
    def _():
        acc[...] = jnp.zeros_like(acc)

    seq_len = h_ref.shape[1]
    lane = lax.broadcasted_iota(jnp.int32, (WIN, seq_len), 1).astype(F32)
    for i in range(per):
        col = jnp.broadcast_to(idx_ref[i], (WIN, WIN)).T
        hot = jnp.concatenate([col] * (seq_len // WIN), axis=1) == lane
        rows = jnp.dot(hot.astype(F32).astype(BF16), h_ref[i], preferred_element_type=F32)
        base = pl.multiple_of(meta_ref[step * per + i], 8)
        acc[pl.ds(base, WIN), :] += rows

    @pl.when(step == pl.num_programs(0) - 1)
    def _():
        out_ref[...] = acc[: out_ref.shape[0], :].astype(BF16)


def gather_pass(hidden, idx_win, base, rows):
    batch, seq_len, width = hidden.shape
    per = 4
    return pl.pallas_call(
        functools.partial(gather_body, per),
        out_shape=jax.ShapeDtypeStruct((rows, width), BF16),
        grid_spec=pltpu.PrefetchScalarGridSpec(
            num_scalar_prefetch=1, grid=(batch // per,),
            in_specs=[
                pl.BlockSpec((per, 1, WIN), lambda b, m: (b, 0, 0)),
                pl.BlockSpec((per, seq_len, width), lambda b, m: (b, 0, 0)),
            ],
            out_specs=whole(rows, width),
            scratch_shapes=[pltpu.VMEM((rows + WIN, width), F32)],
        ),
        compiler_params=pltpu.CompilerParams(dimension_semantics=("arbitrary",), vmem_limit_bytes=VMEM_LIMIT),
        cost_estimate=pl.CostEstimate(flops=2 * batch * WIN * seq_len * width, bytes_accessed=batch * seq_len * width * 2, transcendentals=0),
    )(base, idx_win, hidden)


def transform_body(meta_ref, h_ref, w_ref, vec_ref, t_ref, tt_ref, norm_ref, slope_ref, send_ref, pre, t_s):
    pre[...] = jnp.dot(h_ref[...], w_ref[...], preferred_element_type=F32) + vec_ref[FIRST]

    def some(i, _):
        at = pl.ds(pl.multiple_of(i * SUB, SUB), SUB)
        u = pre[at, :]
        cdf = 0.5 * (1.0 + lax.erf(u * 0.7071067811865476))
        act = u * cdf
        mean = jnp.mean(act, axis=1, keepdims=True)
        cent = act - mean
        inv = lax.rsqrt(jnp.mean(cent * cent, axis=1, keepdims=True) + LN_EPS)
        norm = cent * inv
        norm_ref[at, :] = norm
        slope_ref[at, :] = (cdf + u * (0.3989422804014327 * jnp.exp(-0.5 * u * u))) * inv
        t_s[at, :] = norm * vec_ref[SECOND] + vec_ref[THIRD]
        return 0

    lax.fori_loop(0, h_ref.shape[0] // SUB, some, 0)
    t = t_s[...].astype(BF16)
    t_ref[...] = t
    tt_ref[...] = t.T

    @pl.when(pl.program_id(0) == meta_ref[0])
    def _():
        send_ref[...] = t_s[...]


def transform_pass(h, w_t, vecs, tp, chunk):
    width = h.shape[1]
    part = MAIN // 4
    strip = pl.BlockSpec((part, width), lambda i, m: (i, 0))
    return pl.pallas_call(
        transform_body,
        out_shape=(
            jax.ShapeDtypeStruct((MAIN, width), BF16), jax.ShapeDtypeStruct((width, MAIN), BF16),
            jax.ShapeDtypeStruct((MAIN, width), F32), jax.ShapeDtypeStruct((MAIN, width), F32),
            jax.ShapeDtypeStruct((part, width), F32),
        ),
        grid_spec=pltpu.PrefetchScalarGridSpec(
            num_scalar_prefetch=1, grid=(4,),
            in_specs=[pl.BlockSpec((part, width), lambda i, m: (m[1] * 4 + i, 0)), whole(width, width), whole(8, width)],
            out_specs=(strip, pl.BlockSpec((width, part), lambda i, m: (0, i)), strip, strip, whole(part, width)),
            scratch_shapes=[pltpu.VMEM((part, width), F32), pltpu.VMEM((part, width), F32)],
        ),
        compiler_params=params(),
        cost_estimate=pl.CostEstimate(flops=2 * MAIN * width * width, bytes_accessed=MAIN * width * 14, transcendentals=2 * MAIN * width),
    )(jnp.stack([tp, chunk]), h, w_t, vecs)


def collect_body(place_ref, *refs):
    t_ref, tt_ref = refs[4:]
    for i, piece in enumerate(refs[:4]):
        @pl.when(pl.program_id(0) == i)
        def _():
            t = piece[...].astype(BF16)
            t_ref[...] = t
            tt_ref[...] = t.T


def collect_pass(pieces, tp):
    part, width = pieces[0].shape
    return pl.pallas_call(
        collect_body,
        out_shape=(jax.ShapeDtypeStruct((MAIN, width), BF16), jax.ShapeDtypeStruct((width, MAIN), BF16)),
        grid_spec=pltpu.PrefetchScalarGridSpec(
            num_scalar_prefetch=1, grid=(4,),
            in_specs=[whole(part, width)] * 4,
            out_specs=(pl.BlockSpec((part, width), lambda i, m: (m[i], 0)), pl.BlockSpec((width, part), lambda i, m: (0, m[i]))),
        ),
        compiler_params=params(),
        cost_estimate=pl.CostEstimate(flops=MAIN * width, bytes_accessed=MAIN * width * 8, transcendentals=0),
    )(tp ^ jnp.array([0, 2, 1, 3], jnp.int32), *pieces)


def back_body(meta_ref, mine_a_ref, theirs_a_ref, mine_b_ref, theirs_b_ref, norm_ref, slope_ref, h_ref, w_ref, gamma_ref, old_ref, dh_ref, pack_ref):
    step = pl.program_id(0)
    last = pl.num_programs(0) - 1
    width = w_ref.shape[0]

    @pl.when(step == 0)
    def _():
        pack_ref[...] = jnp.zeros_like(pack_ref)

    @pl.when(step < last)
    def _():
        low = meta_ref[0] == 0
        in_a = step < CUT // BACK
        mine = jnp.where(in_a, mine_a_ref[...], mine_b_ref[...]).T
        theirs = jnp.where(in_a, theirs_a_ref[...], theirs_b_ref[...]).T
        d_t = jnp.concatenate([jnp.where(low, mine, theirs), jnp.where(low, theirs, mine)], axis=1)
        norm = norm_ref[...]
        d_gamma = jnp.sum(d_t * norm, axis=0, keepdims=True)
        d_beta = jnp.sum(d_t, axis=0, keepdims=True)
        g = d_t * gamma_ref[...]
        g_mean = jnp.mean(g, axis=1, keepdims=True)
        gn_mean = jnp.mean(g * norm, axis=1, keepdims=True)
        d_u = (g - g_mean - norm * gn_mean) * slope_ref[...]
        d_b = jnp.sum(d_u, axis=0, keepdims=True)
        pack_ref[width:width + 8] += jnp.concatenate([d_b, d_gamma, d_beta] + [jnp.zeros_like(d_b)] * 5)
        d_u = d_u.astype(BF16)
        pack_ref[:width] += lax.dot_general(h_ref[...], d_u, (((0,), (0,)), ((), ())), preferred_element_type=F32)
        d_h = lax.dot_general(d_u, w_ref[...], (((1,), (1,)), ((), ())), preferred_element_type=F32)
        dh_ref[...] = d_h.astype(BF16).astype(F32)

    @pl.when(step == last)
    def _():
        dh_ref[...] = jnp.zeros_like(dh_ref)


def back_pass(a, b, norm, slope, h, w_t, gamma, core, chunk, old):
    width = norm.shape[1]
    steps = MAIN // BACK
    strip = pl.BlockSpec((BACK, width), lambda i, m: (jnp.minimum(i, steps - 1), 0))
    flat = lambda start, count: pl.BlockSpec((width // 2, BACK), lambda i, m: (0, jnp.clip(i - start, 0, count - 1)))
    at_a, at_b = flat(0, CUT // BACK), flat(CUT // BACK, (MAIN - CUT) // BACK)
    return pl.pallas_call(
        back_body,
        out_shape=(jax.ShapeDtypeStruct(old.shape, F32), jax.ShapeDtypeStruct((width + 32, width), F32)),
        grid_spec=pltpu.PrefetchScalarGridSpec(
            num_scalar_prefetch=1, grid=(steps + 1,),
            in_specs=[
                at_a, at_a, at_b, at_b, strip, strip,
                pl.BlockSpec((BACK, width), lambda i, m: (m[1] * steps + jnp.minimum(i, steps - 1), 0)),
                whole(width, width), whole(1, width), pl.BlockSpec(memory_space=pl.ANY),
            ],
            out_specs=(pl.BlockSpec((BACK, width), lambda i, m: (m[1] * steps + i, 0)), whole(width + 32, width)),
        ),
        input_output_aliases={10: 0},
        compiler_params=params(),
        cost_estimate=pl.CostEstimate(flops=4 * MAIN * width * width, bytes_accessed=MAIN * width * 18, transcendentals=0),
    )(jnp.stack([core, chunk]), *a, *b, norm, slope, h, w_t, gamma, old)


def scatter_body(per, meta_ref, idx_ref, dh_ref, out_ref):
    step = pl.program_id(0)
    seq_len = out_ref.shape[1]
    spot = lax.broadcasted_iota(jnp.int32, (seq_len, WIN), 0).astype(F32)
    for i in range(per):
        hot = (spot == idx_ref[i]).astype(F32).astype(BF16)
        at = pl.multiple_of((meta_ref[step * per + i] - meta_ref[step * per]) * 8, 8)
        rows = dh_ref[pl.ds(at, WIN), :].astype(BF16)
        out_ref[i] = jnp.dot(hot, rows, preferred_element_type=F32).astype(BF16)


def scatter_pass(dh, idx_win, base, batch, seq_len, max_pred):
    width = dh.shape[1]
    per = 4
    span = (per - 1) * max_pred + WIN
    return pl.pallas_call(
        functools.partial(scatter_body, per),
        out_shape=jax.ShapeDtypeStruct((batch, seq_len, width), BF16),
        grid_spec=pltpu.PrefetchScalarGridSpec(
            num_scalar_prefetch=1, grid=(batch // per,),
            in_specs=[
                pl.BlockSpec((per, 1, WIN), lambda b, m: (b, 0, 0)),
                pl.BlockSpec((pl.Element(span), pl.Element(width)), lambda b, m: (m[b * per] * 8, 0)),
            ],
            out_specs=pl.BlockSpec((per, seq_len, width), lambda b, m: (b, 0, 0)),
        ),
        compiler_params=pltpu.CompilerParams(dimension_semantics=("arbitrary",), vmem_limit_bytes=VMEM_LIMIT),
        cost_estimate=pl.CostEstimate(flops=2 * batch * WIN * seq_len * width, bytes_accessed=batch * seq_len * width * 2, transcendentals=0),
    )(lax.div(base, 8), idx_win, dh)


def params():
    return pltpu.CompilerParams(dimension_semantics=("arbitrary",), vmem_limit_bytes=VMEM_LIMIT)


def scratch_array(*shape):
    return pl.pallas_call(
        lambda out_ref: None, out_shape=jax.ShapeDtypeStruct(shape, F32), out_specs=pl.BlockSpec(memory_space=pl.ANY)
    )()


def by_tile(rows, cols, start=0):
    return pl.BlockSpec((rows, cols), lambda j, *_: (j + start, 0))


def strip_of(start=0):
    return pl.BlockSpec((1, VT), lambda j, *_: (0, j + start))


def clear_tail(e_ref, shard):
    tail = shard % VT

    @pl.when(pl.program_id(0) == shard // VT)
    def _():
        e_ref[tail:] = jnp.zeros((VT - tail, e_ref.shape[1]), BF16)


def columns():
    return [slice(i, i + CB) for i in range(0, MAIN, CB)]


def logits_body(shard, target, e_ref, t_ref, bias_ref, lab_ref, soft_ref, stat_ref):
    clear_tail(e_ref, shard)
    bias = jnp.broadcast_to(bias_ref[...], (128, VT)).T
    bias = jnp.concatenate([bias] * (CB // 128), axis=1)
    vocab = lax.broadcasted_iota(jnp.int32, (VT, CB), 0)
    for cols in columns():
        z = jnp.dot(e_ref[...], t_ref[:, cols], preferred_element_type=F32) + bias
        top = jnp.max(z, axis=0, keepdims=True)
        soft = jnp.exp(z - top)
        soft_ref[:, cols] = soft
        stat_ref[FIRST, cols] = top
        stat_ref[SECOND, cols] = jnp.sum(soft, axis=0, keepdims=True)
        if target:
            hot = vocab == lab_ref[:, cols] - pl.program_id(0) * VT
            stat_ref[THIRD, cols] = jnp.sum(jnp.where(hot, z, 0.0), axis=0, keepdims=True)


def logits_pass(embed, t_t, bias, lab, target):
    shard, width = embed.shape
    steps = pl.cdiv(shard, VT)
    return pl.pallas_call(
        functools.partial(logits_body, shard, target),
        out_shape=(jax.ShapeDtypeStruct((steps * VT, MAIN), F32), jax.ShapeDtypeStruct((steps * 8, MAIN), F32)),
        grid_spec=pltpu.PrefetchScalarGridSpec(
            num_scalar_prefetch=0, grid=(steps,),
            in_specs=[by_tile(VT, width), whole(width, MAIN), strip_of(), whole(1, MAIN)],
            out_specs=(by_tile(VT, MAIN), by_tile(8, MAIN)),
        ),
        compiler_params=params(),
        cost_estimate=pl.CostEstimate(flops=2 * MAIN * shard * width, bytes_accessed=MAIN * shard * 4, transcendentals=MAIN * shard),
    )(embed, t_t, bias, lab)


def grad_logits(soft_ref, vec_ref, lab_ref, cols, vocab, step):
    soft = soft_ref[:, cols] * vec_ref[FIRST, cols]
    return jnp.where(vocab == lab_ref[:, cols] - step * VT, soft - vec_ref[SECOND, cols], soft)


def lane_groups(dz):
    acc = dz[:, :128]
    for k in range(128, CB, 128):
        acc = acc + dz[:, k:k + 128]
    return acc


def hidden_body(shard, core_ref, soft_ref, vec_ref, lab_ref, e_ref, dz_ref, keep_ref, give_ref, db_ref, dt_s):
    step = pl.program_id(0)
    half = keep_ref.shape[0]

    @pl.when(step == 0)
    def _():
        dt_s[...] = jnp.zeros_like(dt_s)

    clear_tail(e_ref, shard)
    vocab = lax.broadcasted_iota(jnp.int32, (VT, CB), 0)
    acc = []
    for cols in columns():
        dz = grad_logits(soft_ref, vec_ref, lab_ref, cols, vocab, step)
        acc.append(lane_groups(dz))
        dz_ref[:, cols] = dz.astype(BF16)
    dt_s[...] += lax.dot_general(e_ref[...], dz_ref[...], (((0,), (0,)), ((), ())), preferred_element_type=F32)
    db_ref[...] = jnp.sum(sum(acc[1:], acc[0]).T, axis=0, keepdims=True)

    @pl.when(step == pl.num_programs(0) - 1)
    def _():
        core = core_ref[0]
        keep_ref[...] = dt_s[pl.ds(pl.multiple_of(core * half, 8), half), :]
        give_ref[...] = dt_s[pl.ds(pl.multiple_of((1 - core) * half, 8), half), :]


def hidden_pass(soft, vec, lab, embed, core):
    shard, width = embed.shape
    padded = soft.shape[0]
    flat = whole(width // 2, MAIN)
    return pl.pallas_call(
        functools.partial(hidden_body, shard),
        out_shape=(
            jax.ShapeDtypeStruct((padded, MAIN), BF16),
            jax.ShapeDtypeStruct((width // 2, MAIN), F32), jax.ShapeDtypeStruct((width // 2, MAIN), F32),
            jax.ShapeDtypeStruct((1, padded), F32),
        ),
        grid_spec=pltpu.PrefetchScalarGridSpec(
            num_scalar_prefetch=1, grid=(padded // VT,),
            in_specs=[by_tile(VT, MAIN), by_tile(8, MAIN), whole(1, MAIN), by_tile(VT, width)],
            out_specs=(by_tile(VT, MAIN), flat, flat, strip_of()),
            scratch_shapes=[pltpu.VMEM((width, MAIN), F32)],
        ),
        compiler_params=params(),
        cost_estimate=pl.CostEstimate(flops=2 * MAIN * shard * width, bytes_accessed=MAIN * shard * 6, transcendentals=0),
    )(core.reshape(1), soft, vec, lab, embed)


def embed_body(start, meta_ref, dz_ref, soft_ref, vec_ref, lab_ref, t_own_ref, t_oth_ref, db_own_ref, old_ref, de_ref, db_ref, dz_s, old_s, sem):
    step = pl.program_id(0) + start
    tail = old_ref.shape[0] % VT

    @pl.when(pl.program_id(0) == 0)
    def _():
        old_s[...] = jnp.zeros_like(old_s)

    for rows, here in ((VT, step < old_ref.shape[0] // VT), (tail, step == old_ref.shape[0] // VT)):
        @pl.when((meta_ref[0] > 0) & here)
        def _():
            copy = pltpu.make_async_copy(old_ref.at[pl.ds(pl.multiple_of(step * VT, VT), rows)], old_s.at[:rows], sem)
            copy.start()
            copy.wait()

    vocab = lax.broadcasted_iota(jnp.int32, (VT, CB), 0)
    acc = []
    for cols in columns():
        dz = grad_logits(soft_ref, vec_ref, lab_ref, cols, vocab, step)
        acc.append(lane_groups(dz))
        dz_s[:, cols] = dz.astype(BF16)
    de_ref[...] = old_s[...] + jnp.dot(dz_ref[...], t_own_ref[...], preferred_element_type=F32)
    de_ref[...] += jnp.dot(dz_s[...], t_oth_ref[...], preferred_element_type=F32)
    db_ref[...] = db_own_ref[...] + jnp.sum(sum(acc[1:], acc[0]).T, axis=0, keepdims=True)


def embed_pass(start, count, dz_own, soft_oth, vec, lab, t_own, t_oth, db_own, old, chunk):
    shard, width = old.shape
    return pl.pallas_call(
        functools.partial(embed_body, start),
        out_shape=(jax.ShapeDtypeStruct((shard, width), F32), jax.ShapeDtypeStruct((1, count * VT), F32)),
        grid_spec=pltpu.PrefetchScalarGridSpec(
            num_scalar_prefetch=1, grid=(count,),
            in_specs=[
                by_tile(VT, MAIN, start), by_tile(VT, MAIN, start), by_tile(8, MAIN, start), whole(1, MAIN),
                whole(MAIN, width), whole(MAIN, width), strip_of(start), pl.BlockSpec(memory_space=pl.ANY),
            ],
            out_specs=(by_tile(VT, width, start), strip_of()),
            scratch_shapes=[pltpu.VMEM((VT, MAIN), BF16), pltpu.VMEM((VT, width), F32), pltpu.SemaphoreType.DMA],
        ),
        input_output_aliases={8: 0},
        compiler_params=params(),
        cost_estimate=pl.CostEstimate(flops=4 * MAIN * count * VT * width, bytes_accessed=MAIN * count * VT * 6 + count * VT * width * 4, transcendentals=0),
    )(chunk.reshape(1), dz_own, soft_oth, vec, lab, t_own, t_oth, db_own, old)


def combine(stat):
    top, tot, hit = (stat.reshape(-1, 8, MAIN)[:, i] for i in range(3))
    best = jnp.max(top, axis=0)
    stats = jnp.stack([best, jnp.sum(tot * jnp.exp(top - best), axis=0), jnp.sum(hit, axis=0)])
    for swap in (swap_core, swap_x):
        other = swap(stats)
        best = jnp.maximum(stats[0], other[0])
        stats = jnp.stack([
            best,
            stats[1] * jnp.exp(stats[0] - best) + other[1] * jnp.exp(other[0] - best),
            stats[2] + other[2],
        ])
    return stats, top


def tie(*values):
    return lax.optimization_barrier(values)


def solution(mesh):
    def local_step(hidden, positions, labels, weights, w_t, b_t, gamma, beta, embed, out_bias):
        batch, seq_len, width = hidden.shape
        max_pred = positions.shape[1]
        shard_vocab = embed.shape[0]
        tiles = pl.cdiv(shard_vocab, VT)
        tp = lax.axis_index("tp")
        core = tp % 2
        counts = jnp.sum(weights, axis=1).astype(jnp.int32)
        seq = jnp.arange(batch, dtype=jnp.int32)
        offsets = jnp.sum(jnp.where(seq[None, :] < seq[:, None], counts[None, :], 0), 1)
        n_own = jnp.sum(counts)
        n_oth = swap_dp(jnp.full((8, 128), n_own, jnp.int32))
        shift = offsets % 8
        base = offsets - shift
        live = jnp.where(jnp.arange(max_pred)[None, :] < counts[:, None], positions, -1).astype(F32)
        idx_win = jnp.full((batch, WIN), -1.0, F32)
        for k in range(8):
            moved = jnp.pad(live, ((0, 0), (k, WIN - max_pred - k)), constant_values=-1.0)
            idx_win = jnp.where((shift == k)[:, None], moved, idx_win)
        idx_win = idx_win[:, None, :]
        tok_rows = gather_pass(hidden, idx_win, base, CHUNKS * MAIN)
        n_oth, tok_rows = tie(n_oth, tok_rows)
        n_oth = n_oth[0, 0]
        trips = jnp.where(jnp.maximum(n_own, n_oth) > MAIN, CHUNKS, 1)
        denom = (n_own + n_oth).astype(F32) + LOSS_EPS
        bias = jnp.pad(out_bias, (0, tiles * VT - shard_vocab), constant_values=-jnp.inf)[None, :]
        vecs = jnp.stack([b_t, gamma, beta] + [jnp.zeros_like(b_t)] * 5)

        def local_labels(lab):
            lab = lab - tp * shard_vocab
            return jnp.where((lab >= 0) & (lab < shard_vocab), lab, -1)[None, :]

        def trip(carry):
            chunk, d_embed, d_rows, pack_sum, bias_sum, loss_sum = carry
            row = chunk * MAIN + jnp.arange(MAIN, dtype=jnp.int32)
            in_seq = (row[:, None] >= offsets[None, :]) & (row[:, None] < (offsets + counts)[None, :])
            slot_row = jnp.where(row < n_own, row - jnp.sum(jnp.where(in_seq, offsets[None, :], 0), 1), -1)
            lab_seq = jnp.dot(in_seq.astype(F32), labels.astype(F32), precision=lax.Precision.HIGHEST)
            slot_hot = slot_row[:, None] == jnp.arange(max_pred, dtype=jnp.int32)[None, :]
            lab_own = jnp.sum(jnp.where(slot_hot, lab_seq, 0.0), 1).astype(jnp.int32)
            lab_oth = swap_dp(lab_own)

            def vectors(stats, tops, n):
                scale = (row < n).astype(F32) / denom
                factor = jnp.exp(tops - stats[0]) * (scale / stats[1])
                first = jnp.arange(8, dtype=jnp.int32)[:, None] == 0
                return jnp.where(first, factor[:, None], scale).reshape(-1, MAIN)

            t_own, t_own_t, norm, slope, send = transform_pass(tok_rows, w_t, vecs, tp, chunk)
            got = swap_dp(send)
            soft_own, stat_own = logits_pass(embed, t_own_t, bias, local_labels(lab_own), True)
            got, stat_own, lab_oth = tie(got, stat_own, lab_oth)
            stat_own, tops_own = combine(stat_own)
            got_x, got_core = swap_x(got), swap_core(got)
            loss_sum = loss_sum + jnp.sum(jnp.where(row < n_own, jnp.log(stat_own[1]) + stat_own[0] - stat_own[2], 0.0))
            dz_own, keep, give, db_own = hidden_pass(soft_own, vectors(stat_own, tops_own, n_own), local_labels(lab_own), embed, core)
            got_x, got_core, keep = tie(got_x, got_core, keep)
            got_far, give = tie(swap_core(got_x), give)
            given = swap_core(give)
            t_oth, t_oth_t = collect_pass((got, got_x, got_core, got_far), tp)
            given, t_oth_t = tie(given, t_oth_t)
            chip_a, chip_b = keep[:, :CUT] + given[:, :CUT], keep[:, CUT:] + given[:, CUT:]
            chip_a, chip_b, t_oth_t = tie(chip_a, chip_b, t_oth_t)
            other_a = swap_x(chip_a)
            soft_oth, stat_oth = logits_pass(embed, t_oth_t, bias, local_labels(lab_oth), False)
            other_a, stat_oth = tie(other_a, stat_oth)
            stat_oth, tops_oth = combine(stat_oth)
            chip_b, stat_oth = tie(chip_b, stat_oth)
            other_b = swap_x(chip_b)
            mine_a = chip_a + other_a
            theirs_a = swap_core(mine_a)
            vec_oth = vectors(stat_oth, tops_oth, n_oth)

            def embed_tiles(start, count, old):
                return embed_pass(start, count, dz_own, soft_oth, vec_oth, local_labels(lab_oth), t_own, t_oth, db_own, old, chunk)

            d_embed, db_0 = embed_tiles(0, 7, d_embed)
            other_b, theirs_a, d_embed = tie(other_b, theirs_a, d_embed)
            mine_b = chip_b + other_b
            theirs_b = swap_core(mine_b)
            d_rows, pack = back_pass((mine_a, theirs_a), (mine_b, theirs_b), norm, slope, tok_rows, w_t, gamma[None, :], core, chunk, d_rows)
            quarter = pack.shape[0] // 4
            pack = lax.dynamic_slice_in_dim(pack, tp * quarter, quarter)
            pack, d_embed = tie(pack, d_embed)
            far = swap_dp(pack)
            d_embed, db_1 = embed_tiles(7, tiles - 7, d_embed)
            far, d_embed = tie(far, d_embed)
            bias_sum = bias_sum + jnp.concatenate([db_0, db_1], axis=1)
            return chunk + 1, d_embed, d_rows, pack_sum + (pack + far), bias_sum, loss_sum

        start = (
            jnp.int32(0), scratch_array(shard_vocab, width), scratch_array(CHUNKS * MAIN + BACK, width),
            jnp.zeros(((width + 32) // 4, width), F32), jnp.zeros((1, tiles * VT), F32), jnp.zeros((), F32),
        )
        _, d_embed, d_rows, pack, d_out_bias, loss = lax.while_loop(lambda carry: carry[0] < trips, trip, start)
        far = swap_x(pack)
        loss_oth = swap_dp(jnp.full((8, 128), loss))
        d_hidden = scatter_pass(d_rows, idx_win, base, batch, seq_len, max_pred)
        far, loss_oth, d_hidden = tie(far, loss_oth, d_hidden)
        pair = jnp.where(tp // 2 == 0, jnp.stack([pack, far]), jnp.stack([far, pack]))
        theirs = swap_core(pair)
        pack = jnp.where(core == 0, jnp.stack([pair, theirs], 1), jnp.stack([theirs, pair], 1)).reshape(-1, width)
        loss = (loss + loss_oth[0, 0]) / denom
        return loss, d_hidden, pack[:width], pack[width], pack[width + 1], pack[width + 2], d_embed, d_out_bias[0, :shard_vocab]

    in_specs = (P("dp", None, None), P("dp", None), P("dp", None), P("dp", None), P(None, None), P(None), P(None), P(None), P("tp", None), P("tp"))
    out_specs = (P(), P("dp", None, None), P(None, None), P(None), P(None), P(None), P("tp", None), P("tp"))
    return jax.shard_map(local_step, mesh=mesh, in_specs=in_specs, out_specs=out_specs, check_vma=False)
```

```python
import functools

import jax
import jax.numpy as jnp
from jax import lax
from jax.experimental import pallas as pl
from jax.experimental.pallas import tpu as pltpu
from jax.sharding import PartitionSpec as P


LN_EPS = 1e-12
LOSS_EPS = 1e-5
F32 = jnp.float32
BF16 = jnp.bfloat16
VT = 512
CB = 512
MAIN = 1536
CHUNKS = 2
CUT = 1024
SUB = 64
BACK = 256
WIN = 128
VMEM_LIMIT = 44 * 1024 * 1024

SWAP_DP = tuple((i, i ^ 1) for i in range(2))
SWAP_CORE = tuple((i, i ^ 1) for i in range(4))
SWAP_X = tuple((i, i ^ 2) for i in range(4))
SWAP_DIAGONAL = tuple((i, i ^ 3) for i in range(4))
FIRST, SECOND, THIRD = (slice(i, i + 1) for i in range(3))


def whole(*shape):
    return pl.BlockSpec(shape, lambda *_: (0,) * len(shape))


def swap_dp(x):
    return lax.ppermute(x, "dp", SWAP_DP)


def swap_core(x):
    return lax.ppermute(x, "tp", SWAP_CORE)


def swap_x(x):
    return lax.ppermute(x, "tp", SWAP_X)


def gather_body(per, meta_ref, idx_ref, h_ref, out_ref, acc):
    step = pl.program_id(0)

    @pl.when(step == 0)
    def _():
        acc[...] = jnp.zeros_like(acc)

    seq_len = h_ref.shape[1]
    lane = lax.broadcasted_iota(jnp.int32, (WIN, seq_len), 1).astype(F32)
    for i in range(per):
        col = jnp.broadcast_to(idx_ref[i], (WIN, WIN)).T
        hot = jnp.concatenate([col] * (seq_len // WIN), axis=1) == lane
        rows = jnp.dot(hot.astype(F32).astype(BF16), h_ref[i], preferred_element_type=F32)
        base = pl.multiple_of(meta_ref[step * per + i], 8)
        acc[pl.ds(base, WIN), :] += rows

    @pl.when(step == pl.num_programs(0) - 1)
    def _():
        out_ref[...] = acc[: out_ref.shape[0], :].astype(BF16)


def gather_pass(hidden, idx_win, base, rows):
    batch, seq_len, width = hidden.shape
    per = 4
    return pl.pallas_call(
        functools.partial(gather_body, per),
        out_shape=jax.ShapeDtypeStruct((rows, width), BF16),
        grid_spec=pltpu.PrefetchScalarGridSpec(
            num_scalar_prefetch=1, grid=(batch // per,),
            in_specs=[
                pl.BlockSpec((per, 1, WIN), lambda b, m: (b, 0, 0)),
                pl.BlockSpec((per, seq_len, width), lambda b, m: (b, 0, 0)),
            ],
            out_specs=whole(rows, width),
            scratch_shapes=[pltpu.VMEM((rows + WIN, width), F32)],
        ),
        compiler_params=pltpu.CompilerParams(dimension_semantics=("arbitrary",), vmem_limit_bytes=VMEM_LIMIT),
        cost_estimate=pl.CostEstimate(flops=2 * batch * WIN * seq_len * width, bytes_accessed=batch * seq_len * width * 2, transcendentals=0),
    )(base, idx_win, hidden)


def transform_body(meta_ref, h_ref, w_ref, vec_ref, t_ref, tt_ref, norm_ref, slope_ref, send_ref, pre, t_s):
    pre[...] = jnp.dot(h_ref[...], w_ref[...], preferred_element_type=F32) + vec_ref[FIRST]

    def some(i, _):
        at = pl.ds(pl.multiple_of(i * SUB, SUB), SUB)
        u = pre[at, :]
        cdf = 0.5 * (1.0 + lax.erf(u * 0.7071067811865476))
        act = u * cdf
        mean = jnp.mean(act, axis=1, keepdims=True)
        cent = act - mean
        inv = lax.rsqrt(jnp.mean(cent * cent, axis=1, keepdims=True) + LN_EPS)
        norm = cent * inv
        norm_ref[at, :] = norm
        slope_ref[at, :] = (cdf + u * (0.3989422804014327 * jnp.exp(-0.5 * u * u))) * inv
        t_s[at, :] = norm * vec_ref[SECOND] + vec_ref[THIRD]
        return 0

    lax.fori_loop(0, h_ref.shape[0] // SUB, some, 0)
    t = t_s[...].astype(BF16)
    t_ref[...] = t
    tt_ref[...] = t.T

    @pl.when(pl.program_id(0) == meta_ref[0])
    def _():
        send_ref[...] = t_s[...]


def transform_pass(h, w_t, vecs, tp, chunk):
    width = h.shape[1]
    part = MAIN // 4
    strip = pl.BlockSpec((part, width), lambda i, m: (i, 0))
    return pl.pallas_call(
        transform_body,
        out_shape=(
            jax.ShapeDtypeStruct((MAIN, width), BF16), jax.ShapeDtypeStruct((width, MAIN), BF16),
            jax.ShapeDtypeStruct((MAIN, width), F32), jax.ShapeDtypeStruct((MAIN, width), F32),
            jax.ShapeDtypeStruct((part, width), F32),
        ),
        grid_spec=pltpu.PrefetchScalarGridSpec(
            num_scalar_prefetch=1, grid=(4,),
            in_specs=[pl.BlockSpec((part, width), lambda i, m: (m[1] * 4 + i, 0)), whole(width, width), whole(8, width)],
            out_specs=(strip, pl.BlockSpec((width, part), lambda i, m: (0, i)), strip, strip, whole(part, width)),
            scratch_shapes=[pltpu.VMEM((part, width), F32), pltpu.VMEM((part, width), F32)],
        ),
        compiler_params=params(),
        cost_estimate=pl.CostEstimate(flops=2 * MAIN * width * width, bytes_accessed=MAIN * width * 14, transcendentals=2 * MAIN * width),
    )(jnp.stack([tp, chunk]), h, w_t, vecs)


def collect_body(place_ref, *refs):
    t_ref, tt_ref = refs[4:]
    for i, piece in enumerate(refs[:4]):
        @pl.when(pl.program_id(0) == i)
        def _():
            t = piece[...].astype(BF16)
            t_ref[...] = t
            tt_ref[...] = t.T


def collect_pass(pieces, tp):
    part, width = pieces[0].shape
    return pl.pallas_call(
        collect_body,
        out_shape=(jax.ShapeDtypeStruct((MAIN, width), BF16), jax.ShapeDtypeStruct((width, MAIN), BF16)),
        grid_spec=pltpu.PrefetchScalarGridSpec(
            num_scalar_prefetch=1, grid=(4,),
            in_specs=[whole(part, width)] * 4,
            out_specs=(pl.BlockSpec((part, width), lambda i, m: (m[i], 0)), pl.BlockSpec((width, part), lambda i, m: (0, m[i]))),
        ),
        compiler_params=params(),
        cost_estimate=pl.CostEstimate(flops=MAIN * width, bytes_accessed=MAIN * width * 8, transcendentals=0),
    )(tp ^ jnp.array([0, 2, 1, 3], jnp.int32), *pieces)


def back_body(meta_ref, mine_a_ref, theirs_a_ref, mine_b_ref, theirs_b_ref, norm_ref, slope_ref, h_ref, w_ref, gamma_ref, old_ref, dh_ref, pack_ref):
    step = pl.program_id(0)
    last = pl.num_programs(0) - 1
    width = w_ref.shape[0]

    @pl.when(step == 0)
    def _():
        pack_ref[...] = jnp.zeros_like(pack_ref)

    @pl.when(step < last)
    def _():
        low = meta_ref[0] == 0
        in_a = step < CUT // BACK
        mine = jnp.where(in_a, mine_a_ref[...], mine_b_ref[...]).T
        theirs = jnp.where(in_a, theirs_a_ref[...], theirs_b_ref[...]).T
        d_t = jnp.concatenate([jnp.where(low, mine, theirs), jnp.where(low, theirs, mine)], axis=1)
        norm = norm_ref[...]
        d_gamma = jnp.sum(d_t * norm, axis=0, keepdims=True)
        d_beta = jnp.sum(d_t, axis=0, keepdims=True)
        g = d_t * gamma_ref[...]
        g_mean = jnp.mean(g, axis=1, keepdims=True)
        gn_mean = jnp.mean(g * norm, axis=1, keepdims=True)
        d_u = (g - g_mean - norm * gn_mean) * slope_ref[...]
        d_b = jnp.sum(d_u, axis=0, keepdims=True)
        pack_ref[width:width + 8] += jnp.concatenate([d_b, d_gamma, d_beta] + [jnp.zeros_like(d_b)] * 5)
        d_u = d_u.astype(BF16)
        pack_ref[:width] += lax.dot_general(h_ref[...], d_u, (((0,), (0,)), ((), ())), preferred_element_type=F32)
        d_h = lax.dot_general(d_u, w_ref[...], (((1,), (1,)), ((), ())), preferred_element_type=F32)
        dh_ref[...] = d_h.astype(BF16).astype(F32)

    @pl.when(step == last)
    def _():
        dh_ref[...] = jnp.zeros_like(dh_ref)


def back_pass(a, b, norm, slope, h, w_t, gamma, core, chunk, old):
    width = norm.shape[1]
    steps = MAIN // BACK
    strip = pl.BlockSpec((BACK, width), lambda i, m: (jnp.minimum(i, steps - 1), 0))
    flat = lambda start, count: pl.BlockSpec((width // 2, BACK), lambda i, m: (0, jnp.clip(i - start, 0, count - 1)))
    at_a, at_b = flat(0, CUT // BACK), flat(CUT // BACK, (MAIN - CUT) // BACK)
    return pl.pallas_call(
        back_body,
        out_shape=(jax.ShapeDtypeStruct(old.shape, F32), jax.ShapeDtypeStruct((width + 32, width), F32)),
        grid_spec=pltpu.PrefetchScalarGridSpec(
            num_scalar_prefetch=1, grid=(steps + 1,),
            in_specs=[
                at_a, at_a, at_b, at_b, strip, strip,
                pl.BlockSpec((BACK, width), lambda i, m: (m[1] * steps + jnp.minimum(i, steps - 1), 0)),
                whole(width, width), whole(1, width), pl.BlockSpec(memory_space=pl.ANY),
            ],
            out_specs=(pl.BlockSpec((BACK, width), lambda i, m: (m[1] * steps + i, 0)), whole(width + 32, width)),
        ),
        input_output_aliases={10: 0},
        compiler_params=params(),
        cost_estimate=pl.CostEstimate(flops=4 * MAIN * width * width, bytes_accessed=MAIN * width * 18, transcendentals=0),
    )(jnp.stack([core, chunk]), *a, *b, norm, slope, h, w_t, gamma, old)


def scatter_body(per, meta_ref, idx_ref, dh_ref, out_ref):
    step = pl.program_id(0)
    seq_len = out_ref.shape[1]
    spot = lax.broadcasted_iota(jnp.int32, (seq_len, WIN), 0).astype(F32)
    for i in range(per):
        hot = (spot == idx_ref[i]).astype(F32).astype(BF16)
        at = pl.multiple_of((meta_ref[step * per + i] - meta_ref[step * per]) * 8, 8)
        rows = dh_ref[pl.ds(at, WIN), :].astype(BF16)
        out_ref[i] = jnp.dot(hot, rows, preferred_element_type=F32).astype(BF16)


def scatter_pass(dh, idx_win, base, batch, seq_len, max_pred):
    width = dh.shape[1]
    per = 4
    span = (per - 1) * max_pred + WIN
    return pl.pallas_call(
        functools.partial(scatter_body, per),
        out_shape=jax.ShapeDtypeStruct((batch, seq_len, width), BF16),
        grid_spec=pltpu.PrefetchScalarGridSpec(
            num_scalar_prefetch=1, grid=(batch // per,),
            in_specs=[
                pl.BlockSpec((per, 1, WIN), lambda b, m: (b, 0, 0)),
                pl.BlockSpec((pl.Element(span), pl.Element(width)), lambda b, m: (m[b * per] * 8, 0)),
            ],
            out_specs=pl.BlockSpec((per, seq_len, width), lambda b, m: (b, 0, 0)),
        ),
        compiler_params=pltpu.CompilerParams(dimension_semantics=("arbitrary",), vmem_limit_bytes=VMEM_LIMIT),
        cost_estimate=pl.CostEstimate(flops=2 * batch * WIN * seq_len * width, bytes_accessed=batch * seq_len * width * 2, transcendentals=0),
    )(lax.div(base, 8), idx_win, dh)


def params():
    return pltpu.CompilerParams(dimension_semantics=("arbitrary",), vmem_limit_bytes=VMEM_LIMIT)


def scratch_array(*shape):
    return pl.pallas_call(
        lambda out_ref: None, out_shape=jax.ShapeDtypeStruct(shape, F32), out_specs=pl.BlockSpec(memory_space=pl.ANY)
    )()


def by_tile(rows, cols, start=0):
    return pl.BlockSpec((rows, cols), lambda j, *_: (j + start, 0))


def strip_of(start=0):
    return pl.BlockSpec((1, VT), lambda j, *_: (0, j + start))


def clear_tail(e_ref, shard):
    tail = shard % VT

    @pl.when(pl.program_id(0) == shard // VT)
    def _():
        e_ref[tail:] = jnp.zeros((VT - tail, e_ref.shape[1]), BF16)


def columns():
    return [slice(i, i + CB) for i in range(0, MAIN, CB)]


def logits_body(shard, target, e_ref, t_ref, bias_ref, lab_ref, soft_ref, stat_ref):
    clear_tail(e_ref, shard)
    bias = jnp.broadcast_to(bias_ref[...], (128, VT)).T
    bias = jnp.concatenate([bias] * (CB // 128), axis=1)
    vocab = lax.broadcasted_iota(jnp.int32, (VT, CB), 0)
    for cols in columns():
        z = jnp.dot(e_ref[...], t_ref[:, cols], preferred_element_type=F32) + bias
        top = jnp.max(z, axis=0, keepdims=True)
        soft = jnp.exp(z - top)
        soft_ref[:, cols] = soft
        stat_ref[FIRST, cols] = top
        stat_ref[SECOND, cols] = jnp.sum(soft, axis=0, keepdims=True)
        if target:
            hot = vocab == lab_ref[:, cols] - pl.program_id(0) * VT
            stat_ref[THIRD, cols] = jnp.sum(jnp.where(hot, z, 0.0), axis=0, keepdims=True)


def logits_pass(embed, t_t, bias, lab, target):
    shard, width = embed.shape
    steps = pl.cdiv(shard, VT)
    return pl.pallas_call(
        functools.partial(logits_body, shard, target),
        out_shape=(jax.ShapeDtypeStruct((steps * VT, MAIN), F32), jax.ShapeDtypeStruct((steps * 8, MAIN), F32)),
        grid_spec=pltpu.PrefetchScalarGridSpec(
            num_scalar_prefetch=0, grid=(steps,),
            in_specs=[by_tile(VT, width), whole(width, MAIN), strip_of(), whole(1, MAIN)],
            out_specs=(by_tile(VT, MAIN), by_tile(8, MAIN)),
        ),
        compiler_params=params(),
        cost_estimate=pl.CostEstimate(flops=2 * MAIN * shard * width, bytes_accessed=MAIN * shard * 4, transcendentals=MAIN * shard),
    )(embed, t_t, bias, lab)


def grad_logits(soft_ref, vec_ref, lab_ref, cols, vocab, step):
    soft = soft_ref[:, cols] * vec_ref[FIRST, cols]
    return jnp.where(vocab == lab_ref[:, cols] - step * VT, soft - vec_ref[SECOND, cols], soft)


def lane_groups(dz):
    acc = dz[:, :128]
    for k in range(128, CB, 128):
        acc = acc + dz[:, k:k + 128]
    return acc


def hidden_body(shard, core_ref, soft_ref, vec_ref, lab_ref, e_ref, dz_ref, keep_ref, give_ref, db_ref, dt_s):
    step = pl.program_id(0)
    half = keep_ref.shape[0]

    @pl.when(step == 0)
    def _():
        dt_s[...] = jnp.zeros_like(dt_s)

    clear_tail(e_ref, shard)
    vocab = lax.broadcasted_iota(jnp.int32, (VT, CB), 0)
    acc = []
    for cols in columns():
        dz = grad_logits(soft_ref, vec_ref, lab_ref, cols, vocab, step)
        acc.append(lane_groups(dz))
        dz_ref[:, cols] = dz.astype(BF16)
    dt_s[...] += lax.dot_general(e_ref[...], dz_ref[...], (((0,), (0,)), ((), ())), preferred_element_type=F32)
    db_ref[...] = jnp.sum(sum(acc[1:], acc[0]).T, axis=0, keepdims=True)

    @pl.when(step == pl.num_programs(0) - 1)
    def _():
        core = core_ref[0]
        keep_ref[...] = dt_s[pl.ds(pl.multiple_of(core * half, 8), half), :]
        give_ref[...] = dt_s[pl.ds(pl.multiple_of((1 - core) * half, 8), half), :]


def hidden_pass(soft, vec, lab, embed, core):
    shard, width = embed.shape
    padded = soft.shape[0]
    flat = whole(width // 2, MAIN)
    return pl.pallas_call(
        functools.partial(hidden_body, shard),
        out_shape=(
            jax.ShapeDtypeStruct((padded, MAIN), BF16),
            jax.ShapeDtypeStruct((width // 2, MAIN), F32), jax.ShapeDtypeStruct((width // 2, MAIN), F32),
            jax.ShapeDtypeStruct((1, padded), F32),
        ),
        grid_spec=pltpu.PrefetchScalarGridSpec(
            num_scalar_prefetch=1, grid=(padded // VT,),
            in_specs=[by_tile(VT, MAIN), by_tile(8, MAIN), whole(1, MAIN), by_tile(VT, width)],
            out_specs=(by_tile(VT, MAIN), flat, flat, strip_of()),
            scratch_shapes=[pltpu.VMEM((width, MAIN), F32)],
        ),
        compiler_params=params(),
        cost_estimate=pl.CostEstimate(flops=2 * MAIN * shard * width, bytes_accessed=MAIN * shard * 6, transcendentals=0),
    )(core.reshape(1), soft, vec, lab, embed)


def embed_body(start, meta_ref, dz_ref, soft_ref, vec_ref, lab_ref, t_own_ref, t_oth_ref, db_own_ref, old_ref, de_ref, db_ref, dz_s, old_s, sem):
    step = pl.program_id(0) + start
    tail = old_ref.shape[0] % VT

    @pl.when(pl.program_id(0) == 0)
    def _():
        old_s[...] = jnp.zeros_like(old_s)

    for rows, here in ((VT, step < old_ref.shape[0] // VT), (tail, step == old_ref.shape[0] // VT)):
        @pl.when((meta_ref[0] > 0) & here)
        def _():
            copy = pltpu.make_async_copy(old_ref.at[pl.ds(pl.multiple_of(step * VT, VT), rows)], old_s.at[:rows], sem)
            copy.start()
            copy.wait()

    vocab = lax.broadcasted_iota(jnp.int32, (VT, CB), 0)
    acc = []
    for cols in columns():
        dz = grad_logits(soft_ref, vec_ref, lab_ref, cols, vocab, step)
        acc.append(lane_groups(dz))
        dz_s[:, cols] = dz.astype(BF16)
    de_ref[...] = old_s[...] + jnp.dot(dz_ref[...], t_own_ref[...], preferred_element_type=F32)
    de_ref[...] += jnp.dot(dz_s[...], t_oth_ref[...], preferred_element_type=F32)
    db_ref[...] = db_own_ref[...] + jnp.sum(sum(acc[1:], acc[0]).T, axis=0, keepdims=True)


def embed_pass(start, count, dz_own, soft_oth, vec, lab, t_own, t_oth, db_own, old, chunk):
    shard, width = old.shape
    return pl.pallas_call(
        functools.partial(embed_body, start),
        out_shape=(jax.ShapeDtypeStruct((shard, width), F32), jax.ShapeDtypeStruct((1, count * VT), F32)),
        grid_spec=pltpu.PrefetchScalarGridSpec(
            num_scalar_prefetch=1, grid=(count,),
            in_specs=[
                by_tile(VT, MAIN, start), by_tile(VT, MAIN, start), by_tile(8, MAIN, start), whole(1, MAIN),
                whole(MAIN, width), whole(MAIN, width), strip_of(start), pl.BlockSpec(memory_space=pl.ANY),
            ],
            out_specs=(by_tile(VT, width, start), strip_of()),
            scratch_shapes=[pltpu.VMEM((VT, MAIN), BF16), pltpu.VMEM((VT, width), F32), pltpu.SemaphoreType.DMA],
        ),
        input_output_aliases={8: 0},
        compiler_params=params(),
        cost_estimate=pl.CostEstimate(flops=4 * MAIN * count * VT * width, bytes_accessed=MAIN * count * VT * 6 + count * VT * width * 4, transcendentals=0),
    )(chunk.reshape(1), dz_own, soft_oth, vec, lab, t_own, t_oth, db_own, old)


def combine(stat):
    top, tot, hit = (stat.reshape(-1, 8, MAIN)[:, i] for i in range(3))
    best = jnp.max(top, axis=0)
    stats = jnp.stack([best, jnp.sum(tot * jnp.exp(top - best), axis=0), jnp.sum(hit, axis=0)])
    every = (stats, swap_core(stats), swap_x(stats), lax.ppermute(stats, "tp", SWAP_DIAGONAL))
    tops = [part[0] for part in every]
    best = jnp.maximum(jnp.maximum(tops[0], tops[1]), jnp.maximum(tops[2], tops[3]))
    sums = [part[1] * jnp.exp(part[0] - best) for part in every]
    hits = [part[2] for part in every]
    stats = (best, *((v[0] + v[1]) + (v[2] + v[3]) for v in (sums, hits)))
    return stats, top


def tie(*values):
    return lax.optimization_barrier(values)


def solution(mesh):
    def local_step(hidden, positions, labels, weights, w_t, b_t, gamma, beta, embed, out_bias):
        batch, seq_len, width = hidden.shape
        max_pred = positions.shape[1]
        shard_vocab = embed.shape[0]
        tiles = pl.cdiv(shard_vocab, VT)
        tp = lax.axis_index("tp")
        core = tp % 2
        counts = jnp.sum(weights, axis=1).astype(jnp.int32)
        seq = jnp.arange(batch, dtype=jnp.int32)
        offsets = jnp.sum(jnp.where(seq[None, :] < seq[:, None], counts[None, :], 0), 1)
        n_own = jnp.sum(counts)
        n_oth = swap_dp(jnp.full((8, 128), n_own, jnp.int32))
        shift = offsets % 8
        base = offsets - shift
        live = jnp.where(jnp.arange(max_pred)[None, :] < counts[:, None], positions, -1).astype(F32)
        idx_win = jnp.full((batch, WIN), -1.0, F32)
        for k in range(8):
            moved = jnp.pad(live, ((0, 0), (k, WIN - max_pred - k)), constant_values=-1.0)
            idx_win = jnp.where((shift == k)[:, None], moved, idx_win)
        idx_win = idx_win[:, None, :]
        tok_rows = gather_pass(hidden, idx_win, base, CHUNKS * MAIN)
        n_oth, tok_rows = tie(n_oth, tok_rows)
        n_oth = n_oth[0, 0]
        trips = jnp.where(jnp.maximum(n_own, n_oth) > MAIN, CHUNKS, 1)
        denom = (n_own + n_oth).astype(F32) + LOSS_EPS
        bias = jnp.pad(out_bias, (0, tiles * VT - shard_vocab), constant_values=-jnp.inf)[None, :]
        vecs = jnp.stack([b_t, gamma, beta] + [jnp.zeros_like(b_t)] * 5)

        def local_labels(lab):
            lab = lab - tp * shard_vocab
            return jnp.where((lab >= 0) & (lab < shard_vocab), lab, -1)[None, :]

        def trip(carry):
            chunk, d_embed, d_rows, pack_sum, bias_sum, loss_sum = carry
            row = chunk * MAIN + jnp.arange(MAIN, dtype=jnp.int32)
            in_seq = (row[:, None] >= offsets[None, :]) & (row[:, None] < (offsets + counts)[None, :])
            slot_row = jnp.where(row < n_own, row - jnp.sum(jnp.where(in_seq, offsets[None, :], 0), 1), -1)
            lab_seq = jnp.dot(in_seq.astype(F32), labels.astype(F32), precision=lax.Precision.HIGHEST)
            slot_hot = slot_row[:, None] == jnp.arange(max_pred, dtype=jnp.int32)[None, :]
            lab_own = jnp.sum(jnp.where(slot_hot, lab_seq, 0.0), 1).astype(jnp.int32)
            lab_oth = swap_dp(lab_own)

            def vectors(stats, tops, n):
                scale = (row < n).astype(F32) / denom
                factor = jnp.exp(tops - stats[0]) * (scale / stats[1])
                first = jnp.arange(8, dtype=jnp.int32)[:, None] == 0
                return jnp.where(first, factor[:, None], scale).reshape(-1, MAIN)

            t_own, t_own_t, norm, slope, send = transform_pass(tok_rows, w_t, vecs, tp, chunk)
            got = swap_dp(send)
            soft_own, stat_own = logits_pass(embed, t_own_t, bias, local_labels(lab_own), True)
            got, stat_own, lab_oth = tie(got, stat_own, lab_oth)
            stat_own, tops_own = combine(stat_own)
            got_x, got_core = swap_x(got), swap_core(got)
            loss_sum = loss_sum + jnp.sum(jnp.where(row < n_own, jnp.log(stat_own[1]) + stat_own[0] - stat_own[2], 0.0))
            dz_own, keep, give, db_own = hidden_pass(soft_own, vectors(stat_own, tops_own, n_own), local_labels(lab_own), embed, core)
            got_x, got_core, keep = tie(got_x, got_core, keep)
            got_far, give = tie(swap_core(got_x), give)
            given = swap_core(give)
            t_oth, t_oth_t = collect_pass((got, got_x, got_core, got_far), tp)
            given, t_oth_t = tie(given, t_oth_t)
            chip_a, chip_b = keep[:, :CUT] + given[:, :CUT], keep[:, CUT:] + given[:, CUT:]
            chip_a, chip_b, t_oth_t = tie(chip_a, chip_b, t_oth_t)
            other_a = swap_x(chip_a)
            soft_oth, stat_oth = logits_pass(embed, t_oth_t, bias, local_labels(lab_oth), False)
            other_a, stat_oth = tie(other_a, stat_oth)
            stat_oth, tops_oth = combine(stat_oth)
            chip_b, *stat_oth = tie(chip_b, *stat_oth)
            other_b = swap_x(chip_b)
            mine_a = chip_a + other_a
            theirs_a = swap_core(mine_a)
            vec_oth = vectors(stat_oth, tops_oth, n_oth)

            def embed_tiles(start, count, old):
                return embed_pass(start, count, dz_own, soft_oth, vec_oth, local_labels(lab_oth), t_own, t_oth, db_own, old, chunk)

            d_embed, db_0 = embed_tiles(0, 7, d_embed)
            other_b, theirs_a, d_embed = tie(other_b, theirs_a, d_embed)
            mine_b = chip_b + other_b
            theirs_b = swap_core(mine_b)
            d_rows, pack = back_pass((mine_a, theirs_a), (mine_b, theirs_b), norm, slope, tok_rows, w_t, gamma[None, :], core, chunk, d_rows)
            quarter = pack.shape[0] // 4
            pack = lax.dynamic_slice_in_dim(pack, tp * quarter, quarter)
            pack, d_embed = tie(pack, d_embed)
            far = swap_dp(pack)
            d_embed, db_1 = embed_tiles(7, tiles - 7, d_embed)
            far, d_embed = tie(far, d_embed)
            bias_sum = bias_sum + jnp.concatenate([db_0, db_1], axis=1)
            return chunk + 1, d_embed, d_rows, pack_sum + (pack + far), bias_sum, loss_sum

        start = (
            jnp.int32(0), scratch_array(shard_vocab, width), scratch_array(CHUNKS * MAIN + BACK, width),
            jnp.zeros(((width + 32) // 4, width), F32), jnp.zeros((1, tiles * VT), F32), jnp.zeros((), F32),
        )
        _, d_embed, d_rows, pack, d_out_bias, loss = lax.while_loop(lambda carry: carry[0] < trips, trip, start)
        far = swap_x(pack)
        loss_oth = swap_dp(jnp.full((8, 128), loss))
        d_hidden = scatter_pass(d_rows, idx_win, base, batch, seq_len, max_pred)
        far, loss_oth, d_hidden = tie(far, loss_oth, d_hidden)
        pair = jnp.where(tp // 2 == 0, jnp.stack([pack, far]), jnp.stack([far, pack]))
        theirs = swap_core(pair)
        pack = jnp.where(core == 0, jnp.stack([pair, theirs], 1), jnp.stack([theirs, pair], 1)).reshape(-1, width)
        loss = (loss + loss_oth[0, 0]) / denom
        return loss, d_hidden, pack[:width], pack[width], pack[width + 1], pack[width + 2], d_embed, d_out_bias[0, :shard_vocab]

    in_specs = (P("dp", None, None), P("dp", None), P("dp", None), P("dp", None), P(None, None), P(None), P(None), P(None), P("tp", None), P("tp"))
    out_specs = (P(), P("dp", None, None), P(None, None), P(None), P(None), P(None), P("tp", None), P("tp"))
    return jax.shard_map(local_step, mesh=mesh, in_specs=in_specs, out_specs=out_specs, check_vma=False)
```
